32 devices in a mesh: dp: 2 (over core), seq: 16 (over z, y, x).
Axes of the slice: x: 2, y: 2, z: 4, core: 2. Of those that a mesh axis runs over, the one named last changes fastest.
Arguments:
- tokens: bfloat16 [16, 1024, 768], P('dp', 'seq'), may hold values from -6 to 6
- lengths: int32 [16], P('dp'), may hold values from 256 to 1024, as said below
- w_qkv: bfloat16 [768, 2304], P('seq', 'dp'), may hold values from -0.21875 to 0.21875
- w_out: bfloat16 [768, 768], P('seq', 'dp'), may hold values from -6 to 6
- w_gate: bfloat16 [768, 3072], P('seq', 'dp'), may hold values from -0.21875 to 0.21875
- w_up: bfloat16 [768, 3072], P('seq', 'dp'), may hold values from -0.21875 to 0.21875
- w_down: bfloat16 [3072, 768], P('seq', 'dp'), may hold values from -0.109375 to 0.109375
- ln_params: bfloat16 [4, 768], P(None, ('dp', 'seq')), may hold values from -2 to 2, as said below
- cotangent: bfloat16 [16, 1024, 768], P('dp', 'seq'), may hold values from -6 to 6
Outputs:
- output: bfloat16 [16, 1024, 768], P('dp', 'seq')
- grad_tokens: bfloat16 [16, 1024, 768], P('dp', 'seq')
- grad_w_qkv: float32 [768, 2304], P('seq', 'dp')
- grad_w_out: float32 [768, 768], P('seq', 'dp')
- grad_w_gate: float32 [768, 3072], P('seq', 'dp')
- grad_w_up: float32 [768, 3072], P('seq', 'dp')
- grad_w_down: float32 [3072, 768], P('seq', 'dp')
- grad_ln_params: float32 [4, 768], P(None, ('dp', 'seq'))
The draws below stay inside these ranges and needn't reach their ends.
Inputs may be any that keep to these rules, and one draw needn't show every extreme that they name: Slot s holds valid tokens at positions below lengths[s]; in every draw one slot has 1024 and one 1024 / 4. `ln_params`: rows 0 and 2 are gains, rows 1 and 3 biases.
All inputs are finite; a program needn't handle non-finite values.
Results may differ from the reference program's by a relative error of at most 0.025.
Values may be sent and summed in bfloat16 or wider, within the bound.
A program may use at most 192 MiB of HBM per device.

```python
import jax
import jax.numpy as jnp
from jax import lax

D = 768
HEADS = 12
HEAD_DIM = 64
FF = 3072
SLOT_LEN = 1024
SLOTS = 16


def draw_lengths(key, part):
    value_key, order_key = jax.random.split(jax.random.fold_in(key, 11))
    lowest = SLOT_LEN // 4
    drawn_len = jax.random.randint(value_key, (SLOTS,), lowest, SLOT_LEN + 1)
    order_idx = jax.random.permutation(order_key, SLOTS)
    drawn_len = jnp.where(order_idx == 0, SLOT_LEN, drawn_len)
    drawn_len = jnp.where(order_idx == 1, lowest, drawn_len)
    return drawn_len.astype(jnp.int32)


def draw_ln_params(key, part):
    gain_key, bias_key = jax.random.split(jax.random.fold_in(key, 23))
    row_kind = (jnp.arange(4) % 2 == 0)[:, None]
    gain_rows = 1.0 + 0.15 * jnp.clip(jax.random.normal(gain_key, (4, D), jnp.float32), -2.0, 2.0)
    bias_rows = 0.5 * jnp.clip(jax.random.normal(bias_key, (4, D), jnp.float32), -3.0, 3.0)
    return jnp.where(row_kind, gain_rows, bias_rows).astype(jnp.bfloat16)


def block_scale(key, shape, cuts, smallest, top_value):
    def one(position, blocks):
        steps = jax.random.uniform(jax.random.fold_in(jax.random.fold_in(key, 6), position), (blocks,), jnp.float32, smallest / len(cuts), top_value / len(cuts))
        return jnp.repeat(jnp.exp(steps), shape[position] // blocks).reshape((-1,) + (1,) * (len(shape) - position - 1))

    loudness = one(*cuts[0])
    for cut in cuts[1:]:
        loudness = loudness * one(*cut)
    return loudness


def scatter_about(rng, dims, width, most, pieces=(), kind=jnp.bfloat16):
    values = width * jax.random.normal(rng, dims, jnp.float32)
    if pieces:
        values = values * block_scale(rng, dims, pieces, -0.22, 0.18)
    return jnp.clip(values, -most, most).astype(kind)


def setup_inputs(seed: int = 0) -> dict:
    key_list = jax.random.split(jax.random.key(seed), 10)
    return {
        "tokens": scatter_about(key_list[0], (SLOTS, SLOT_LEN, D), 1.0, 6.0, ((0, 2), (1, 16))),
        "lengths": draw_lengths(jax.random.fold_in(key_list[9], 71), 0),
        "w_qkv": scatter_about(key_list[2], (D, 3 * D), D ** -0.5, 0.21875, ((0, 16), (1, 2))),
        "w_out": scatter_about(key_list[3], (D, D), 1 ** -0.5, 6.0, ((0, 16), (1, 2))),
        "w_gate": scatter_about(key_list[4], (D, FF), D ** -0.5, 0.21875, ((0, 16), (1, 2))),
        "w_up": scatter_about(key_list[5], (D, FF), D ** -0.5, 0.21875, ((0, 16), (1, 2))),
        "w_down": scatter_about(key_list[6], (FF, D), FF ** -0.5, 0.109375, ((0, 16), (1, 2))),
        "ln_params": draw_ln_params(jax.random.fold_in(key_list[9], 71), 0),
        "cotangent": scatter_about(key_list[8], (SLOTS, SLOT_LEN, D), 1.0, 6.0, ((0, 2), (1, 16))),
    }


@jax.custom_vjp
def low(v):
    return lax.optimization_barrier(v.astype(jnp.bfloat16)).astype(jnp.float32)

@jax.custom_vjp
def low_back(v):
    return v

def low_keep(v):
    return (low(v), None)

def low_pass(kept, grad):
    return (grad,)

def back_keep(v):
    return (v, None)

def back_low(kept, grad):
    return (low(grad),)
low.defvjp(low_keep, low_pass)
low_back.defvjp(back_keep, back_low)
highest_precision = lax.Precision.HIGHEST
norm_epsilon = 1e-12
score_scale = 0.125
masked_score = -1e+30

def rotary_tables(positions):
    pair_index = jnp.arange(HEAD_DIM // 2, dtype=jnp.float32)
    inverse = jnp.power(jnp.float32(1000.0), -2.0 * pair_index / HEAD_DIM)
    angles = positions.astype(jnp.float32)[:, None] * inverse[None, :]
    cos_tab = jnp.concatenate([jnp.cos(angles), jnp.cos(angles)], axis=-1)
    sin_tab = jnp.concatenate([jnp.sin(angles), jnp.sin(angles)], axis=-1)
    return (cos_tab, sin_tab)

def rotate(values, cos_tab, sin_tab):
    half_dim = values.shape[-1] // 2
    turned = jnp.concatenate([-values[..., half_dim:], values[..., :half_dim]], axis=-1)
    return values * cos_tab + turned * sin_tab

def layer_norm(values, gain_vec, bias_vec):
    center = values - lax.optimization_barrier(jnp.mean(values, axis=-1, keepdims=True))
    inv_std = lax.rsqrt(lax.optimization_barrier(jnp.mean(center * center, axis=-1, keepdims=True)) + norm_epsilon)
    return center * inv_std * gain_vec + bias_vec

def slot_forward(tokens, valid_keys, w_qkv, w_out, w_gate, w_up, w_down, ln_params):
    row_count = tokens.shape[0]
    qkv_pre = low_back(jnp.dot(tokens, w_qkv, precision=highest_precision))
    cos_tab, sin_tab = rotary_tables(jnp.arange(row_count))
    cos_tab = cos_tab[:, None, :]
    sin_tab = sin_tab[:, None, :]
    queries = low(rotate(qkv_pre[:, :D].reshape(row_count, HEADS, HEAD_DIM), cos_tab, sin_tab))
    keys_rot = low(rotate(qkv_pre[:, D:2 * D].reshape(row_count, HEADS, HEAD_DIM), cos_tab, sin_tab))
    values = low(qkv_pre[:, 2 * D:].reshape(row_count, HEADS, HEAD_DIM))
    block_len = min(512, row_count)

    def attend(query_block):
        scores = jnp.einsum('qhd,khd->hqk', query_block, keys_rot, precision=highest_precision) * score_scale
        scores = low_back(scores)
        scores = jnp.where(valid_keys[None, None, :], scores, masked_score)
        weights = low(jax.nn.softmax(scores, axis=-1))
        return jnp.einsum('hqk,khd->qhd', weights, values, precision=highest_precision)
    attended = lax.map(jax.checkpoint(attend), queries.reshape(row_count // block_len, block_len, HEADS, HEAD_DIM))
    attended = low(low_back(attended.reshape(row_count, D)))
    branch = low_back(jnp.dot(attended, w_out, precision=highest_precision))
    hidden = layer_norm(tokens + branch, ln_params[0], ln_params[1])
    hidden_low = low(hidden)
    gate_pre = low_back(jnp.dot(hidden_low, w_gate, precision=highest_precision))
    up_proj = low_back(jnp.dot(hidden_low, w_up, precision=highest_precision))
    inner_act = low(jax.nn.silu(gate_pre) * up_proj)
    branch_two = low_back(jnp.dot(inner_act, w_down, precision=highest_precision))
    result = layer_norm(hidden + branch_two, ln_params[2], ln_params[3])
    return result * valid_keys.astype(jnp.float32)[:, None]

def reference(tokens, lengths, w_qkv, w_out, w_gate, w_up, w_down, ln_params, cotangent):
    weights = tuple((matrix.astype(jnp.float32) for matrix in (w_qkv, w_out, w_gate, w_up, w_down, ln_params)))
    positions = jnp.arange(SLOT_LEN)

    def one_slot(totals, inputs):
        slot_tokens, length, slot_cot = inputs
        valid_keys = positions < length

        def forward(token_rows, mat_qkv, mat_out, mat_gate, mat_up, mat_down, norm_rows):
            return slot_forward(token_rows, valid_keys, mat_qkv, mat_out, mat_gate, mat_up, mat_down, norm_rows)
        result, pullback = jax.vjp(forward, slot_tokens.astype(jnp.float32), *weights)
        grads = pullback(slot_cot.astype(jnp.float32))
        totals = tuple((total + grad_in for total, grad_in in zip(totals, grads[1:])))
        return (totals, (result.astype(jnp.bfloat16), grads[0].astype(jnp.bfloat16)))
    zero_grads = tuple((jnp.zeros(matrix.shape, jnp.float32) for matrix in weights))
    totals, (outputs, input_grad) = lax.scan(one_slot, zero_grads, (tokens, lengths, cotangent))
    return (outputs, input_grad, totals[0], totals[1], totals[2], totals[3], totals[4], totals[5])
```

```python
import functools

import jax
import jax.numpy as jnp
from jax import lax
from jax.experimental import pallas as pl
from jax.experimental.pallas import tpu as pltpu
from jax.sharding import PartitionSpec as P

HEADS = 12
HEAD_DIM = 64


norm_epsilon = 1e-12
score_scale = 0.125
masked_score = -1e30


def shifted(shard, axis, by):
    count = lax.axis_size(axis)
    return lax.ppermute(shard, axis, [(i, (i + by) % count) for i in range(count)])


def rotary_tables(positions):
    pair_index = jnp.arange(HEAD_DIM // 2, dtype=jnp.float32)
    inverse = jnp.power(jnp.float32(1000.0), -2.0 * pair_index / HEAD_DIM)
    angles = positions.astype(jnp.float32)[:, None] * inverse[None, :]
    cos_tab = jnp.concatenate([jnp.cos(angles), jnp.cos(angles)], axis=-1)
    sin_tab = jnp.concatenate([jnp.sin(angles), jnp.sin(angles)], axis=-1)
    return (cos_tab, sin_tab)


def rotate(values, cos_tab, sin_tab):
    half_dim = values.shape[-1] // 2
    turned = jnp.concatenate([-values[..., half_dim:], values[..., :half_dim]], axis=-1)
    return values * cos_tab + turned * sin_tab


def norm_parts(values, gain_vec, bias_vec):
    center = values - jnp.mean(values, axis=-1, keepdims=True)
    inv_std = lax.rsqrt(jnp.mean(center * center, axis=-1, keepdims=True) + norm_epsilon)
    normed = center * inv_std
    return (normed * gain_vec + bias_vec, normed, inv_std)


def norm_back(grad_in, normed, inv_std, gain_vec):
    scaled = grad_in * gain_vec
    return inv_std * (
        scaled
        - jnp.mean(scaled, axis=-1, keepdims=True)
        - normed * jnp.mean(scaled * normed, axis=-1, keepdims=True)
    )


def heads_view(flat_rows):
    return flat_rows.reshape(flat_rows.shape[0], flat_rows.shape[1], HEADS, HEAD_DIM)


def attend_block(run_state, queries, key_blk, value_blk, key_start, lengths):
    run_max, run_sum, run_acc = run_state
    scores = (
        jnp.einsum(
            "sqhd,skhd->shqk",
            heads_view(queries),
            heads_view(key_blk),
            preferred_element_type=jnp.float32,
        )
        * score_scale
    )
    key_pos = key_start + jnp.arange(key_blk.shape[1], dtype=jnp.int32)
    key_mask = (key_pos[None, :] < lengths[:, None])[:, None, None, :]
    scores = jnp.where(key_mask, scores, masked_score)
    new_max = jnp.maximum(run_max, jnp.max(scores, axis=-1))
    exp_scores = jnp.where(key_mask, jnp.exp(scores - new_max[..., None]), 0.0)
    factor = jnp.exp(run_max - new_max)
    run_sum = run_sum * factor + jnp.sum(exp_scores, axis=-1)
    run_acc = run_acc * factor[..., None] + jnp.einsum(
        "shqk,skhd->shqd",
        exp_scores.astype(jnp.bfloat16),
        heads_view(value_blk),
        preferred_element_type=jnp.float32,
    )
    return (new_max, run_sum, run_acc)


def block_grads(queries, grad_att, log_total, delta_rows, key_blk, value_blk, key_ok):
    query_h = heads_view(queries)
    grad_h = heads_view(grad_att)
    key_h = heads_view(key_blk)
    scores = (
        jnp.einsum("sqhd,skhd->shqk", query_h, key_h, preferred_element_type=jnp.float32)
        * score_scale
    )
    key_mask = key_ok[:, None, None, :]
    soft_probs = jnp.where(key_mask, jnp.exp(scores - log_total[..., None]), 0.0)
    grad_probs = jnp.einsum(
        "sqhd,skhd->shqk", grad_h, heads_view(value_blk), preferred_element_type=jnp.float32
    )
    grad_scores = (soft_probs * (grad_probs - delta_rows[..., None])).astype(jnp.bfloat16)
    part_q = (
        jnp.einsum("shqk,skhd->sqhd", grad_scores, key_h, preferred_element_type=jnp.float32)
        * score_scale
    )
    part_k = (
        jnp.einsum("shqk,sqhd->skhd", grad_scores, query_h, preferred_element_type=jnp.float32)
        * score_scale
    )
    part_v = jnp.einsum(
        "shqk,sqhd->skhd",
        soft_probs.astype(jnp.bfloat16),
        grad_h,
        preferred_element_type=jnp.float32,
    )
    shape_out = queries.shape
    return (part_q.reshape(shape_out), part_k.reshape(key_blk.shape), part_v.reshape(key_blk.shape))


def local(tokens, lengths, w_qkv, w_out, w_gate, w_up, w_down, ln_params, cotangent):
    slot_count, span_len, width = tokens.shape
    row_count = slot_count * span_len
    cycle_size = lax.axis_size("seq")
    my_index = lax.axis_index("seq")
    row_qkv, row_out, row_gate, row_up, row_down, row_norm = (
        lax.all_gather(w_qkv, "seq", axis=0, tiled=True),
        lax.all_gather(w_out, "seq", axis=0, tiled=True),
        lax.all_gather(w_gate, "seq", axis=0, tiled=True),
        lax.all_gather(w_up, "seq", axis=0, tiled=True),
        lax.all_gather(w_down, "seq", axis=0, tiled=True),
        lax.all_gather(ln_params, "seq", axis=1, tiled=True),
    )
    wide_qkv, wide_out, wide_gate, wide_up, wide_down, wide_norm = (
        lax.all_gather(row_qkv, "dp", axis=1, tiled=True),
        lax.all_gather(row_out, "dp", axis=1, tiled=True),
        lax.all_gather(row_gate, "dp", axis=1, tiled=True),
        lax.all_gather(row_up, "dp", axis=1, tiled=True),
        lax.all_gather(row_down, "dp", axis=1, tiled=True),
        lax.all_gather(row_norm, "dp", axis=1, tiled=True),
    )
    norm_full = wide_norm.astype(jnp.float32)
    flat_tokens = tokens.reshape(row_count, width)
    token_f32 = flat_tokens.astype(jnp.float32)
    positions = my_index * span_len + jnp.arange(span_len, dtype=jnp.int32)
    row_valid = (positions[None, :] < lengths[:, None]).astype(jnp.float32).reshape(row_count, 1)
    cos_tab, sin_tab = rotary_tables(positions)
    cos_four = cos_tab[None, :, None, :]
    sin_four = sin_tab[None, :, None, :]
    qkv_pre = jnp.dot(flat_tokens, wide_qkv, preferred_element_type=jnp.float32)
    split_qkv = qkv_pre.reshape(slot_count, span_len, 3, HEADS, HEAD_DIM)
    queries = (
        rotate(split_qkv[:, :, 0], cos_four, sin_four)
        .astype(jnp.bfloat16)
        .reshape(slot_count, span_len, width)
    )
    keys_rot = (
        rotate(split_qkv[:, :, 1], cos_four, sin_four)
        .astype(jnp.bfloat16)
        .reshape(slot_count, span_len, width)
    )
    values = split_qkv[:, :, 2].astype(jnp.bfloat16).reshape(slot_count, span_len, width)
    start_state = (
        jnp.full((slot_count, HEADS, span_len), masked_score, jnp.float32),
        jnp.zeros((slot_count, HEADS, span_len), jnp.float32),
        jnp.zeros((slot_count, HEADS, span_len, HEAD_DIM), jnp.float32),
    )
    key_piece = lax.all_gather(keys_rot, "seq", axis=1, tiled=True)
    value_piece = lax.all_gather(values, "seq", axis=1, tiled=True)
    block_count = key_piece.shape[1] // span_len

    def one_block(block_id, inner_state):
        offset = block_id * span_len
        key_blk = lax.dynamic_slice_in_dim(key_piece, offset, span_len, axis=1)
        value_blk = lax.dynamic_slice_in_dim(value_piece, offset, span_len, axis=1)
        return attend_block(inner_state, queries, key_blk, value_blk, offset, lengths)

    run_max, run_sum, run_acc = lax.fori_loop(0, block_count, one_block, start_state)
    attended = run_acc / run_sum[..., None]
    log_total = run_max + jnp.log(run_sum)
    attn_low = attended.transpose(0, 2, 1, 3).reshape(row_count, width).astype(jnp.bfloat16)
    branch = jnp.dot(attn_low, wide_out, preferred_element_type=jnp.float32)
    hidden, normed_one, inv_one = norm_parts(token_f32 + branch, norm_full[0], norm_full[1])
    hidden_low = hidden.astype(jnp.bfloat16)
    gate_pre = jnp.dot(hidden_low, wide_gate, preferred_element_type=jnp.float32)
    up_proj = jnp.dot(hidden_low, wide_up, preferred_element_type=jnp.float32)
    activated = jax.nn.silu(gate_pre)
    inner_low = (activated * up_proj).astype(jnp.bfloat16)
    branch_two = jnp.dot(inner_low, wide_down, preferred_element_type=jnp.float32)
    result, normed_two, inv_two = norm_parts(hidden + branch_two, norm_full[2], norm_full[3])
    output = (result * row_valid).astype(jnp.bfloat16).reshape(slot_count, span_len, width)
    back_qkv, back_out, back_gate, back_up, back_down, back_norm = (
        lax.all_gather(w_qkv, "seq", axis=0, tiled=True),
        lax.all_gather(w_out, "seq", axis=0, tiled=True),
        lax.all_gather(w_gate, "seq", axis=0, tiled=True),
        lax.all_gather(w_up, "seq", axis=0, tiled=True),
        lax.all_gather(w_down, "seq", axis=0, tiled=True),
        lax.all_gather(ln_params, "seq", axis=1, tiled=True),
    )
    wide_qkv, wide_out, wide_gate, wide_up, wide_down, wide_norm = (
        lax.all_gather(back_qkv, "dp", axis=1, tiled=True),
        lax.all_gather(back_out, "dp", axis=1, tiled=True),
        lax.all_gather(back_gate, "dp", axis=1, tiled=True),
        lax.all_gather(back_up, "dp", axis=1, tiled=True),
        lax.all_gather(back_down, "dp", axis=1, tiled=True),
        lax.all_gather(back_norm, "dp", axis=1, tiled=True),
    )
    norm_full = wide_norm.astype(jnp.float32)
    grad_out = cotangent.reshape(row_count, width).astype(jnp.float32) * row_valid
    gain_two_grad = jnp.sum(grad_out * normed_two, axis=0)
    bias_two_grad = jnp.sum(grad_out, axis=0)
    grad_res2 = norm_back(grad_out, normed_two, inv_two, norm_full[2])
    grad_branch2 = grad_res2.astype(jnp.bfloat16)
    grad_wdown = jnp.einsum(
        "rf,rd->fd", inner_low, grad_branch2, preferred_element_type=jnp.float32
    )
    grad_inner = jnp.einsum(
        "rd,fd->rf", grad_branch2, wide_down, preferred_element_type=jnp.float32
    )
    sigma = jax.nn.sigmoid(gate_pre)
    grad_gate = (grad_inner * up_proj * sigma * (1.0 + gate_pre * (1.0 - sigma))).astype(
        jnp.bfloat16
    )
    grad_up = (grad_inner * activated).astype(jnp.bfloat16)
    grad_wgate = jnp.einsum("rd,rf->df", hidden_low, grad_gate, preferred_element_type=jnp.float32)
    grad_wup = jnp.einsum("rd,rf->df", hidden_low, grad_up, preferred_element_type=jnp.float32)
    grad_hidden = (
        grad_res2
        + jnp.einsum("rf,df->rd", grad_gate, wide_gate, preferred_element_type=jnp.float32)
        + jnp.einsum("rf,df->rd", grad_up, wide_up, preferred_element_type=jnp.float32)
    )
    gain_one_grad = jnp.sum(grad_hidden * normed_one, axis=0)
    bias_one_grad = jnp.sum(grad_hidden, axis=0)
    grad_res1 = norm_back(grad_hidden, normed_one, inv_one, norm_full[0])
    grad_branch1 = grad_res1.astype(jnp.bfloat16)
    grad_wout = jnp.einsum("ri,rd->id", attn_low, grad_branch1, preferred_element_type=jnp.float32)
    grad_att = (
        jnp.einsum("rd,id->ri", grad_branch1, wide_out, preferred_element_type=jnp.float32)
        .astype(jnp.bfloat16)
        .reshape(slot_count, span_len, width)
    )
    zero_rows = jnp.zeros((slot_count, span_len, width), jnp.float32)
    delta_rows = jnp.einsum("sqhd,shqd->shq", heads_view(grad_att).astype(jnp.float32), attended)

    def key_turn(turn_id, run_state):
        key_cur, value_cur, grad_keys, grad_values, grad_query = run_state
        key_start = (my_index - turn_id) % cycle_size * span_len
        key_ok = (key_start + jnp.arange(span_len, dtype=jnp.int32))[None, :] < lengths[:, None]
        part_q, part_k, part_v = block_grads(
            queries, grad_att, log_total, delta_rows, key_cur, value_cur, key_ok
        )
        key_cur, value_cur = shifted((key_cur, value_cur), "seq", 1)
        grad_keys, grad_values = (
            shifted((grad_keys + part_k).astype(jnp.bfloat16), "seq", 1).astype(jnp.float32),
            shifted((grad_values + part_v).astype(jnp.bfloat16), "seq", 1).astype(jnp.float32),
        )
        return (key_cur, value_cur, grad_keys, grad_values, grad_query + part_q)

    key_cur, value_cur, grad_keys, grad_values, grad_query = lax.fori_loop(
        0, cycle_size - 1, key_turn, (keys_rot, values, zero_rows, zero_rows, zero_rows)
    )
    key_start = (my_index - (cycle_size - 1)) % cycle_size * span_len
    key_ok = (key_start + jnp.arange(span_len, dtype=jnp.int32))[None, :] < lengths[:, None]
    part_q, part_k, part_v = block_grads(
        queries, grad_att, log_total, delta_rows, key_cur, value_cur, key_ok
    )
    grad_query = grad_query + part_q
    grad_keys, grad_values = (
        shifted((grad_keys + part_k).astype(jnp.bfloat16), "seq", 1).astype(jnp.float32),
        shifted((grad_values + part_v).astype(jnp.bfloat16), "seq", 1).astype(jnp.float32),
    )
    query_back = rotate(heads_view(grad_query), cos_four, -sin_four)
    key_back = rotate(heads_view(grad_keys), cos_four, -sin_four)
    grad_qkv = jnp.stack([query_back, key_back, heads_view(grad_values)], axis=2)
    grad_qkv = grad_qkv.reshape(row_count, 3 * width).astype(jnp.bfloat16)
    grad_wqkv = jnp.einsum("rd,re->de", flat_tokens, grad_qkv, preferred_element_type=jnp.float32)
    grad_tokens = grad_res1 + jnp.einsum(
        "re,de->rd", grad_qkv, wide_qkv, preferred_element_type=jnp.float32
    )
    grad_tokens = grad_tokens.astype(jnp.bfloat16).reshape(slot_count, span_len, width)
    grad_norm = jnp.stack([gain_one_grad, bias_one_grad, gain_two_grad, bias_two_grad], axis=0)
    col_qkv, col_out, col_gate, col_up, col_down, col_norm = (
        lax.psum_scatter(
            grad_wqkv.astype(jnp.bfloat16), "dp", scatter_dimension=1, tiled=True
        ).astype(jnp.float32),
        lax.psum_scatter(
            grad_wout.astype(jnp.bfloat16), "dp", scatter_dimension=1, tiled=True
        ).astype(jnp.float32),
        lax.psum_scatter(
            grad_wgate.astype(jnp.bfloat16), "dp", scatter_dimension=1, tiled=True
        ).astype(jnp.float32),
        lax.psum_scatter(
            grad_wup.astype(jnp.bfloat16), "dp", scatter_dimension=1, tiled=True
        ).astype(jnp.float32),
        lax.psum_scatter(
            grad_wdown.astype(jnp.bfloat16), "dp", scatter_dimension=1, tiled=True
        ).astype(jnp.float32),
        lax.psum_scatter(
            grad_norm.astype(jnp.bfloat16), "dp", scatter_dimension=1, tiled=True
        ).astype(jnp.float32),
    )
    own_qkv, own_out, own_gate, own_up, own_down, own_norm = (
        lax.psum_scatter(
            col_qkv.astype(jnp.bfloat16), "seq", scatter_dimension=0, tiled=True
        ).astype(jnp.float32),
        lax.psum_scatter(
            col_out.astype(jnp.bfloat16), "seq", scatter_dimension=0, tiled=True
        ).astype(jnp.float32),
        lax.psum_scatter(
            col_gate.astype(jnp.bfloat16), "seq", scatter_dimension=0, tiled=True
        ).astype(jnp.float32),
        lax.psum_scatter(
            col_up.astype(jnp.bfloat16), "seq", scatter_dimension=0, tiled=True
        ).astype(jnp.float32),
        lax.psum_scatter(
            col_down.astype(jnp.bfloat16), "seq", scatter_dimension=0, tiled=True
        ).astype(jnp.float32),
        lax.psum_scatter(
            col_norm.astype(jnp.bfloat16), "seq", scatter_dimension=1, tiled=True
        ).astype(jnp.float32),
    )
    return (output, grad_tokens, own_qkv, own_out, own_gate, own_up, own_down, own_norm)


MESH = pl.DeviceIdType.MESH
CHIPS, ZS = 16, 4
OFFSETS = sorted(((dx, dy, dz) for dx in (0, 1) for dy in (0, 1) for dz in range(-3, 4)),
                 key=lambda o: (o[0] + o[1], abs(o[2]), o))
ORDERS = ("zxy", "zxy", "xzy", "yzx", "zyx", "zxy")


def pick(index, values):
    out = jnp.int32(0)
    for place, value in enumerate(values):
        if value:
            out = out + jnp.where(index == place, jnp.int32(value), 0)
    return out


def place():
    core, chip = lax.axis_index("dp"), lax.axis_index("seq")
    return core, chip, chip % 2, (chip // 2) % 2, chip // 4


def chip_at(x, y, z):
    return (z * 2 + y) * 2 + x


def meet_all(core, chip):
    barrier = pltpu.get_barrier_semaphore()
    me = core * CHIPS + chip

    def greet(step, carry):
        other = (me + step) % (2 * CHIPS)
        pl.semaphore_signal(barrier, inc=1, device_id={"dp": other // CHIPS, "seq": other % CHIPS}, device_id_type=MESH)
        return carry

    lax.fori_loop(1, 2 * CHIPS, greet, 0)
    pl.semaphore_wait(barrier, 2 * CHIPS - 1)


def spread(order, dx, dy, dz):
    zero = {"x": dx == 0, "y": dy == 0, "z": dz == 0}
    flags = {}
    for position, axis in enumerate(order):
        flag = zero[axis] if axis != "z" else None
        for later in order[position + 1:]:
            flag = zero[later] if flag is None else flag & zero[later]
        flags[axis] = flag
    up, down = dz <= 0, dz >= 0
    if flags["z"] is not None:
        up, down = up & flags["z"], down & flags["z"]
    return flags["x"], flags["y"], up, down


def gather_kernel(tok, cot, *refs):
    count = len(ORDERS)
    shards, refs = refs[:count], refs[count:]
    (x_all, c_own), refs = refs[:2], refs[2:]
    wides, refs = refs[:count], refs[count:]
    send_sem, recv_sem, sib_sem, tok_send, tok_recv, tok_sib, cot_recv, own_sem = refs
    core, chip, x, y, z = place()
    other = 1 - core
    slots, span = tok.shape[0], tok.shape[1]
    half = CHIPS // 2

    def region(m, owner, source):
        if m == count - 1:
            return wides[m].at[owner * CHIPS + source]
        rows, cols = shards[m].shape
        return wides[m].at[owner, pl.ds(pl.multiple_of(source * rows, rows), rows)]

    def piece(m, source, link, device, own=None):
        target = region(m, core, source)
        if link == 4:
            recv = sib_sem.at[m, source]
        else:
            recv = recv_sem.at[m, source]
        return pltpu.make_async_remote_copy(
            src_ref=target if own is None else own, dst_ref=target, send_sem=send_sem.at[m, link, source],
            recv_sem=recv, device_id=device, device_id_type=MESH)

    neighbours = (
        {"dp": core, "seq": chip_at(1 - x, y, z)},
        {"dp": core, "seq": chip_at(x, 1 - y, z)},
        {"dp": core, "seq": chip_at(x, y, jnp.minimum(z + 1, ZS - 1))},
        {"dp": core, "seq": chip_at(x, y, jnp.maximum(z - 1, 0))},
        {"dp": other, "seq": chip},
    )

    def goes(m, dx, dy, dz):
        fx, fy, up, down = spread(ORDERS[m], dx, dy, dz)
        return fx, fy, up & (z < ZS - 1), down & (z > 0), None

    meet_all(core, chip)

    def deliver(source, target, sends, recvs):
        mine = (chip // half == core)

        def one(j, carry):
            slot = (chip + 1 + j) % half
            to = core * half + slot
            src, dst = source.at[slot], target
            self_copy = mine & (to == chip)

            @pl.when(self_copy)
            def _():
                pltpu.make_async_copy(src, dst, recvs.at[chip % half]).start()

            @pl.when(jnp.logical_not(self_copy))
            def _():
                pltpu.make_async_remote_copy(
                    src_ref=src, dst_ref=dst, send_sem=sends.at[slot], recv_sem=recvs.at[chip % half],
                    device_id={"dp": chip // half, "seq": to}, device_id_type=MESH).start()
            return carry

        lax.fori_loop(0, slots, one, 0)

    def rows_of(ref, index):
        return ref.at[pl.ds(pl.multiple_of(index * span, span), span)]

    deliver(tok, rows_of(x_all, chip), tok_send.at[0], tok_recv)
    for m in range(count):
        for link in range(5):
            copy = piece(m, chip, link, neighbours[link], own=shards[m])
            if link == 2:
                pl.when(z < ZS - 1)(copy.start)
            elif link == 3:
                pl.when(z > 0)(copy.start)
            else:
                copy.start()
        pltpu.make_async_copy(shards[m], region(m, core, chip), own_sem.at[m]).start()
    deliver(cot, rows_of(c_own, chip % half), tok_send.at[1], cot_recv)

    def step(index, carry):
        dx = pick(index, [o[0] for o in OFFSETS])
        dy = pick(index, [o[1] for o in OFFSETS])
        dz = pick(index, [o[2] for o in OFFSETS])

        @pl.when((z + dz >= 0) & (z + dz < ZS))
        def _():
            source = chip_at((x + dx) % 2, (y + dy) % 2, z + dz)
            for m in range(count):
                piece(m, source, 0, neighbours[0]).wait_recv()
                flags = goes(m, dx, dy, dz)
                for link in range(5):
                    copy = piece(m, source, link, neighbours[link])
                    if flags[link] is None:
                        copy.start()
                    else:
                        pl.when(flags[link])(copy.start)
        return carry

    lax.fori_loop(1, 5, step, 0)

    def relay(i, carry):
        source = core * half + i
        block = rows_of(x_all, source)
        pltpu.make_async_copy(block, block, tok_recv.at[i]).wait()
        pltpu.make_async_remote_copy(
            src_ref=block, dst_ref=block, send_sem=tok_send.at[2, i], recv_sem=tok_sib.at[i],
            device_id=neighbours[4], device_id_type=MESH).start()
        return carry

    lax.fori_loop(0, half, relay, 0)
    lax.fori_loop(5, len(OFFSETS), step, 0)

    def ends(i, carry):
        block = rows_of(c_own, i)
        pltpu.make_async_copy(block, block, cot_recv.at[i]).wait()
        block = rows_of(x_all, other * half + i)
        pltpu.make_async_copy(block, block, tok_sib.at[i]).wait()
        block = rows_of(x_all, core * half + i)
        pltpu.make_async_copy(block, block, tok_send.at[2, i]).wait()
        slot = i
        self_copy = (chip // half == core) & (core * half + slot == chip)

        @pl.when(jnp.logical_not(self_copy))
        def _():
            pltpu.make_async_copy(tok.at[slot], tok.at[slot], tok_send.at[0, slot]).wait()
            pltpu.make_async_copy(cot.at[slot], cot.at[slot], tok_send.at[1, slot]).wait()
        return carry

    lax.fori_loop(0, half, ends, 0)

    def last(source, carry):
        dx, dy = (source % 2 - x) % 2, ((source // 2) % 2 - y) % 2
        dz = source // 4 - z
        for m in range(count):
            block = region(m, other, source)
            pltpu.make_async_copy(block, block, sib_sem.at[m, source]).wait()
            block = region(m, core, source)
            flags = goes(m, dx, dy, dz)
            for link in range(5):
                sent = pltpu.make_async_copy(block, block, send_sem.at[m, link, source])
                if flags[link] is None:
                    sent.wait()
                else:
                    pl.when(flags[link])(sent.wait)
        return carry

    lax.fori_loop(0, CHIPS, last, 0)
    for m in range(count):
        pltpu.make_async_copy(shards[m], region(m, core, chip), own_sem.at[m]).wait()


def gather(tokens, cotangent, shards):
    count = len(shards)
    slots, span, width = tokens.shape
    low = jnp.bfloat16
    outs = [jax.ShapeDtypeStruct((span * CHIPS, width), low), jax.ShapeDtypeStruct((span * CHIPS // 2, width), low)]
    for m, shard in enumerate(shards):
        if m == count - 1:
            outs.append(jax.ShapeDtypeStruct((2 * CHIPS,) + shard.shape, shard.dtype))
        else:
            outs.append(jax.ShapeDtypeStruct((2, shard.shape[0] * CHIPS, shard.shape[1]), shard.dtype))
    dma = pltpu.SemaphoreType.DMA
    anywhere = pl.BlockSpec(memory_space=pl.ANY)
    return pl.pallas_call(
        gather_kernel,
        out_shape=outs,
        in_specs=[anywhere] * (2 + count),
        out_specs=[anywhere] * len(outs),
        scratch_shapes=[dma((count, 5, CHIPS)), dma((count, CHIPS)), dma((count, CHIPS)), dma((3, 8)), dma((8,)), dma((8,)), dma((8,)), dma((count,))],
        compiler_params=pltpu.CompilerParams(collective_id=0, has_side_effects=True),
        name="gather",
    )(tokens, cotangent, *shards)


SIDES = {"x": 2, "y": 2, "z": ZS}


def slots_of(order):
    sizes = {}
    room = 1
    for axis in order:
        sizes[axis] = room * (ZS if axis == "z" else 1)
        room *= SIDES[axis]
    return sizes["x"], sizes["y"], sizes["z"], sizes["z"]


def slot_index(order, link, x, y, z):
    axis = "xyzz"[link]
    index = 0
    for before in order:
        if before == axis:
            break
        index = index * SIDES[before] + {"x": x, "y": y, "z": z}[before]
    if axis == "z":
        index = index * ZS + z
    return index


def scatter_kernel(y_own, gt_own, gt_other, *refs):
    count = len(ORDERS)
    grads, refs = refs[:count], refs[count:]
    (y_out, gt_out), refs = refs[:2], refs[2:]
    finals, refs = refs[:count], refs[count:]
    accs, refs = refs[:count], refs[count:]
    sibs, refs = refs[:count], refs[count:]
    lands, refs = refs[:4 * count], refs[4 * count:]
    tmps, refs = refs[:count], refs[count:]
    gt_mine, gt_sib, gt_low, refs = refs[0], refs[1], refs[2], refs[3:]
    send_sem, recv_sem, sib_send, sib_recv, own_sem, gt_sem, tok_send, y_recv, gt_recv = refs
    core, chip, x, y, z = place()
    other = 1 - core
    half = CHIPS // 2
    span = y_out.shape[1]
    rows_of = [tmp.shape[0] for tmp in tmps]

    neighbours = (
        {"dp": core, "seq": chip_at(1 - x, y, z)},
        {"dp": core, "seq": chip_at(x, 1 - y, z)},
        {"dp": core, "seq": chip_at(x, y, jnp.minimum(z + 1, ZS - 1))},
        {"dp": core, "seq": chip_at(x, y, jnp.maximum(z - 1, 0))},
    )
    sibling = {"dp": other, "seq": chip}

    def block(ref, m, dest):
        if m == count - 1:
            return ref.at[dest]
        return ref.at[pl.ds(pl.multiple_of(dest * rows_of[m], rows_of[m]), rows_of[m])]

    def to_sibling(m, dest):
        source = grads[m].at[other * CHIPS + dest] if m == count - 1 else block(grads[m].at[other], m, dest)
        return pltpu.make_async_remote_copy(
            src_ref=source, dst_ref=block(sibs[m], m, dest), send_sem=sib_send.at[m, dest], recv_sem=sib_recv.at[m, dest],
            device_id=sibling, device_id_type=MESH)

    def own_load(m, dest):
        source = grads[m].at[core * CHIPS + dest] if m == count - 1 else block(grads[m].at[core], m, dest)
        return pltpu.make_async_copy(source, block(accs[m], m, dest), own_sem.at[m, dest])

    meet_all(core, chip)

    mine = pltpu.make_async_copy(gt_own, gt_mine, gt_sem.at[0])
    mine.start()
    cross = pltpu.make_async_remote_copy(src_ref=gt_other, dst_ref=gt_sib, send_sem=gt_sem.at[1], recv_sem=gt_sem.at[2],
                                         device_id=sibling, device_id_type=MESH)
    cross.start()

    def dest_of(index):
        dx = pick(index, [o[0] for o in OFFSETS[::-1]])
        dy = pick(index, [o[1] for o in OFFSETS[::-1]])
        dz = pick(index, [o[2] for o in OFFSETS[::-1]])
        return dx, dy, dz, (z + dz >= 0) & (z + dz < ZS), (x + dx) % 2, (y + dy) % 2, jnp.clip(z + dz, 0, ZS - 1)

    def begin(index, carry):
        dx, dy, dz, valid, tx, ty, tz = dest_of(index)

        @pl.when(valid)
        def _():
            dest = chip_at(tx, ty, tz)
            for m in range(count):
                to_sibling(m, dest).start()
                own_load(m, dest).start()
        return carry

    lax.fori_loop(0, len(OFFSETS), begin, 0)

    def deliver(source, target, k, recvs):
        def one(j, carry):
            i = (chip + 1 + j) % half
            to_core, to_chip = chip // half, core * half + i
            src = source.at[pl.ds(pl.multiple_of(i * span, span), span)]
            dst = target.at[chip % half]
            self_copy = (to_core == core) & (to_chip == chip)

            @pl.when(self_copy)
            def _():
                pltpu.make_async_copy(src, dst, recvs.at[chip % half]).start()

            @pl.when(jnp.logical_not(self_copy))
            def _():
                pltpu.make_async_remote_copy(
                    src_ref=src, dst_ref=dst, send_sem=tok_send.at[k, i], recv_sem=recvs.at[chip % half],
                    device_id={"dp": to_core, "seq": to_chip}, device_id_type=MESH).start()
            return carry

        lax.fori_loop(0, half, one, 0)

    deliver(y_own, y_out, 0, y_recv)
    mine.wait()
    cross.wait()
    gt_low[...] = (gt_mine[...] + gt_sib[...].astype(jnp.float32)).astype(jnp.bfloat16)
    deliver(gt_low, gt_out, 1, gt_recv)

    def step(index, carry):
        dx, dy, dz, valid, tx, ty, tz = dest_of(index)

        @pl.when(valid)
        def _():
            dest = chip_at(tx, ty, tz)
            for m in range(count):
                order = ORDERS[m]
                fx, fy, up, down = spread(order, dx, dy, dz)
                flags = (fx, fy, up & (z < ZS - 1), down & (z > 0))
                own_load(m, dest).wait()
                to_sibling(m, dest).wait_recv()
                tmp, acc = tmps[m], block(accs[m], m, dest)
                tmp[...] = acc[...].astype(jnp.float32) + block(sibs[m], m, dest)[...].astype(jnp.float32)
                for link in range(4):
                    land = lands[4 * m + link].at[slot_index(order, link, tx, ty, tz)]

                    @pl.when(flags[link])
                    def _():
                        pltpu.make_async_copy(land, land, recv_sem.at[m, link, dest]).wait()
                        tmp[...] += land[...].astype(jnp.float32)
                away = {"x": dx != 0, "y": dy != 0, "z": dz != 0}
                taken = None
                last = (index == len(OFFSETS) - 1)

                @pl.when(jnp.logical_not(last))
                def _():
                    acc[...] = tmp[...].astype(acc.dtype)

                for axis in order[::-1]:
                    here = away[axis] if taken is None else away[axis] & jnp.logical_not(taken)
                    taken = away[axis] if taken is None else taken | away[axis]
                    for link in {"x": (0,), "y": (1,), "z": (2, 3)}[axis]:
                        go = here if axis != "z" else (here & (dz > 0 if link == 2 else dz < 0))
                        there = {0: 0, 1: 1, 2: 3, 3: 2}[link]

                        @pl.when(go)
                        def _():
                            pltpu.make_async_remote_copy(
                                src_ref=acc, dst_ref=lands[4 * m + there].at[slot_index(order, there, tx, ty, tz)],
                                send_sem=send_sem.at[m, dest], recv_sem=recv_sem.at[m, there, dest],
                                device_id=neighbours[link], device_id_type=MESH).start()

                @pl.when(last)
                def _():
                    finals[m][...] = tmp[...]
        return carry

    lax.fori_loop(0, len(OFFSETS), step, 0)

    def ends(i, carry):
        for out, recvs, k in ((y_out, y_recv, 0), (gt_out, gt_recv, 1)):
            pltpu.make_async_copy(out.at[i], out.at[i], recvs.at[i]).wait()
            self_copy = (chip // half == core) & (core * half + i == chip)

            @pl.when(jnp.logical_not(self_copy))
            def _():
                pltpu.make_async_copy(out.at[i], out.at[i], tok_send.at[k, i]).wait()
        return carry

    lax.fori_loop(0, half, ends, 0)

    def last(dest, carry):
        for m in range(count):
            to_sibling(m, dest).wait_send()

            @pl.when(dest != chip)
            def _():
                part = block(accs[m], m, dest)
                pltpu.make_async_copy(part, part, send_sem.at[m, dest]).wait()
        return carry

    lax.fori_loop(0, CHIPS, last, 0)


def scatter(y_own, gt_own, gt_other, grads):
    count = len(grads)
    half_rows, width = y_own.shape
    span = half_rows // 8
    anywhere, vmem = pl.BlockSpec(memory_space=pl.ANY), pl.BlockSpec(memory_space=pltpu.VMEM)
    finals, accs, sibs, lands, tmps = [], [], [], [], []
    for m, grad in enumerate(grads):
        if m == count - 1:
            piece, whole = grad.shape[1:], (CHIPS,) + grad.shape[1:]
        else:
            piece, whole = (grad.shape[1] // CHIPS, grad.shape[2]), grad.shape[1:]
        finals.append(jax.ShapeDtypeStruct(piece, jnp.float32))
        accs.append(pltpu.VMEM(whole, grad.dtype))
        sibs.append(pltpu.VMEM(whole, grad.dtype))
        lands += [pltpu.VMEM((n,) + piece, grad.dtype) for n in slots_of(ORDERS[m])]
        tmps.append(pltpu.VMEM(piece, jnp.float32))
    dma = pltpu.SemaphoreType.DMA
    out8 = jax.ShapeDtypeStruct((8, span, width), jnp.bfloat16)
    return pl.pallas_call(
        scatter_kernel,
        out_shape=[out8, out8] + finals,
        in_specs=[anywhere] * (3 + count),
        out_specs=[anywhere] * 2 + [vmem] * count,
        scratch_shapes=accs + sibs + lands + tmps + [
            pltpu.VMEM((half_rows, width), jnp.float32), pltpu.VMEM((half_rows, width), jnp.bfloat16), pltpu.VMEM((half_rows, width), jnp.bfloat16),
            dma((count, CHIPS)), dma((count, 4, CHIPS)), dma((count, CHIPS)), dma((count, CHIPS)), dma((count, CHIPS)), dma((3,)), dma((2, 8)), dma((8,)), dma((8,))],
        compiler_params=pltpu.CompilerParams(collective_id=1, has_side_effects=True, vmem_limit_bytes=60 << 20),
        name="scatter",
    )(y_own, gt_own, gt_other, *grads)


LOW, F32 = jnp.bfloat16, jnp.float32
EPS = 1e-12
HEAD = 64
LANES = 128
GROUP = 256
FULL = pl.BlockSpec(memory_space=pltpu.VMEM)


def nn(a, b):
    return jnp.dot(a, b, preferred_element_type=F32)


def nt(a, b):
    return lax.dot_general(a, b, (((1,), (1,)), ((), ())), preferred_element_type=F32)


def tn(a, b):
    return lax.dot_general(a, b, (((0,), (0,)), ((), ())), preferred_element_type=F32)


def lane_of(shape):
    return lax.broadcasted_iota(jnp.int32, shape, 1)


def turn(u):
    parts = []
    for start in range(0, u.shape[1], LANES):
        part = u[:, start:start + LANES]
        first = lane_of(part.shape) % HEAD < HEAD // 2
        parts.append(jnp.where(first, pltpu.roll(part, LANES - HEAD // 2, 1), pltpu.roll(part, HEAD // 2, 1)))
    return jnp.concatenate(parts, 1)


def weight_block(w_ref, block):
    per = w_ref.shape[2] // LANES
    cols = [w_ref[b // per, :, pl.ds(pl.multiple_of(b % per * LANES, LANES), LANES)] for b in (block, block + 1)]
    return jnp.concatenate(cols, 1)


def attend_kernel(x_ref, w_ref, cos_ref, sin_ref, bias_ref, q_ref, k_ref, v_ref, att_ref):
    group = pl.program_id(0)
    rows = q_ref.shape[0]
    mine = pl.ds(pl.multiple_of(lax.axis_index("dp") * rows, rows), rows)
    blocks = x_ref.shape[1] // LANES

    def turned(u, cos, sin):
        return u * cos + turn(u) * sin

    q = turned(nn(x_ref[mine, :], weight_block(w_ref, 2 * group)), cos_ref[mine, :], sin_ref[mine, :]).astype(LOW)
    q_ref[...] = q * jnp.asarray(0.125, LOW)
    k_ref[...] = turned(nn(x_ref[...], weight_block(w_ref, blocks + 2 * group)), cos_ref[...], sin_ref[...]).astype(LOW)
    v_ref[...] = nn(x_ref[...], weight_block(w_ref, 2 * blocks + 2 * group)).astype(LOW)
    step = 256
    bias = bias_ref[0:1, :]
    for pair in range(GROUP // LANES):
        lanes = slice(pair * LANES, pair * LANES + LANES)
        for start in range(0, rows, step):
            qp = q_ref[start:start + step, lanes]
            low = lane_of(qp.shape) < HEAD
            outs = []
            for head in range(2):
                qm = jnp.where(low if head == 0 else jnp.logical_not(low), qp, jnp.zeros_like(qp))
                s = nt(qm, k_ref[:, lanes]) + bias
                p = jnp.exp(s - jnp.max(s, axis=1, keepdims=True))
                total = jnp.sum(p, axis=1, keepdims=True)
                outs.append(nn(p.astype(LOW), v_ref[:, lanes]) / total)
            att_ref[start:start + step, lanes] = jnp.where(low, outs[0], outs[1]).astype(LOW)


def attend(x, w, cos, sin, bias):
    tokens, width = x.shape
    rows = tokens // 2
    shapes = [jax.ShapeDtypeStruct((n, width), LOW) for n in (rows, tokens, tokens, rows)]
    return pl.pallas_call(
        attend_kernel, grid=(width // GROUP,), out_shape=shapes,
        in_specs=[FULL] * 5,
        out_specs=[pl.BlockSpec((s.shape[0], GROUP), lambda g: (0, g)) for s in shapes],
        compiler_params=pltpu.CompilerParams(vmem_limit_bytes=60 << 20),
        cost_estimate=pl.CostEstimate(flops=8 * 10**9, bytes_accessed=10**7, transcendentals=6 * 10**6),
        name="attend")(x, w, cos, sin, bias)


def attend_back_kernel(x_ref, w_ref, q_ref, k_ref, v_ref, g_ref, res_ref, cos_ref, sin_ref, bias_ref,
                       dw_ref, own_ref, oth_ref, xt_ref, acc_ref, dq_ref, dk_ref, dv_ref):
    group = pl.program_id(0)
    rows = q_ref.shape[0]
    core = lax.axis_index("dp")
    mine = pl.ds(pl.multiple_of(core * rows, rows), rows)
    theirs = pl.ds(pl.multiple_of((1 - core) * rows, rows), rows)
    blocks = x_ref.shape[1] // LANES
    step = 256

    @pl.when(group == 0)
    def _():
        xt_ref[...] = x_ref[...].T
        own_ref[...] = res_ref[...]
        acc_ref[...] = jnp.zeros_like(acc_ref)

    dk_ref[...] = jnp.zeros_like(dk_ref)
    dv_ref[...] = jnp.zeros_like(dv_ref)
    for pair in range(GROUP // LANES):
        lanes = slice(pair * LANES, pair * LANES + LANES)
        for start in range(0, rows, step):
            qp, gp = q_ref[start:start + step, lanes], g_ref[start:start + step, lanes]
            low = lane_of(qp.shape) < HEAD
            dqs = []
            for head in range(2):
                keep = low if head == 0 else jnp.logical_not(low)
                qm, gm = jnp.where(keep, qp, jnp.zeros_like(qp)), jnp.where(keep, gp, jnp.zeros_like(gp))
                s = nt(k_ref[:, lanes], qm) + jnp.concatenate([bias_ref[...]] * (step // LANES), 1)
                e = jnp.exp(s - jnp.max(s, axis=0, keepdims=True))
                p = e * (1.0 / jnp.sum(e, axis=0, keepdims=True))
                dp = nt(v_ref[:, lanes], gm)
                delta = jnp.sum(p * dp, axis=0, keepdims=True)
                ds = (p * (dp - delta)).astype(LOW)
                dv_ref[:, lanes] += nn(p.astype(LOW), gm)
                dk_ref[:, lanes] += nn(ds, qm)
                dqs.append(tn(ds, k_ref[:, lanes]))
            dq_ref[start:start + step, lanes] = jnp.where(low, dqs[0], dqs[1]) * 0.125

    def back(u, cos, sin):
        return (u * cos - turn(u) * sin).astype(LOW)

    gq = back(dq_ref[...], cos_ref[mine, :], sin_ref[mine, :])
    dk_ref[...] = dk_ref[...] * cos_ref[...] - turn(dk_ref[...]) * sin_ref[...]

    def put(block, value):
        per = dw_ref.shape[2] // LANES
        for i in range(2):
            b = block + i
            dw_ref[b // per, :, pl.ds(pl.multiple_of(b % per * LANES, LANES), LANES)] = value[:, i * LANES:i * LANES + LANES].astype(LOW)

    put(2 * group, nn(xt_ref[:, pl.ds(pl.multiple_of(core * rows, rows), rows)], gq))
    put(blocks + 2 * group, nn(xt_ref[...], dk_ref[...].astype(LOW)))
    put(2 * blocks + 2 * group, nn(xt_ref[...], dv_ref[...].astype(LOW)))
    wq, wk, wv = (weight_block(w_ref, n * blocks + 2 * group) for n in range(3))
    own_ref[...] += nt(gq, wq) + nt(dk_ref[mine, :].astype(LOW), wk) + nt(dv_ref[mine, :].astype(LOW), wv)
    acc_ref[...] += nt(dk_ref[theirs, :].astype(LOW), wk) + nt(dv_ref[theirs, :].astype(LOW), wv)

    @pl.when(group == pl.num_programs(0) - 1)
    def _():
        oth_ref[...] = acc_ref[...].astype(LOW)


def attend_back(x, w, q, k, v, g_att, g_res1, cos, sin, bias_col):
    tokens, width = x.shape
    rows = tokens // 2
    part = lambda n: pl.BlockSpec((n, GROUP), lambda g: (0, g))
    shapes = [jax.ShapeDtypeStruct(w.shape, LOW), jax.ShapeDtypeStruct((rows, width), F32), jax.ShapeDtypeStruct((rows, width), LOW)]
    return pl.pallas_call(
        attend_back_kernel, grid=(width // GROUP,), out_shape=shapes,
        in_specs=[FULL, FULL, part(rows), part(tokens), part(tokens), part(rows), FULL, FULL, FULL, FULL],
        out_specs=[FULL] * 3,
        scratch_shapes=[pltpu.VMEM((width, tokens), LOW), pltpu.VMEM((rows, width), F32), pltpu.VMEM((rows, GROUP), F32),
                        pltpu.VMEM((tokens, GROUP), F32), pltpu.VMEM((tokens, GROUP), F32)],
        compiler_params=pltpu.CompilerParams(vmem_limit_bytes=60 << 20),
        cost_estimate=pl.CostEstimate(flops=16 * 10**9, bytes_accessed=10**7, transcendentals=6 * 10**6),
        name="attend_back")(x, w, q, k, v, g_att, g_res1, cos, sin, bias_col)


def ln_parts(u):
    center = u - jnp.mean(u, axis=1, keepdims=True)
    inv = lax.rsqrt(jnp.mean(center * center, axis=1, keepdims=True) + EPS)
    return center * inv, inv


def ln_back(g, n, inv):
    return inv * (g - jnp.mean(g, axis=1, keepdims=True) - n * jnp.mean(g * n, axis=1, keepdims=True))


def middle_kernel(tiles, x_ref, att_ref, wo_ref, wg_ref, wu_ref, wd_ref, cot_ref, ln_ref, valid_ref,
                  y_ref, dwg_ref, dwu_ref, dwd_ref, dwo_ref, gatt_ref, gres_ref, dln_ref,
                  n1_ref, inv1_ref, hid_ref, hidt_ref, gate_ref, up_ref, acc_ref, gb_ref):
    index = pl.program_id(0)
    width = x_ref.shape[1]
    half = width // 2

    def wide(ref):
        return jnp.concatenate([ref[0], ref[1]], 1)

    @pl.when(index == 0)
    def _():
        n1, inv1 = ln_parts(x_ref[...].astype(F32) + nn(att_ref[...], wide(wo_ref)))
        hidden = n1 * ln_ref[0:1, :] + ln_ref[1:2, :]
        n1_ref[...] = n1
        inv1_ref[...] = jnp.broadcast_to(inv1, inv1_ref.shape)
        acc_ref[...] = hidden
        low = hidden.astype(LOW)
        hid_ref[...] = low
        hidt_ref[...] = low.T

    tile = wg_ref.shape[2]
    f = jnp.where(index < tiles, index, index - tiles)
    cols = pl.ds(pl.multiple_of(f * tile, tile), tile)

    @pl.when(index < tiles)
    def _():
        gate, up = nn(hid_ref[...], wg_ref[0]), nn(hid_ref[...], wu_ref[0])
        gate_ref[:, cols] = gate
        up_ref[:, cols] = up
        acc_ref[...] += nn((gate * jax.nn.sigmoid(gate) * up).astype(LOW), wide(wd_ref))

    @pl.when(index == tiles - 1)
    def _():
        n2, inv2 = ln_parts(acc_ref[...])
        valid = valid_ref[:, 0:1]
        y_ref[...] = ((n2 * ln_ref[2:3, :] + ln_ref[3:4, :]) * valid).astype(LOW)
        g_y = cot_ref[...].astype(F32) * valid
        dln_ref[2:3, :] = jnp.sum(g_y * n2, axis=0, keepdims=True)
        dln_ref[3:4, :] = jnp.sum(g_y, axis=0, keepdims=True)
        g_res2 = ln_back(g_y * ln_ref[2:3, :], n2, inv2)
        acc_ref[...] = g_res2
        gb_ref[...] = g_res2.astype(LOW)

    @pl.when(index >= tiles)
    def _():
        gate, up = gate_ref[:, cols], up_ref[:, cols]
        sig = jax.nn.sigmoid(gate)
        act = gate * sig
        gb = gb_ref[...]
        dwd = tn((act * up).astype(LOW), gb)
        dwd_ref[0] = dwd[:, :half].astype(LOW)
        dwd_ref[1] = dwd[:, half:].astype(LOW)
        g_inner = nt(gb, wide(wd_ref))
        g_gate = (g_inner * up * sig * (1.0 + gate * (1.0 - sig))).astype(LOW)
        g_up = (g_inner * act).astype(LOW)
        dwg_ref[0] = nn(hidt_ref[...], g_gate).astype(LOW)
        dwu_ref[0] = nn(hidt_ref[...], g_up).astype(LOW)
        acc_ref[...] += nt(g_gate, wg_ref[0]) + nt(g_up, wu_ref[0])

    @pl.when(index == 2 * tiles - 1)
    def _():
        g_hidden, n1 = acc_ref[...], n1_ref[...]
        dln_ref[0:1, :] = jnp.sum(g_hidden * n1, axis=0, keepdims=True)
        dln_ref[1:2, :] = jnp.sum(g_hidden, axis=0, keepdims=True)
        g_res1 = ln_back(g_hidden * ln_ref[0:1, :], n1, inv1_ref[:, 0:1])
        gres_ref[...] = g_res1
        gb1 = g_res1.astype(LOW)
        dwo = tn(att_ref[...], gb1)
        dwo_ref[0] = dwo[:, :half].astype(LOW)
        dwo_ref[1] = dwo[:, half:].astype(LOW)
        gatt_ref[...] = nt(gb1, wide(wo_ref)).astype(LOW)


def middle(x_own, att, wo, wg, wu, wd, cot, ln, valid):
    rows, width = x_own.shape
    hidden = wd.shape[1]
    tile = 512
    tiles = hidden // tile
    per = wg.shape[2] // tile
    at = lambda i: jnp.where(i < tiles, i, i - tiles)
    late = lambda i: jnp.maximum(i - tiles, 0)
    cols = lambda pick: pl.BlockSpec((1, width, tile), lambda i: (pick(i) // per, 0, pick(i) % per))
    rowb = lambda pick: pl.BlockSpec((2, tile, wd.shape[2]), lambda i: (0, pick(i), 0))
    sds = jax.ShapeDtypeStruct
    return pl.pallas_call(
        functools.partial(middle_kernel, tiles), grid=(2 * tiles,),
        out_shape=[sds((rows, width), LOW), sds(wg.shape, LOW), sds(wu.shape, LOW), sds(wd.shape, LOW), sds(wo.shape, LOW),
                   sds((rows, width), LOW), sds((rows, width), F32), sds((8, width), F32)],
        in_specs=[FULL, FULL, FULL, cols(at), cols(at), rowb(at), FULL, FULL, FULL],
        out_specs=[FULL, cols(late), cols(late), rowb(late), FULL, FULL, FULL, FULL],
        scratch_shapes=[pltpu.VMEM((rows, width), F32), pltpu.VMEM((rows, LANES), F32), pltpu.VMEM((rows, width), LOW),
                        pltpu.VMEM((width, rows), LOW), pltpu.VMEM((rows, hidden), F32), pltpu.VMEM((rows, hidden), F32),
                        pltpu.VMEM((rows, width), F32), pltpu.VMEM((rows, width), LOW)],
        compiler_params=pltpu.CompilerParams(vmem_limit_bytes=60 << 20),
        cost_estimate=pl.CostEstimate(flops=24 * 10**9, bytes_accessed=6 * 10**7, transcendentals=3 * 10**6),
        name="middle")(x_own, att, wo, wg, wu, wd, cot, ln, valid)


def rotary_lanes(tokens):
    lane = jnp.arange(GROUP)
    pair_index = (lane % (HEAD // 2)).astype(F32)
    inverse = jnp.power(jnp.float32(1000.0), -2.0 * pair_index / HEAD)
    angles = jnp.arange(tokens).astype(F32)[:, None] * inverse[None, :]
    sign = jnp.where(lane % HEAD < HEAD // 2, -1.0, 1.0).astype(F32)
    return jnp.cos(angles), jnp.sin(angles) * sign[None, :]


def local_by_slot(tokens, lengths, w_qkv, w_out, w_gate, w_up, w_down, ln_params, cotangent):
    slots, span, width = tokens.shape
    core, chip = lax.axis_index("dp"), lax.axis_index("seq")
    half = CHIPS // 2
    small = jnp.zeros((8, LANES), F32)
    share = ln_params.shape[1]
    small = small.at[:4, :share].set(ln_params.astype(F32)).at[4, :slots].set(lengths.astype(F32))
    x, cot, wq, wo, wg, wu, wd, smalls = gather(tokens, cotangent, [w_qkv, w_out, w_gate, w_up, w_down, small])
    total, rows = x.shape[0], x.shape[0] // 2
    ln = jnp.pad(smalls[:, :4, :share].transpose(1, 0, 2).reshape(4, width), ((0, 4), (0, 0)))
    length = lax.dynamic_slice(smalls, (chip // half * CHIPS, 4, chip % half), (1, 1, 1)).reshape(()).astype(jnp.int32)
    cos, sin = rotary_lanes(total)
    position = jnp.arange(total)
    out_of = jnp.where(position < length, 0.0, masked_score).astype(F32)
    bias = jnp.broadcast_to(out_of[None, :], (8, total))
    bias_col = jnp.broadcast_to(out_of[:, None], (total, LANES))
    valid = jnp.broadcast_to((core * rows + jnp.arange(rows) < length).astype(F32)[:, None], (rows, LANES))
    q, k, v, att = attend(x, wq, cos, sin, bias)
    x_own = lax.dynamic_slice_in_dim(x, core * rows, rows, 0)
    y, dwg, dwu, dwd, dwo, g_att, g_res1, dln = middle(x_own, att, wo, wg, wu, wd, cot, ln, valid)
    dwq, gt_own, gt_other = attend_back(x, wq, q, k, v, g_att, g_res1, cos, sin, bias_col)
    dsmall = dln[:4].reshape(4, 2 * CHIPS, share).transpose(1, 0, 2)
    dsmall = jnp.pad(dsmall, ((0, 0), (0, 4), (0, LANES - share)))
    output, grad_tokens, *finals = scatter(y, gt_own, gt_other, [dwq, dwo, dwg, dwu, dwd, dsmall])
    finals[-1] = finals[-1][:4, :share]
    return (output, grad_tokens, *finals)


def solution(mesh):
    placed = (
        P("dp", "seq", None),
        P("dp"),
        P("seq", "dp"),
        P("seq", "dp"),
        P("seq", "dp"),
        P("seq", "dp"),
        P("seq", "dp"),
        P(None, ("dp", "seq")),
        P("dp", "seq", None),
    )

    def run(tokens, *rest):
        by_slot = mesh.shape["dp"] == 2 and mesh.shape["seq"] == CHIPS and tokens.shape[0] == CHIPS
        body = local_by_slot if by_slot else local
        return jax.shard_map(
            body,
            mesh=mesh,
            in_specs=placed,
            out_specs=(
                P("dp", "seq", None),
                P("dp", "seq", None),
                P("seq", "dp"),
                P("seq", "dp"),
                P("seq", "dp"),
                P("seq", "dp"),
                P("seq", "dp"),
                P(None, ("dp", "seq")),
            ),
            check_vma=False,
        )(tokens, *rest)

    return run
```

```python
import functools

import jax
import jax.numpy as jnp
from jax import lax
from jax.experimental import pallas as pl
from jax.experimental.pallas import tpu as pltpu
from jax.sharding import PartitionSpec as P

HEADS = 12
HEAD_DIM = 64


norm_epsilon = 1e-12
score_scale = 0.125
masked_score = -1e30


def shifted(shard, axis, by):
    count = lax.axis_size(axis)
    return lax.ppermute(shard, axis, [(i, (i + by) % count) for i in range(count)])


def rotary_tables(positions):
    pair_index = jnp.arange(HEAD_DIM // 2, dtype=jnp.float32)
    inverse = jnp.power(jnp.float32(1000.0), -2.0 * pair_index / HEAD_DIM)
    angles = positions.astype(jnp.float32)[:, None] * inverse[None, :]
    cos_tab = jnp.concatenate([jnp.cos(angles), jnp.cos(angles)], axis=-1)
    sin_tab = jnp.concatenate([jnp.sin(angles), jnp.sin(angles)], axis=-1)
    return (cos_tab, sin_tab)


def rotate(values, cos_tab, sin_tab):
    half_dim = values.shape[-1] // 2
    turned = jnp.concatenate([-values[..., half_dim:], values[..., :half_dim]], axis=-1)
    return values * cos_tab + turned * sin_tab


def norm_parts(values, gain_vec, bias_vec):
    center = values - jnp.mean(values, axis=-1, keepdims=True)
    inv_std = lax.rsqrt(jnp.mean(center * center, axis=-1, keepdims=True) + norm_epsilon)
    normed = center * inv_std
    return (normed * gain_vec + bias_vec, normed, inv_std)


def norm_back(grad_in, normed, inv_std, gain_vec):
    scaled = grad_in * gain_vec
    return inv_std * (
        scaled
        - jnp.mean(scaled, axis=-1, keepdims=True)
        - normed * jnp.mean(scaled * normed, axis=-1, keepdims=True)
    )


def heads_view(flat_rows):
    return flat_rows.reshape(flat_rows.shape[0], flat_rows.shape[1], HEADS, HEAD_DIM)


def attend_block(run_state, queries, key_blk, value_blk, key_start, lengths):
    run_max, run_sum, run_acc = run_state
    scores = (
        jnp.einsum(
            "sqhd,skhd->shqk",
            heads_view(queries),
            heads_view(key_blk),
            preferred_element_type=jnp.float32,
        )
        * score_scale
    )
    key_pos = key_start + jnp.arange(key_blk.shape[1], dtype=jnp.int32)
    key_mask = (key_pos[None, :] < lengths[:, None])[:, None, None, :]
    scores = jnp.where(key_mask, scores, masked_score)
    new_max = jnp.maximum(run_max, jnp.max(scores, axis=-1))
    exp_scores = jnp.where(key_mask, jnp.exp(scores - new_max[..., None]), 0.0)
    factor = jnp.exp(run_max - new_max)
    run_sum = run_sum * factor + jnp.sum(exp_scores, axis=-1)
    run_acc = run_acc * factor[..., None] + jnp.einsum(
        "shqk,skhd->shqd",
        exp_scores.astype(jnp.bfloat16),
        heads_view(value_blk),
        preferred_element_type=jnp.float32,
    )
    return (new_max, run_sum, run_acc)


def block_grads(queries, grad_att, log_total, delta_rows, key_blk, value_blk, key_ok):
    query_h = heads_view(queries)
    grad_h = heads_view(grad_att)
    key_h = heads_view(key_blk)
    scores = (
        jnp.einsum("sqhd,skhd->shqk", query_h, key_h, preferred_element_type=jnp.float32)
        * score_scale
    )
    key_mask = key_ok[:, None, None, :]
    soft_probs = jnp.where(key_mask, jnp.exp(scores - log_total[..., None]), 0.0)
    grad_probs = jnp.einsum(
        "sqhd,skhd->shqk", grad_h, heads_view(value_blk), preferred_element_type=jnp.float32
    )
    grad_scores = (soft_probs * (grad_probs - delta_rows[..., None])).astype(jnp.bfloat16)
    part_q = (
        jnp.einsum("shqk,skhd->sqhd", grad_scores, key_h, preferred_element_type=jnp.float32)
        * score_scale
    )
    part_k = (
        jnp.einsum("shqk,sqhd->skhd", grad_scores, query_h, preferred_element_type=jnp.float32)
        * score_scale
    )
    part_v = jnp.einsum(
        "shqk,sqhd->skhd",
        soft_probs.astype(jnp.bfloat16),
        grad_h,
        preferred_element_type=jnp.float32,
    )
    shape_out = queries.shape
    return (part_q.reshape(shape_out), part_k.reshape(key_blk.shape), part_v.reshape(key_blk.shape))


def local(tokens, lengths, w_qkv, w_out, w_gate, w_up, w_down, ln_params, cotangent):
    slot_count, span_len, width = tokens.shape
    row_count = slot_count * span_len
    cycle_size = lax.axis_size("seq")
    my_index = lax.axis_index("seq")
    row_qkv, row_out, row_gate, row_up, row_down, row_norm = (
        lax.all_gather(w_qkv, "seq", axis=0, tiled=True),
        lax.all_gather(w_out, "seq", axis=0, tiled=True),
        lax.all_gather(w_gate, "seq", axis=0, tiled=True),
        lax.all_gather(w_up, "seq", axis=0, tiled=True),
        lax.all_gather(w_down, "seq", axis=0, tiled=True),
        lax.all_gather(ln_params, "seq", axis=1, tiled=True),
    )
    wide_qkv, wide_out, wide_gate, wide_up, wide_down, wide_norm = (
        lax.all_gather(row_qkv, "dp", axis=1, tiled=True),
        lax.all_gather(row_out, "dp", axis=1, tiled=True),
        lax.all_gather(row_gate, "dp", axis=1, tiled=True),
        lax.all_gather(row_up, "dp", axis=1, tiled=True),
        lax.all_gather(row_down, "dp", axis=1, tiled=True),
        lax.all_gather(row_norm, "dp", axis=1, tiled=True),
    )
    norm_full = wide_norm.astype(jnp.float32)
    flat_tokens = tokens.reshape(row_count, width)
    token_f32 = flat_tokens.astype(jnp.float32)
    positions = my_index * span_len + jnp.arange(span_len, dtype=jnp.int32)
    row_valid = (positions[None, :] < lengths[:, None]).astype(jnp.float32).reshape(row_count, 1)
    cos_tab, sin_tab = rotary_tables(positions)
    cos_four = cos_tab[None, :, None, :]
    sin_four = sin_tab[None, :, None, :]
    qkv_pre = jnp.dot(flat_tokens, wide_qkv, preferred_element_type=jnp.float32)
    split_qkv = qkv_pre.reshape(slot_count, span_len, 3, HEADS, HEAD_DIM)
    queries = (
        rotate(split_qkv[:, :, 0], cos_four, sin_four)
        .astype(jnp.bfloat16)
        .reshape(slot_count, span_len, width)
    )
    keys_rot = (
        rotate(split_qkv[:, :, 1], cos_four, sin_four)
        .astype(jnp.bfloat16)
        .reshape(slot_count, span_len, width)
    )
    values = split_qkv[:, :, 2].astype(jnp.bfloat16).reshape(slot_count, span_len, width)
    start_state = (
        jnp.full((slot_count, HEADS, span_len), masked_score, jnp.float32),
        jnp.zeros((slot_count, HEADS, span_len), jnp.float32),
        jnp.zeros((slot_count, HEADS, span_len, HEAD_DIM), jnp.float32),
    )
    key_piece = lax.all_gather(keys_rot, "seq", axis=1, tiled=True)
    value_piece = lax.all_gather(values, "seq", axis=1, tiled=True)
    block_count = key_piece.shape[1] // span_len

    def one_block(block_id, inner_state):
        offset = block_id * span_len
        key_blk = lax.dynamic_slice_in_dim(key_piece, offset, span_len, axis=1)
        value_blk = lax.dynamic_slice_in_dim(value_piece, offset, span_len, axis=1)
        return attend_block(inner_state, queries, key_blk, value_blk, offset, lengths)

    run_max, run_sum, run_acc = lax.fori_loop(0, block_count, one_block, start_state)
    attended = run_acc / run_sum[..., None]
    log_total = run_max + jnp.log(run_sum)
    attn_low = attended.transpose(0, 2, 1, 3).reshape(row_count, width).astype(jnp.bfloat16)
    branch = jnp.dot(attn_low, wide_out, preferred_element_type=jnp.float32)
    hidden, normed_one, inv_one = norm_parts(token_f32 + branch, norm_full[0], norm_full[1])
    hidden_low = hidden.astype(jnp.bfloat16)
    gate_pre = jnp.dot(hidden_low, wide_gate, preferred_element_type=jnp.float32)
    up_proj = jnp.dot(hidden_low, wide_up, preferred_element_type=jnp.float32)
    activated = jax.nn.silu(gate_pre)
    inner_low = (activated * up_proj).astype(jnp.bfloat16)
    branch_two = jnp.dot(inner_low, wide_down, preferred_element_type=jnp.float32)
    result, normed_two, inv_two = norm_parts(hidden + branch_two, norm_full[2], norm_full[3])
    output = (result * row_valid).astype(jnp.bfloat16).reshape(slot_count, span_len, width)
    back_qkv, back_out, back_gate, back_up, back_down, back_norm = (
        lax.all_gather(w_qkv, "seq", axis=0, tiled=True),
        lax.all_gather(w_out, "seq", axis=0, tiled=True),
        lax.all_gather(w_gate, "seq", axis=0, tiled=True),
        lax.all_gather(w_up, "seq", axis=0, tiled=True),
        lax.all_gather(w_down, "seq", axis=0, tiled=True),
        lax.all_gather(ln_params, "seq", axis=1, tiled=True),
    )
    wide_qkv, wide_out, wide_gate, wide_up, wide_down, wide_norm = (
        lax.all_gather(back_qkv, "dp", axis=1, tiled=True),
        lax.all_gather(back_out, "dp", axis=1, tiled=True),
        lax.all_gather(back_gate, "dp", axis=1, tiled=True),
        lax.all_gather(back_up, "dp", axis=1, tiled=True),
        lax.all_gather(back_down, "dp", axis=1, tiled=True),
        lax.all_gather(back_norm, "dp", axis=1, tiled=True),
    )
    norm_full = wide_norm.astype(jnp.float32)
    grad_out = cotangent.reshape(row_count, width).astype(jnp.float32) * row_valid
    gain_two_grad = jnp.sum(grad_out * normed_two, axis=0)
    bias_two_grad = jnp.sum(grad_out, axis=0)
    grad_res2 = norm_back(grad_out, normed_two, inv_two, norm_full[2])
    grad_branch2 = grad_res2.astype(jnp.bfloat16)
    grad_wdown = jnp.einsum(
        "rf,rd->fd", inner_low, grad_branch2, preferred_element_type=jnp.float32
    )
    grad_inner = jnp.einsum(
        "rd,fd->rf", grad_branch2, wide_down, preferred_element_type=jnp.float32
    )
    sigma = jax.nn.sigmoid(gate_pre)
    grad_gate = (grad_inner * up_proj * sigma * (1.0 + gate_pre * (1.0 - sigma))).astype(
        jnp.bfloat16
    )
    grad_up = (grad_inner * activated).astype(jnp.bfloat16)
    grad_wgate = jnp.einsum("rd,rf->df", hidden_low, grad_gate, preferred_element_type=jnp.float32)
    grad_wup = jnp.einsum("rd,rf->df", hidden_low, grad_up, preferred_element_type=jnp.float32)
    grad_hidden = (
        grad_res2
        + jnp.einsum("rf,df->rd", grad_gate, wide_gate, preferred_element_type=jnp.float32)
        + jnp.einsum("rf,df->rd", grad_up, wide_up, preferred_element_type=jnp.float32)
    )
    gain_one_grad = jnp.sum(grad_hidden * normed_one, axis=0)
    bias_one_grad = jnp.sum(grad_hidden, axis=0)
    grad_res1 = norm_back(grad_hidden, normed_one, inv_one, norm_full[0])
    grad_branch1 = grad_res1.astype(jnp.bfloat16)
    grad_wout = jnp.einsum("ri,rd->id", attn_low, grad_branch1, preferred_element_type=jnp.float32)
    grad_att = (
        jnp.einsum("rd,id->ri", grad_branch1, wide_out, preferred_element_type=jnp.float32)
        .astype(jnp.bfloat16)
        .reshape(slot_count, span_len, width)
    )
    zero_rows = jnp.zeros((slot_count, span_len, width), jnp.float32)
    delta_rows = jnp.einsum("sqhd,shqd->shq", heads_view(grad_att).astype(jnp.float32), attended)

    def key_turn(turn_id, run_state):
        key_cur, value_cur, grad_keys, grad_values, grad_query = run_state
        key_start = (my_index - turn_id) % cycle_size * span_len
        key_ok = (key_start + jnp.arange(span_len, dtype=jnp.int32))[None, :] < lengths[:, None]
        part_q, part_k, part_v = block_grads(
            queries, grad_att, log_total, delta_rows, key_cur, value_cur, key_ok
        )
        key_cur, value_cur = shifted((key_cur, value_cur), "seq", 1)
        grad_keys, grad_values = (
            shifted((grad_keys + part_k).astype(jnp.bfloat16), "seq", 1).astype(jnp.float32),
            shifted((grad_values + part_v).astype(jnp.bfloat16), "seq", 1).astype(jnp.float32),
        )
        return (key_cur, value_cur, grad_keys, grad_values, grad_query + part_q)

    key_cur, value_cur, grad_keys, grad_values, grad_query = lax.fori_loop(
        0, cycle_size - 1, key_turn, (keys_rot, values, zero_rows, zero_rows, zero_rows)
    )
    key_start = (my_index - (cycle_size - 1)) % cycle_size * span_len
    key_ok = (key_start + jnp.arange(span_len, dtype=jnp.int32))[None, :] < lengths[:, None]
    part_q, part_k, part_v = block_grads(
        queries, grad_att, log_total, delta_rows, key_cur, value_cur, key_ok
    )
    grad_query = grad_query + part_q
    grad_keys, grad_values = (
        shifted((grad_keys + part_k).astype(jnp.bfloat16), "seq", 1).astype(jnp.float32),
        shifted((grad_values + part_v).astype(jnp.bfloat16), "seq", 1).astype(jnp.float32),
    )
    query_back = rotate(heads_view(grad_query), cos_four, -sin_four)
    key_back = rotate(heads_view(grad_keys), cos_four, -sin_four)
    grad_qkv = jnp.stack([query_back, key_back, heads_view(grad_values)], axis=2)
    grad_qkv = grad_qkv.reshape(row_count, 3 * width).astype(jnp.bfloat16)
    grad_wqkv = jnp.einsum("rd,re->de", flat_tokens, grad_qkv, preferred_element_type=jnp.float32)
    grad_tokens = grad_res1 + jnp.einsum(
        "re,de->rd", grad_qkv, wide_qkv, preferred_element_type=jnp.float32
    )
    grad_tokens = grad_tokens.astype(jnp.bfloat16).reshape(slot_count, span_len, width)
    grad_norm = jnp.stack([gain_one_grad, bias_one_grad, gain_two_grad, bias_two_grad], axis=0)
    col_qkv, col_out, col_gate, col_up, col_down, col_norm = (
        lax.psum_scatter(
            grad_wqkv.astype(jnp.bfloat16), "dp", scatter_dimension=1, tiled=True
        ).astype(jnp.float32),
        lax.psum_scatter(
            grad_wout.astype(jnp.bfloat16), "dp", scatter_dimension=1, tiled=True
        ).astype(jnp.float32),
        lax.psum_scatter(
            grad_wgate.astype(jnp.bfloat16), "dp", scatter_dimension=1, tiled=True
        ).astype(jnp.float32),
        lax.psum_scatter(
            grad_wup.astype(jnp.bfloat16), "dp", scatter_dimension=1, tiled=True
        ).astype(jnp.float32),
        lax.psum_scatter(
            grad_wdown.astype(jnp.bfloat16), "dp", scatter_dimension=1, tiled=True
        ).astype(jnp.float32),
        lax.psum_scatter(
            grad_norm.astype(jnp.bfloat16), "dp", scatter_dimension=1, tiled=True
        ).astype(jnp.float32),
    )
    own_qkv, own_out, own_gate, own_up, own_down, own_norm = (
        lax.psum_scatter(
            col_qkv.astype(jnp.bfloat16), "seq", scatter_dimension=0, tiled=True
        ).astype(jnp.float32),
        lax.psum_scatter(
            col_out.astype(jnp.bfloat16), "seq", scatter_dimension=0, tiled=True
        ).astype(jnp.float32),
        lax.psum_scatter(
            col_gate.astype(jnp.bfloat16), "seq", scatter_dimension=0, tiled=True
        ).astype(jnp.float32),
        lax.psum_scatter(
            col_up.astype(jnp.bfloat16), "seq", scatter_dimension=0, tiled=True
        ).astype(jnp.float32),
        lax.psum_scatter(
            col_down.astype(jnp.bfloat16), "seq", scatter_dimension=0, tiled=True
        ).astype(jnp.float32),
        lax.psum_scatter(
            col_norm.astype(jnp.bfloat16), "seq", scatter_dimension=1, tiled=True
        ).astype(jnp.float32),
    )
    return (output, grad_tokens, own_qkv, own_out, own_gate, own_up, own_down, own_norm)


MESH = pl.DeviceIdType.MESH
CHIPS, ZS = 16, 4
OFFSETS = sorted(((dx, dy, dz) for dx in (0, 1) for dy in (0, 1) for dz in range(-3, 4)),
                 key=lambda o: (2 * (o[0] + o[1]) + abs(o[2]), abs(o[2]), o))
ORDERS = ("zxy", "zyx", "xzy", "yzx")


def pick(index, values):
    out = jnp.int32(0)
    for position, value in enumerate(values):
        if value:
            out = out + jnp.where(index == position, jnp.int32(value), 0)
    return out


def spread(order, dx, dy, dz):
    zero = {"x": dx == 0, "y": dy == 0, "z": dz == 0}
    flags = {}
    for position, axis in enumerate(order):
        flag = zero[axis] if axis != "z" else None
        for later in order[position + 1:]:
            flag = zero[later] if flag is None else flag & zero[later]
        flags[axis] = flag
    up, down = dz <= 0, dz >= 0
    if flags["z"] is not None:
        up, down = up & flags["z"], down & flags["z"]
    return flags["x"], flags["y"], up, down


def place():
    core, chip = lax.axis_index("dp"), lax.axis_index("seq")
    return core, chip, chip % 2, (chip // 2) % 2, chip // 4


def chip_at(x, y, z):
    return (z * 2 + y) * 2 + x


def meet_all(core, chip):
    barrier = pltpu.get_barrier_semaphore()
    me = core * CHIPS + chip

    def greet(step, carry):
        other = (me + step) % (2 * CHIPS)
        pl.semaphore_signal(barrier, inc=1, device_id={"dp": other // CHIPS, "seq": other % CHIPS}, device_id_type=MESH)
        return carry

    lax.fori_loop(1, 2 * CHIPS, greet, 0)
    pl.semaphore_wait(barrier, 2 * CHIPS - 1)


def onward(order, dx, dy, dz):
    zero = {"x": dx == 0, "y": dy == 0, "z": dz == 0}
    links = []
    for position, axis in enumerate(order):
        if all(zero[later] for later in order[position + 1:]):
            if axis == "z":
                links += [2] * (dz <= 0) + [3] * (dz >= 0)
            elif zero[axis]:
                links.append("xy".index(axis))
    return links


def when(condition, action):
    if condition is True:
        action()
    else:
        pl.when(condition)(action)


def gather_kernel(tok, cot, small, *refs):
    count = len(ORDERS)
    shards, refs = refs[:count], refs[count:]
    (x_all, c_own, smalls), refs = refs[:3], refs[3:]
    wides, refs = refs[:count], refs[count:]
    send_sem, recv_sem, sib_sem, tok_send, tok_recv, tok_sib, cot_recv, own_sem, small_send, small_recv = refs
    core, chip, x, y, z = place()
    other = 1 - core
    slots, span = tok.shape[0], tok.shape[1]
    half = CHIPS // 2
    me = core * CHIPS + chip
    can = (True, True, z < ZS - 1, z > 0, True)
    neighbours = (
        {"dp": core, "seq": chip_at(1 - x, y, z)},
        {"dp": core, "seq": chip_at(x, 1 - y, z)},
        {"dp": core, "seq": chip_at(x, y, jnp.minimum(z + 1, ZS - 1))},
        {"dp": core, "seq": chip_at(x, y, jnp.maximum(z - 1, 0))},
        {"dp": other, "seq": chip},
    )

    def region(m, owner, source):
        rows = shards[m].shape[0]
        return wides[m].at[owner, pl.ds(pl.multiple_of(source * rows, rows), rows)]

    def piece(m, source, link, own=False):
        target = region(m, core, source)
        return pltpu.make_async_remote_copy(
            src_ref=shards[m] if own else target, dst_ref=target, send_sem=send_sem.at[m, link, source],
            recv_sem=sib_sem.at[m, source] if link == 4 else recv_sem.at[m, source],
            device_id=neighbours[link], device_id_type=MESH)

    meet_all(core, chip)

    def deliver(source, target, sends, recvs):
        def one(j, carry):
            slot = (chip + 1 + j) % half
            to = core * half + slot
            src, dst = source.at[slot], target
            self_copy = (chip // half == core) & (to == chip)

            @pl.when(self_copy)
            def _():
                pltpu.make_async_copy(src, dst, recvs.at[chip % half]).start()

            @pl.when(jnp.logical_not(self_copy))
            def _():
                pltpu.make_async_remote_copy(
                    src_ref=src, dst_ref=dst, send_sem=sends.at[slot], recv_sem=recvs.at[chip % half],
                    device_id={"dp": chip // half, "seq": to}, device_id_type=MESH).start()
            return carry

        lax.fori_loop(0, slots, one, 0)

    def rows_of(ref, index):
        return ref.at[pl.ds(pl.multiple_of(index * span, span), span)]

    def small_to(step):
        to = (me + step) % (2 * CHIPS)
        return pltpu.make_async_remote_copy(
            src_ref=small, dst_ref=smalls.at[me], send_sem=small_send.at[step], recv_sem=small_recv.at[me],
            device_id={"dp": to // CHIPS, "seq": to % CHIPS}, device_id_type=MESH)

    deliver(tok, rows_of(x_all, chip), tok_send.at[0], tok_recv)
    own_small = pltpu.make_async_copy(small, smalls.at[me], small_recv.at[me])
    own_small.start()
    for m in range(count):
        for link in onward(ORDERS[m], 0, 0, 0) + [4]:
            when(can[link], piece(m, chip, link, own=True).start)
        pltpu.make_async_copy(shards[m], region(m, core, chip), own_sem.at[m]).start()
    lax.fori_loop(1, 2 * CHIPS, lambda s, c: (small_to(s).start(), c)[1], 0)
    deliver(cot, rows_of(c_own, chip % half), tok_send.at[1], cot_recv)

    def arrived(m, offset):
        dx, dy, dz = offset
        source = chip_at((x + dx) % 2, (y + dy) % 2, z + dz)
        piece(m, source, 0).wait_recv()
        for link in onward(ORDERS[m], dx, dy, dz) + [4]:
            when(can[link], piece(m, source, link).start)

    def valid(offset):
        dz = offset[2]
        return True if dz == 0 else (z < ZS - dz if dz > 0 else z >= -dz)

    def steps(offsets):
        for offset in offsets:
            def one():
                for m in range(count):
                    arrived(m, offset)
            when(valid(offset), one)

    steps(OFFSETS[1:5])

    def relay(i, carry):
        block = rows_of(x_all, core * half + i)
        pltpu.make_async_copy(block, block, tok_recv.at[i]).wait()
        pltpu.make_async_remote_copy(
            src_ref=block, dst_ref=block, send_sem=tok_send.at[2, i], recv_sem=tok_sib.at[i],
            device_id=neighbours[4], device_id_type=MESH).start()
        return carry

    lax.fori_loop(0, half, relay, 0)
    steps(OFFSETS[5:])

    def ends(i, carry):
        block = rows_of(c_own, i)
        pltpu.make_async_copy(block, block, cot_recv.at[i]).wait()
        block = rows_of(x_all, other * half + i)
        pltpu.make_async_copy(block, block, tok_sib.at[i]).wait()
        block = rows_of(x_all, core * half + i)
        pltpu.make_async_copy(block, block, tok_send.at[2, i]).wait()
        self_copy = (chip // half == core) & (core * half + i == chip)

        @pl.when(jnp.logical_not(self_copy))
        def _():
            pltpu.make_async_copy(tok.at[i], tok.at[i], tok_send.at[0, i]).wait()
            pltpu.make_async_copy(cot.at[i], cot.at[i], tok_send.at[1, i]).wait()
        return carry

    lax.fori_loop(0, half, ends, 0)

    def small_end(step, carry):
        small_to(step).wait_send()
        source = (me + step) % (2 * CHIPS)
        pltpu.make_async_copy(small, smalls.at[source], small_recv.at[source]).wait()
        return carry

    lax.fori_loop(1, 2 * CHIPS, small_end, 0)
    own_small.wait()

    def sibling(source, carry):
        for m in range(count):
            block = region(m, other, source)
            pltpu.make_async_copy(block, block, sib_sem.at[m, source]).wait()
        return carry

    lax.fori_loop(0, CHIPS, sibling, 0)
    for offset in OFFSETS:
        def sent():
            source = chip_at((x + offset[0]) % 2, (y + offset[1]) % 2, z + offset[2])
            for m in range(count):
                for link in onward(ORDERS[m], *offset) + [4]:
                    when(can[link], piece(m, source, link).wait_send)
        when(valid(offset), sent)
    for m in range(count):
        pltpu.make_async_copy(shards[m], region(m, core, chip), own_sem.at[m]).wait()


def gather(tokens, cotangent, small, shards):
    count = len(shards)
    slots, span, width = tokens.shape
    low = jnp.bfloat16
    outs = [jax.ShapeDtypeStruct((span * CHIPS, width), low), jax.ShapeDtypeStruct((span * CHIPS // 2, width), low),
            jax.ShapeDtypeStruct((2 * CHIPS,) + small.shape, small.dtype)]
    outs += [jax.ShapeDtypeStruct((2, s.shape[0] * CHIPS, s.shape[1]), s.dtype) for s in shards]
    dma = pltpu.SemaphoreType.DMA
    anywhere = pl.BlockSpec(memory_space=pl.ANY)
    return pl.pallas_call(
        gather_kernel,
        out_shape=outs,
        in_specs=[anywhere] * (3 + count),
        out_specs=[anywhere] * len(outs),
        scratch_shapes=[dma((count, 5, CHIPS)), dma((count, CHIPS)), dma((count, CHIPS)), dma((3, 8)), dma((8,)), dma((8,)), dma((8,)), dma((count,)),
                        dma((2 * CHIPS,)), dma((2 * CHIPS,))],
        compiler_params=pltpu.CompilerParams(collective_id=0, has_side_effects=True),
        name="gather",
    )(tokens, cotangent, small, *shards)


LOW, F32 = jnp.bfloat16, jnp.float32
EPS = 1e-12
HEAD = 64
LANES = 128
GROUP = 256
FULL = pl.BlockSpec(memory_space=pltpu.VMEM)


def nn(a, b):
    return jnp.dot(a, b, preferred_element_type=F32)


def nt(a, b):
    return lax.dot_general(a, b, (((1,), (1,)), ((), ())), preferred_element_type=F32)


def tn(a, b):
    return lax.dot_general(a, b, (((0,), (0,)), ((), ())), preferred_element_type=F32)


def lane_of(shape):
    return lax.broadcasted_iota(jnp.int32, shape, 1)


def turn(u):
    parts = []
    for start in range(0, u.shape[1], LANES):
        part = u[:, start:start + LANES]
        first = lane_of(part.shape) % HEAD < HEAD // 2
        parts.append(jnp.where(first, pltpu.roll(part, LANES - HEAD // 2, 1), pltpu.roll(part, HEAD // 2, 1)))
    return jnp.concatenate(parts, 1)


def weight_block(w_ref, block):
    per = 3 * w_ref.shape[1] // 2 // LANES
    cols = [w_ref[b // per, :, pl.ds(pl.multiple_of(b % per * LANES, LANES), LANES)] for b in (block, block + 1)]
    return jnp.concatenate(cols, 1)


def attend_kernel(x_ref, w_ref, cos_ref, sin_ref, bias_ref, q_ref, k_ref, v_ref, att_ref):
    group = pl.program_id(0)
    rows = q_ref.shape[0]
    mine = pl.ds(pl.multiple_of(lax.axis_index("dp") * rows, rows), rows)
    blocks = x_ref.shape[1] // LANES

    def turned(u, cos, sin):
        return u * jnp.concatenate([cos, cos], 1) + turn(u) * jnp.concatenate([sin, sin], 1)

    q = turned(nn(x_ref[mine, :], weight_block(w_ref, 2 * group)), cos_ref[mine, :], sin_ref[mine, :]).astype(LOW)
    q_ref[...] = q * jnp.asarray(0.125, LOW)
    k_ref[...] = turned(nn(x_ref[...], weight_block(w_ref, blocks + 2 * group)), cos_ref[...], sin_ref[...]).astype(LOW)
    v_ref[...] = nn(x_ref[...], weight_block(w_ref, 2 * blocks + 2 * group)).astype(LOW)
    step = 256
    bias = bias_ref[0:1, :]
    for pair in range(GROUP // LANES):
        lanes = slice(pair * LANES, pair * LANES + LANES)
        for start in range(0, rows, step):
            qp = q_ref[start:start + step, lanes]
            low = lane_of(qp.shape) < HEAD
            outs = []
            for head in range(2):
                qm = jnp.where(low if head == 0 else jnp.logical_not(low), qp, jnp.zeros_like(qp))
                s = nt(qm, k_ref[:, lanes]) + bias
                p = jnp.exp(s - jnp.max(s, axis=1, keepdims=True))
                total = jnp.sum(p, axis=1, keepdims=True)
                outs.append(nn(p.astype(LOW), v_ref[:, lanes]) / total)
            att_ref[start:start + step, lanes] = jnp.where(low, outs[0], outs[1]).astype(LOW)


def attend(x, w, cos, sin, bias):
    tokens, width = x.shape
    rows = tokens // 2
    shapes = [jax.ShapeDtypeStruct((n, width), LOW) for n in (rows, tokens, tokens, rows)]
    return pl.pallas_call(
        attend_kernel, grid=(width // GROUP,), out_shape=shapes,
        in_specs=[FULL] * 5,
        out_specs=[pl.BlockSpec((s.shape[0], GROUP), lambda g: (0, g)) for s in shapes],
        compiler_params=pltpu.CompilerParams(vmem_limit_bytes=60 << 20),
        cost_estimate=pl.CostEstimate(flops=8 * 10**9, bytes_accessed=10**7, transcendentals=6 * 10**6),
        name="attend")(x, w, cos, sin, bias)


def ln_parts(u):
    center = u - jnp.mean(u, axis=1, keepdims=True)
    inv = lax.rsqrt(jnp.mean(center * center, axis=1, keepdims=True) + EPS)
    return center * inv, inv


def ln_back(g, n, inv):
    return inv * (g - jnp.mean(g, axis=1, keepdims=True) - n * jnp.mean(g * n, axis=1, keepdims=True))


def middle_kernel(tiles, x_ref, att_ref, wo_ref, wg_ref, wu_ref, wd_ref, cot_ref, ln_ref, valid_ref,
                  y_ref, dwg_ref, dwu_ref, dwd_ref, dwo_ref, gatt_ref, gres_ref, dln_ref,
                  n1_ref, inv1_ref, hid_ref, hidt_ref, gate_ref, up_ref, acc_ref, gb_ref):
    index = pl.program_id(0)
    width = x_ref.shape[1]
    half = width // 2

    def wide(ref):
        return jnp.concatenate([ref[0], ref[1]], 1)

    @pl.when(index == 0)
    def _():
        n1, inv1 = ln_parts(x_ref[...].astype(F32) + nn(att_ref[...], wide(wo_ref)))
        hidden = n1 * ln_ref[0:1, :] + ln_ref[1:2, :]
        n1_ref[...] = n1
        inv1_ref[...] = jnp.broadcast_to(inv1, inv1_ref.shape)
        acc_ref[...] = hidden
        low = hidden.astype(LOW)
        hid_ref[...] = low
        hidt_ref[...] = low.T

    tile = wg_ref.shape[2]
    f = jnp.where(index < tiles, index, index - tiles)
    cols = pl.ds(pl.multiple_of(f * tile, tile), tile)

    @pl.when(index < tiles)
    def _():
        gate, up = nn(hid_ref[...], wg_ref[0]), nn(hid_ref[...], wu_ref[0])
        gate_ref[:, cols] = gate
        up_ref[:, cols] = up
        acc_ref[...] += nn((gate * jax.nn.sigmoid(gate) * up).astype(LOW), wide(wd_ref))

    @pl.when(index == tiles - 1)
    def _():
        n2, inv2 = ln_parts(acc_ref[...])
        valid = valid_ref[:, 0:1]
        y_ref[...] = ((n2 * ln_ref[2:3, :] + ln_ref[3:4, :]) * valid).astype(LOW)
        g_y = cot_ref[...].astype(F32) * valid
        dln_ref[2:3, :] = jnp.sum(g_y * n2, axis=0, keepdims=True)
        dln_ref[3:4, :] = jnp.sum(g_y, axis=0, keepdims=True)
        g_res2 = ln_back(g_y * ln_ref[2:3, :], n2, inv2)
        acc_ref[...] = g_res2
        gb_ref[...] = g_res2.astype(LOW)

    @pl.when(index >= tiles)
    def _():
        gate, up = gate_ref[:, cols], up_ref[:, cols]
        sig = jax.nn.sigmoid(gate)
        act = gate * sig
        gb = gb_ref[...]
        dwd = tn((act * up).astype(LOW), gb)
        dwd_ref[0] = dwd[:, :half].astype(LOW)
        dwd_ref[1] = dwd[:, half:].astype(LOW)
        g_inner = nt(gb, wide(wd_ref))
        g_gate = (g_inner * up * sig * (1.0 + gate * (1.0 - sig))).astype(LOW)
        g_up = (g_inner * act).astype(LOW)
        dwg_ref[0] = nn(hidt_ref[...], g_gate).astype(LOW)
        dwu_ref[0] = nn(hidt_ref[...], g_up).astype(LOW)
        acc_ref[...] += nt(g_gate, wg_ref[0]) + nt(g_up, wu_ref[0])

    @pl.when(index == 2 * tiles - 1)
    def _():
        g_hidden, n1 = acc_ref[...], n1_ref[...]
        dln_ref[0:1, :] = jnp.sum(g_hidden * n1, axis=0, keepdims=True)
        dln_ref[1:2, :] = jnp.sum(g_hidden, axis=0, keepdims=True)
        g_res1 = ln_back(g_hidden * ln_ref[0:1, :], n1, inv1_ref[:, 0:1])
        gres_ref[...] = g_res1
        gb1 = g_res1.astype(LOW)
        dwo = tn(att_ref[...], gb1)
        dwo_ref[0] = dwo[:, :half].astype(LOW)
        dwo_ref[1] = dwo[:, half:].astype(LOW)
        gatt_ref[...] = nt(gb1, wide(wo_ref)).astype(LOW)


def middle(x_own, att, wo, wg, wu, wd, cot, ln, valid):
    rows, width = x_own.shape
    hidden = wd.shape[1]
    tile = 512
    tiles = hidden // tile
    per = wg.shape[2] // tile
    at = lambda i: jnp.where(i < tiles, i, i - tiles)
    late = lambda i: jnp.maximum(i - tiles, 0)
    cols = lambda pick: pl.BlockSpec((1, width, tile), lambda i: (pick(i) // per, 0, pick(i) % per))
    rowb = lambda pick: pl.BlockSpec((2, tile, wd.shape[2]), lambda i: (0, pick(i), 0))
    sds = jax.ShapeDtypeStruct
    return pl.pallas_call(
        functools.partial(middle_kernel, tiles), grid=(2 * tiles,),
        out_shape=[sds((rows, width), LOW), sds(wg.shape, LOW), sds(wu.shape, LOW), sds(wd.shape, LOW), sds((2, width, width // 2), LOW),
                   sds((rows, width), LOW), sds((rows, width), F32), sds((8, width), F32)],
        in_specs=[FULL, FULL, pl.BlockSpec((2, width, width // 2), lambda i: (0, 0, 3)), cols(at), cols(at), rowb(at), FULL, FULL, FULL],
        out_specs=[FULL, cols(late), cols(late), rowb(late), FULL, FULL, FULL, FULL],
        scratch_shapes=[pltpu.VMEM((rows, width), F32), pltpu.VMEM((rows, LANES), F32), pltpu.VMEM((rows, width), LOW),
                        pltpu.VMEM((width, rows), LOW), pltpu.VMEM((rows, hidden), F32), pltpu.VMEM((rows, hidden), F32),
                        pltpu.VMEM((rows, width), F32), pltpu.VMEM((rows, width), LOW)],
        compiler_params=pltpu.CompilerParams(vmem_limit_bytes=60 << 20),
        cost_estimate=pl.CostEstimate(flops=24 * 10**9, bytes_accessed=6 * 10**7, transcendentals=3 * 10**6),
        name="middle")(x_own, att, wo, wg, wu, wd, cot, ln, valid)

BACK_ORDERS = ("xzy", "zyx", "zyx")
LATE_ORDERS = ("zxy", "zyx", "zxy")
FAR_FIRST = OFFSETS[::-1]
SIDES = {"x": 2, "y": 2, "z": ZS}


def landing_slots(order):
    sizes, room = {}, 1
    for axis in order:
        sizes[axis] = room * (ZS if axis == "z" else 1)
        room *= SIDES[axis]
    return sizes["x"], sizes["y"], sizes["z"], sizes["z"]


def landing_index(order, link, x, y, z):
    axis = "xyzz"[link]
    index = 0
    for before in order:
        if before == axis:
            break
        index = index * SIDES[before] + {"x": x, "y": y, "z": z}[before]
    return index * ZS + z if axis == "z" else index


def back_scatter_kernel(y_own, dwg, dwu, dwd, dwo, dsmall, x_in, w_in, q_in, k_in, v_in, g_in, res_in, cos_in, sin_in, bias_in,
                        y_out, gt_out, f_gate, f_up, f_down, f_out, f_qkv, f_small, *refs):
    (xv, wv, qv, kv, vv, gv, own_acc, cosv, sinv, biasv, xt, oth_acc, dq, dk, dv, dw), refs = refs[:16], refs[16:]
    owns, refs = refs[:3], refs[3:]
    sibs, refs = refs[:4], refs[4:]
    down_out, refs = refs[0], refs[1:]
    lands, refs = refs[:24], refs[24:]
    (gt_low, gt_sib, smalls), refs = refs[:3], refs[3:]
    (in_sem, send_sem, recv_sem, sib_send, sib_recv, own_sem, late_send, late_recv, late_sib_send, late_sib_recv,
     gt_sem, tok_send, y_recv, gt_recv, small_send, small_recv) = refs
    core, chip, x, y, z = place()
    other = 1 - core
    half = CHIPS // 2
    me = core * CHIPS + chip
    span = y_out.shape[1]
    rows = qv.shape[0]
    mine = pl.ds(pl.multiple_of(core * rows, rows), rows)
    theirs = pl.ds(pl.multiple_of(other * rows, rows), rows)
    neighbours = (
        {"dp": core, "seq": chip_at(1 - x, y, z)},
        {"dp": core, "seq": chip_at(x, 1 - y, z)},
        {"dp": core, "seq": chip_at(x, y, jnp.minimum(z + 1, ZS - 1))},
        {"dp": core, "seq": chip_at(x, y, jnp.maximum(z - 1, 0))},
    )
    sibling = {"dp": other, "seq": chip}

    loads = [pltpu.make_async_copy(source, target, in_sem.at[n]) for n, (source, target) in enumerate((
        (k_in, kv), (q_in, qv), (bias_in, biasv), (v_in, vv), (g_in, gv), (x_in, xv), (w_in, wv), (res_in, own_acc), (cos_in, cosv), (sin_in, sinv)))]
    for load in loads:
        load.start()

    def cut(ref, size, index):
        return ref.at[pl.ds(pl.multiple_of(index * size, size), size)]

    rows_gate, rows_down, rows_out = f_gate.shape[0], f_down.shape[0], f_out.shape[0]

    def parts(m, owner, dest):
        if m == 0:
            return [(cut(dwg.at[owner], rows_gate, dest), 0, rows_gate)]
        if m == 1:
            return [(cut(dwu.at[owner], rows_gate, dest), 0, rows_gate)]
        return [(cut(dwd.at[owner], rows_down, dest), 0, rows_down), (cut(dwo.at[owner], rows_out, dest), rows_down, rows_out)]

    def to_sibling(m, dest):
        return [pltpu.make_async_remote_copy(
            src_ref=source, dst_ref=sibs[m].at[dest, pl.ds(start, size)], send_sem=sib_send.at[m + n, dest],
            recv_sem=sib_recv.at[m + n, dest], device_id=sibling, device_id_type=MESH)
            for n, (source, start, size) in enumerate(parts(m, other, dest))]

    def own_load(m, dest, slot):
        return [pltpu.make_async_copy(source, owns[m].at[slot, pl.ds(start, size)], own_sem.at[m + n, slot])
                for n, (source, start, size) in enumerate(parts(m, core, dest))]

    def dest_of(index):
        dx = pick(index, [o[0] for o in FAR_FIRST])
        dy = pick(index, [o[1] for o in FAR_FIRST])
        dz = pick(index, [o[2] for o in FAR_FIRST])
        return dx, dy, dz, (z + dz >= 0) & (z + dz < ZS), (x + dx) % 2, (y + dy) % 2, jnp.clip(z + dz, 0, ZS - 1)

    meet_all(core, chip)

    def begin(index, carry):
        dx, dy, dz, valid, tx, ty, tz = dest_of(index)

        @pl.when(valid)
        def _():
            for m in range(3):
                for copy in to_sibling(m, chip_at(tx, ty, tz)):
                    copy.start()
        return carry

    lax.fori_loop(0, len(FAR_FIRST), begin, 0)

    def prefetch(index):
        dx, dy, dz, valid, tx, ty, tz = dest_of(index)

        @pl.when(valid & (index < len(FAR_FIRST)))
        def _():
            for m in range(3):
                for copy in own_load(m, chip_at(tx, ty, tz), index % 3):
                    copy.start()

    prefetch(jnp.int32(0))
    prefetch(jnp.int32(1))

    def deliver(source, target, k, recvs):
        def one(j, carry):
            i = (chip + 1 + j) % half
            to_core, to_chip = chip // half, core * half + i
            src, dst = cut(source, span, i), target.at[chip % half]
            self_copy = (to_core == core) & (to_chip == chip)

            @pl.when(self_copy)
            def _():
                pltpu.make_async_copy(src, dst, recvs.at[chip % half]).start()

            @pl.when(jnp.logical_not(self_copy))
            def _():
                pltpu.make_async_remote_copy(
                    src_ref=src, dst_ref=dst, send_sem=tok_send.at[k, i], recv_sem=recvs.at[chip % half],
                    device_id={"dp": to_core, "seq": to_chip}, device_id_type=MESH).start()
            return carry

        lax.fori_loop(0, half, one, 0)

    def small_to(step):
        to = (me + step) % (2 * CHIPS)
        return pltpu.make_async_remote_copy(
            src_ref=dsmall.at[to], dst_ref=smalls.at[me], send_sem=small_send.at[step], recv_sem=small_recv.at[me],
            device_id={"dp": to // CHIPS, "seq": to % CHIPS}, device_id_type=MESH)

    deliver(y_own, y_out, 0, y_recv)
    lax.fori_loop(1, 2 * CHIPS, lambda s, c: (small_to(s).start(), c)[1], 0)
    own_small = pltpu.make_async_copy(dsmall.at[me], smalls.at[me], small_recv.at[me])
    own_small.start()

    def reduce_piece(order, lands_m, send_at, recv_at, own, acc, offset, target, last, final):
        dx, dy, dz = offset
        tx, ty, tz = target
        fx, fy, up, down = spread(order, dx, dy, dz)
        flags = (fx, fy, up & (z < ZS - 1), down & (z > 0))

        @pl.when(jnp.logical_not(last))
        def _():
            acc[...] += own()

        @pl.when(last)
        def _():
            final[...] = acc[...].astype(F32) + own().astype(F32)

        for link in range(4):
            land = lands_m[link].at[landing_index(order, link, tx, ty, tz)]

            @pl.when(flags[link])
            def _():
                pltpu.make_async_copy(land, land, recv_at(link)).wait()

            @pl.when(flags[link] & jnp.logical_not(last))
            def _():
                acc[...] += land[...]

            @pl.when(flags[link] & last)
            def _():
                final[...] += land[...].astype(F32)

        away = {"x": dx != 0, "y": dy != 0, "z": dz != 0}
        taken = None
        for axis in order[::-1]:
            here = away[axis] if taken is None else away[axis] & jnp.logical_not(taken)
            taken = away[axis] if taken is None else taken | away[axis]
            for link in {"x": (0,), "y": (1,), "z": (2, 3)}[axis]:
                go = here if axis != "z" else (here & (dz > 0 if link == 2 else dz < 0))
                there = {0: 0, 1: 1, 2: 3, 3: 2}[link]

                @pl.when(go)
                def _():
                    pltpu.make_async_remote_copy(
                        src_ref=acc, dst_ref=lands_m[there].at[landing_index(order, there, tx, ty, tz)],
                        send_sem=send_at, recv_sem=recv_at(there), device_id=neighbours[link], device_id_type=MESH).start()

    def early(index):
        dx, dy, dz, valid, tx, ty, tz = dest_of(index)
        last = index == len(FAR_FIRST) - 1
        prefetch(index + 2)

        @pl.when(valid)
        def _():
            dest = chip_at(tx, ty, tz)
            for m in range(3):
                for copy in own_load(m, dest, index % 3):
                    copy.wait()
                for copy in to_sibling(m, dest):
                    copy.wait_recv()
                reduce_piece(BACK_ORDERS[m], lands[4 * m:4 * m + 4], send_sem.at[m, dest], lambda link: recv_sem.at[m, link, dest],
                             lambda: owns[m][index % 3], sibs[m].at[dest], (dx, dy, dz), (tx, ty, tz), last, (f_gate, f_up, down_out)[m])

    step = 256
    per_group = (GROUP // LANES) * (rows // step) * 2
    groups = xv.shape[1] // GROUP
    chunks = groups * per_group
    blocks = xv.shape[1] // LANES
    for load in loads[:5]:
        load.wait()

    def chunk(index):
        group, inner = index // per_group, index % per_group
        pair, block, head = inner // (per_group // 2), inner // 2 % (rows // step), inner % 2
        here = pl.ds(pl.multiple_of(block * step, step), step)
        lanes = pl.ds(pl.multiple_of(group * GROUP + pair * LANES, LANES), LANES)
        out_lanes = pl.ds(pl.multiple_of(pair * LANES, LANES), LANES)

        @pl.when(inner == 0)
        def _():
            dq[...] = jnp.zeros_like(dq)
            dk[...] = jnp.zeros_like(dk)
            dv[...] = jnp.zeros_like(dv)

        qp, gp = qv[here, lanes], gv[here, lanes]
        keep = lane_of(qp.shape) // HEAD == head
        qm, gm = jnp.where(keep, qp, jnp.zeros_like(qp)), jnp.where(keep, gp, jnp.zeros_like(gp))
        kp, vp = kv[:, lanes], vv[:, lanes]
        s = nt(kp, qm) + jnp.concatenate([biasv[...]] * (step // LANES), 1)
        e = jnp.exp(s - jnp.max(s, axis=0, keepdims=True))
        p = e * (1.0 / jnp.sum(e, axis=0, keepdims=True))
        dp = nt(vp, gm)
        delta = jnp.sum(p * dp, axis=0, keepdims=True)
        ds = (p * (dp - delta)).astype(LOW)
        dv[:, out_lanes] += nn(p.astype(LOW), gm)
        dk[:, out_lanes] += nn(ds, qm)
        dq[here, out_lanes] += jnp.where(keep, tn(ds, kp), 0.0)

        @pl.when(index == per_group - 1)
        def _():
            for load in loads[5:]:
                load.wait()
            xt[...] = xv[...].T
            oth_acc[...] = jnp.zeros_like(oth_acc)

        @pl.when(inner == per_group - 1)
        def _():
            finish(group)

    def finish(group):
        def back(u, cos, sin):
            return u * jnp.concatenate([cos, cos], 1) - turn(u) * jnp.concatenate([sin, sin], 1)

        def put(block, value):
            per = dw.shape[2] // LANES
            for i in range(2):
                b = block + i
                dw[b // per, :, pl.ds(pl.multiple_of(b % per * LANES, LANES), LANES)] = value[:, i * LANES:i * LANES + LANES].astype(LOW)

        def weights(block):
            per = dw.shape[2] // LANES
            return jnp.concatenate([wv[b // per, :, pl.ds(pl.multiple_of(b % per * LANES, LANES), LANES)] for b in (block, block + 1)], 1)

        gq = back(dq[...] * 0.125, cosv[mine, :], sinv[mine, :]).astype(LOW)
        dk[...] = back(dk[...], cosv[...], sinv[...])
        put(2 * group, nn(xt[:, mine], gq))
        put(blocks + 2 * group, nn(xt[...], dk[...].astype(LOW)))
        put(2 * blocks + 2 * group, nn(xt[...], dv[...].astype(LOW)))
        wq, wk, wvv = (weights(n * blocks + 2 * group) for n in range(3))
        own_acc[...] += nt(gq, wq) + nt(dk[mine, :].astype(LOW), wk) + nt(dv[mine, :].astype(LOW), wvv)
        oth_acc[...] += nt(dk[theirs, :].astype(LOW), wk) + nt(dv[theirs, :].astype(LOW), wvv)

    def turn_of(index, carry):
        chunk(index)

        @pl.when(index < mixed)
        def _():
            early(index)
        return carry

    mixed = min(chunks, len(FAR_FIRST) - 4)
    lax.fori_loop(0, chunks, turn_of, 0)

    gt_low[...] = oth_acc[...].astype(LOW)
    third = f_qkv.shape[1] // len(LATE_ORDERS)

    def late_to_sibling(dest):
        return pltpu.make_async_remote_copy(
            src_ref=cut(dw.at[other], rows_gate, dest), dst_ref=sibs[3].at[dest], send_sem=late_sib_send.at[dest],
            recv_sem=late_sib_recv.at[dest], device_id=sibling, device_id_type=MESH)

    def late_begin(index, carry):
        dx, dy, dz, valid, tx, ty, tz = dest_of(index)

        @pl.when(valid)
        def _():
            late_to_sibling(chip_at(tx, ty, tz)).start()
        return carry

    lax.fori_loop(0, len(FAR_FIRST), late_begin, 0)
    cross = pltpu.make_async_remote_copy(src_ref=gt_low, dst_ref=gt_sib, send_sem=gt_sem.at[0], recv_sem=gt_sem.at[1],
                                         device_id=sibling, device_id_type=MESH)
    cross.start()

    def late(index, carry):
        dx, dy, dz, valid, tx, ty, tz = dest_of(index)
        last = index == len(FAR_FIRST) - 1

        @pl.when(valid)
        def _():
            dest = chip_at(tx, ty, tz)
            late_to_sibling(dest).wait_recv()
            for n, order in enumerate(LATE_ORDERS):
                lanes = slice(n * third, n * third + third)
                acc = sibs[3].at[dest, :, lanes]
                reduce_piece(order, lands[12 + 4 * n:16 + 4 * n], late_send.at[n, dest], lambda link: late_recv.at[n, link, dest],
                             lambda: dw[core, pl.ds(pl.multiple_of(dest * rows_gate, rows_gate), rows_gate), lanes],
                             acc, (dx, dy, dz), (tx, ty, tz), last, f_qkv.at[:, lanes])

        @pl.when((index % 2 == 1) & (mixed + index // 2 < len(FAR_FIRST)))
        def _():
            early(mixed + index // 2)
        return carry

    early_steps = 8
    lax.fori_loop(0, early_steps, late, 0)
    cross.wait()
    gt_low[...] = (own_acc[...] + gt_sib[...].astype(F32)).astype(LOW)
    deliver(gt_low, gt_out, 1, gt_recv)
    lax.fori_loop(early_steps, len(FAR_FIRST), late, 0)
    f_down[...] = down_out[0:rows_down, :]
    f_out[...] = down_out[rows_down:rows_down + rows_out, :]

    def small_end(s, carry):
        small_to(s).wait_send()
        source = (me + s) % (2 * CHIPS)
        pltpu.make_async_copy(smalls.at[source], smalls.at[source], small_recv.at[source]).wait()
        return carry

    lax.fori_loop(1, 2 * CHIPS, small_end, 0)
    own_small.wait()
    f_small[...] = jnp.sum(smalls[...], axis=0)

    def ends(i, carry):
        for out, recvs, k in ((y_out, y_recv, 0), (gt_out, gt_recv, 1)):
            pltpu.make_async_copy(out.at[i], out.at[i], recvs.at[i]).wait()
            self_copy = (chip // half == core) & (core * half + i == chip)

            @pl.when(jnp.logical_not(self_copy))
            def _():
                pltpu.make_async_copy(out.at[i], out.at[i], tok_send.at[k, i]).wait()
        return carry

    lax.fori_loop(0, half, ends, 0)

    def sent(dest, carry):
        for m in range(3):
            for copy in to_sibling(m, dest):
                copy.wait_send()
        late_to_sibling(dest).wait_send()

        @pl.when(dest != chip)
        def _():
            for m in range(3):
                pltpu.make_async_copy(sibs[m].at[dest], sibs[m].at[dest], send_sem.at[m, dest]).wait()
            for n in range(len(LATE_ORDERS)):
                part = sibs[3].at[dest, :, pl.ds(n * third, third)]
                pltpu.make_async_copy(part, part, late_send.at[n, dest]).wait()
        return carry

    lax.fori_loop(0, CHIPS, sent, 0)


def back_scatter(y_own, dwg, dwu, dwd, dwo, dsmall, x, w, q, k, v, g_att, g_res1, cos, sin, bias_col):
    tokens, width = x.shape
    rows = tokens // 2
    span = rows // 8
    anywhere, vmem = pl.BlockSpec(memory_space=pl.ANY), pl.BlockSpec(memory_space=pltpu.VMEM)
    n_gate, n_down, n_out = width // CHIPS, dwd.shape[1] // CHIPS, dwo.shape[1] // CHIPS
    c_gate, c_down = dwg.shape[2], dwd.shape[2]
    c_qkv = 3 * width // 2
    third = c_qkv // len(LATE_ORDERS)
    sds, mem = jax.ShapeDtypeStruct, pltpu.VMEM
    out8 = sds((8, span, width), LOW)
    finals = [sds((n_gate, c_gate), F32), sds((n_gate, c_gate), F32), sds((n_down, c_down), F32), sds((n_out, c_down), F32),
              sds((n_gate, c_qkv), F32), sds(dsmall.shape[1:], F32)]
    pieces = [(n_gate, c_gate), (n_gate, c_gate), (n_down + n_out, c_down)]
    scratch = [mem((tokens, width), LOW), mem(w.shape, LOW), mem((rows, width), LOW), mem((tokens, width), LOW), mem((tokens, width), LOW),
               mem((rows, width), LOW), mem((rows, width), F32), mem(cos.shape, F32), mem(sin.shape, F32), mem(bias_col.shape, F32),
               mem((width, tokens), LOW), mem((rows, width), F32), mem((rows, GROUP), F32), mem((tokens, GROUP), F32), mem((tokens, GROUP), F32),
               mem((2, width, c_qkv), LOW)]
    scratch += [mem((3,) + piece, LOW) for piece in pieces]
    scratch += [mem((CHIPS,) + piece, LOW) for piece in pieces] + [mem((CHIPS, n_gate, c_qkv), LOW)]
    scratch += [mem(pieces[2], F32)]
    for order, piece in zip(BACK_ORDERS, pieces):
        scratch += [mem((n,) + piece, LOW) for n in landing_slots(order)]
    for order in LATE_ORDERS:
        scratch += [mem((n, n_gate, third), LOW) for n in landing_slots(order)]
    scratch += [mem((rows, width), LOW), mem((rows, width), LOW), mem(dsmall.shape, F32)]
    dma = pltpu.SemaphoreType.DMA
    scratch += [dma((10,)), dma((3, CHIPS)), dma((3, 4, CHIPS)), dma((4, CHIPS)), dma((4, CHIPS)), dma((4, 3)), dma((3, CHIPS)), dma((3, 4, CHIPS)),
                dma((CHIPS,)), dma((CHIPS,)), dma((2,)), dma((2, 8)), dma((8,)), dma((8,)), dma((2 * CHIPS,)), dma((2 * CHIPS,))]
    return pl.pallas_call(
        back_scatter_kernel,
        out_shape=[out8, out8] + finals,
        in_specs=[anywhere] * 16,
        out_specs=[anywhere] * 2 + [vmem] * len(finals),
        scratch_shapes=scratch,
        compiler_params=pltpu.CompilerParams(collective_id=1, has_side_effects=True, vmem_limit_bytes=67043328),
        name="back_scatter",
    )(y_own, dwg, dwu, dwd, dwo, dsmall, x, w, q, k, v, g_att, g_res1, cos, sin, bias_col)


def rotary_lanes(tokens):
    lane = jnp.arange(LANES)
    pair_index = (lane % (HEAD // 2)).astype(F32)
    inverse = jnp.power(jnp.float32(1000.0), -2.0 * pair_index / HEAD)
    angles = jnp.arange(tokens).astype(F32)[:, None] * inverse[None, :]
    sign = jnp.where(lane % HEAD < HEAD // 2, -1.0, 1.0).astype(F32)
    return jnp.cos(angles), jnp.sin(angles) * sign[None, :]


def local_by_slot(tokens, lengths, w_qkv, w_out, w_gate, w_up, w_down, ln_params, cotangent):
    slots, span, width = tokens.shape
    core, chip = lax.axis_index("dp"), lax.axis_index("seq")
    half = CHIPS // 2
    small = jnp.zeros((8, LANES), F32)
    share = ln_params.shape[1]
    small = small.at[:4, :share].set(ln_params.astype(F32)).at[4, :slots].set(lengths.astype(F32))
    x, cot, smalls, w_in, wg, wu, wd = gather(tokens, cotangent, small, [jnp.concatenate([w_qkv, w_out], 1), w_gate, w_up, w_down])
    total, rows = x.shape[0], x.shape[0] // 2
    ln = jnp.pad(smalls[:, :4, :share].transpose(1, 0, 2).reshape(4, width), ((0, 4), (0, 0)))
    length = lax.dynamic_slice(smalls, (chip // half * CHIPS, 4, chip % half), (1, 1, 1)).reshape(()).astype(jnp.int32)
    cos, sin = rotary_lanes(total)
    position = jnp.arange(total)
    out_of = jnp.where(position < length, 0.0, masked_score).astype(F32)
    bias = jnp.broadcast_to(out_of[None, :], (8, total))
    bias_col = jnp.broadcast_to(out_of[:, None], (total, LANES))
    valid = jnp.broadcast_to((core * rows + jnp.arange(rows) < length).astype(F32)[:, None], (rows, LANES))
    q, k, v, att = attend(x, w_in, cos, sin, bias)
    x_own = lax.dynamic_slice_in_dim(x, core * rows, rows, 0)
    y, dwg, dwu, dwd, dwo, g_att, g_res1, dln = middle(x_own, att, w_in, wg, wu, wd, cot, ln, valid)
    dsmall = dln[:4].reshape(4, 2 * CHIPS, share).transpose(1, 0, 2)
    dsmall = jnp.pad(dsmall, ((0, 0), (0, 4), (0, LANES - share)))
    output, grad_tokens, d_gate, d_up, d_down, d_out, d_qkv, d_small = back_scatter(
        y, dwg, dwu, dwd, dwo, dsmall, x, w_in, q, k, v, g_att, g_res1, cos, sin, bias_col)
    return (output, grad_tokens, d_qkv, d_out, d_gate, d_up, d_down, d_small[:4, :share])


def solution(mesh):
    placed = (
        P("dp", "seq", None),
        P("dp"),
        P("seq", "dp"),
        P("seq", "dp"),
        P("seq", "dp"),
        P("seq", "dp"),
        P("seq", "dp"),
        P(None, ("dp", "seq")),
        P("dp", "seq", None),
    )

    def run(tokens, *rest):
        by_slot = mesh.shape["dp"] == 2 and mesh.shape["seq"] == CHIPS and tokens.shape[0] == CHIPS
        body = local_by_slot if by_slot else local
        return jax.shard_map(
            body,
            mesh=mesh,
            in_specs=placed,
            out_specs=(
                P("dp", "seq", None),
                P("dp", "seq", None),
                P("seq", "dp"),
                P("seq", "dp"),
                P("seq", "dp"),
                P("seq", "dp"),
                P("seq", "dp"),
                P(None, ("dp", "seq")),
            ),
            check_vma=False,
        )(tokens, *rest)

    return run
```

```python
import functools

import jax
import jax.numpy as jnp
from jax import lax
from jax.experimental import pallas as pl
from jax.experimental.pallas import tpu as pltpu
from jax.sharding import PartitionSpec as P

HEADS = 12
HEAD_DIM = 64


norm_epsilon = 1e-12
score_scale = 0.125
masked_score = -1e30


def shifted(shard, axis, by):
    count = lax.axis_size(axis)
    return lax.ppermute(shard, axis, [(i, (i + by) % count) for i in range(count)])


def rotary_tables(positions):
    pair_index = jnp.arange(HEAD_DIM // 2, dtype=jnp.float32)
    inverse = jnp.power(jnp.float32(1000.0), -2.0 * pair_index / HEAD_DIM)
    angles = positions.astype(jnp.float32)[:, None] * inverse[None, :]
    cos_tab = jnp.concatenate([jnp.cos(angles), jnp.cos(angles)], axis=-1)
    sin_tab = jnp.concatenate([jnp.sin(angles), jnp.sin(angles)], axis=-1)
    return (cos_tab, sin_tab)


def rotate(values, cos_tab, sin_tab):
    half_dim = values.shape[-1] // 2
    turned = jnp.concatenate([-values[..., half_dim:], values[..., :half_dim]], axis=-1)
    return values * cos_tab + turned * sin_tab


def norm_parts(values, gain_vec, bias_vec):
    center = values - jnp.mean(values, axis=-1, keepdims=True)
    inv_std = lax.rsqrt(jnp.mean(center * center, axis=-1, keepdims=True) + norm_epsilon)
    normed = center * inv_std
    return (normed * gain_vec + bias_vec, normed, inv_std)


def norm_back(grad_in, normed, inv_std, gain_vec):
    scaled = grad_in * gain_vec
    return inv_std * (
        scaled
        - jnp.mean(scaled, axis=-1, keepdims=True)
        - normed * jnp.mean(scaled * normed, axis=-1, keepdims=True)
    )


def heads_view(flat_rows):
    return flat_rows.reshape(flat_rows.shape[0], flat_rows.shape[1], HEADS, HEAD_DIM)


def attend_block(run_state, queries, key_blk, value_blk, key_start, lengths):
    run_max, run_sum, run_acc = run_state
    scores = (
        jnp.einsum(
            "sqhd,skhd->shqk",
            heads_view(queries),
            heads_view(key_blk),
            preferred_element_type=jnp.float32,
        )
        * score_scale
    )
    key_pos = key_start + jnp.arange(key_blk.shape[1], dtype=jnp.int32)
    key_mask = (key_pos[None, :] < lengths[:, None])[:, None, None, :]
    scores = jnp.where(key_mask, scores, masked_score)
    new_max = jnp.maximum(run_max, jnp.max(scores, axis=-1))
    exp_scores = jnp.where(key_mask, jnp.exp(scores - new_max[..., None]), 0.0)
    factor = jnp.exp(run_max - new_max)
    run_sum = run_sum * factor + jnp.sum(exp_scores, axis=-1)
    run_acc = run_acc * factor[..., None] + jnp.einsum(
        "shqk,skhd->shqd",
        exp_scores.astype(jnp.bfloat16),
        heads_view(value_blk),
        preferred_element_type=jnp.float32,
    )
    return (new_max, run_sum, run_acc)


def block_grads(queries, grad_att, log_total, delta_rows, key_blk, value_blk, key_ok):
    query_h = heads_view(queries)
    grad_h = heads_view(grad_att)
    key_h = heads_view(key_blk)
    scores = (
        jnp.einsum("sqhd,skhd->shqk", query_h, key_h, preferred_element_type=jnp.float32)
        * score_scale
    )
    key_mask = key_ok[:, None, None, :]
    soft_probs = jnp.where(key_mask, jnp.exp(scores - log_total[..., None]), 0.0)
    grad_probs = jnp.einsum(
        "sqhd,skhd->shqk", grad_h, heads_view(value_blk), preferred_element_type=jnp.float32
    )
    grad_scores = (soft_probs * (grad_probs - delta_rows[..., None])).astype(jnp.bfloat16)
    part_q = (
        jnp.einsum("shqk,skhd->sqhd", grad_scores, key_h, preferred_element_type=jnp.float32)
        * score_scale
    )
    part_k = (
        jnp.einsum("shqk,sqhd->skhd", grad_scores, query_h, preferred_element_type=jnp.float32)
        * score_scale
    )
    part_v = jnp.einsum(
        "shqk,sqhd->skhd",
        soft_probs.astype(jnp.bfloat16),
        grad_h,
        preferred_element_type=jnp.float32,
    )
    shape_out = queries.shape
    return (part_q.reshape(shape_out), part_k.reshape(key_blk.shape), part_v.reshape(key_blk.shape))


def local(tokens, lengths, w_qkv, w_out, w_gate, w_up, w_down, ln_params, cotangent):
    slot_count, span_len, width = tokens.shape
    row_count = slot_count * span_len
    cycle_size = lax.axis_size("seq")
    my_index = lax.axis_index("seq")
    row_qkv, row_out, row_gate, row_up, row_down, row_norm = (
        lax.all_gather(w_qkv, "seq", axis=0, tiled=True),
        lax.all_gather(w_out, "seq", axis=0, tiled=True),
        lax.all_gather(w_gate, "seq", axis=0, tiled=True),
        lax.all_gather(w_up, "seq", axis=0, tiled=True),
        lax.all_gather(w_down, "seq", axis=0, tiled=True),
        lax.all_gather(ln_params, "seq", axis=1, tiled=True),
    )
    wide_qkv, wide_out, wide_gate, wide_up, wide_down, wide_norm = (
        lax.all_gather(row_qkv, "dp", axis=1, tiled=True),
        lax.all_gather(row_out, "dp", axis=1, tiled=True),
        lax.all_gather(row_gate, "dp", axis=1, tiled=True),
        lax.all_gather(row_up, "dp", axis=1, tiled=True),
        lax.all_gather(row_down, "dp", axis=1, tiled=True),
        lax.all_gather(row_norm, "dp", axis=1, tiled=True),
    )
    norm_full = wide_norm.astype(jnp.float32)
    flat_tokens = tokens.reshape(row_count, width)
    token_f32 = flat_tokens.astype(jnp.float32)
    positions = my_index * span_len + jnp.arange(span_len, dtype=jnp.int32)
    row_valid = (positions[None, :] < lengths[:, None]).astype(jnp.float32).reshape(row_count, 1)
    cos_tab, sin_tab = rotary_tables(positions)
    cos_four = cos_tab[None, :, None, :]
    sin_four = sin_tab[None, :, None, :]
    qkv_pre = jnp.dot(flat_tokens, wide_qkv, preferred_element_type=jnp.float32)
    split_qkv = qkv_pre.reshape(slot_count, span_len, 3, HEADS, HEAD_DIM)
    queries = (
        rotate(split_qkv[:, :, 0], cos_four, sin_four)
        .astype(jnp.bfloat16)
        .reshape(slot_count, span_len, width)
    )
    keys_rot = (
        rotate(split_qkv[:, :, 1], cos_four, sin_four)
        .astype(jnp.bfloat16)
        .reshape(slot_count, span_len, width)
    )
    values = split_qkv[:, :, 2].astype(jnp.bfloat16).reshape(slot_count, span_len, width)
    start_state = (
        jnp.full((slot_count, HEADS, span_len), masked_score, jnp.float32),
        jnp.zeros((slot_count, HEADS, span_len), jnp.float32),
        jnp.zeros((slot_count, HEADS, span_len, HEAD_DIM), jnp.float32),
    )
    key_piece = lax.all_gather(keys_rot, "seq", axis=1, tiled=True)
    value_piece = lax.all_gather(values, "seq", axis=1, tiled=True)
    block_count = key_piece.shape[1] // span_len

    def one_block(block_id, inner_state):
        offset = block_id * span_len
        key_blk = lax.dynamic_slice_in_dim(key_piece, offset, span_len, axis=1)
        value_blk = lax.dynamic_slice_in_dim(value_piece, offset, span_len, axis=1)
        return attend_block(inner_state, queries, key_blk, value_blk, offset, lengths)

    run_max, run_sum, run_acc = lax.fori_loop(0, block_count, one_block, start_state)
    attended = run_acc / run_sum[..., None]
    log_total = run_max + jnp.log(run_sum)
    attn_low = attended.transpose(0, 2, 1, 3).reshape(row_count, width).astype(jnp.bfloat16)
    branch = jnp.dot(attn_low, wide_out, preferred_element_type=jnp.float32)
    hidden, normed_one, inv_one = norm_parts(token_f32 + branch, norm_full[0], norm_full[1])
    hidden_low = hidden.astype(jnp.bfloat16)
    gate_pre = jnp.dot(hidden_low, wide_gate, preferred_element_type=jnp.float32)
    up_proj = jnp.dot(hidden_low, wide_up, preferred_element_type=jnp.float32)
    activated = jax.nn.silu(gate_pre)
    inner_low = (activated * up_proj).astype(jnp.bfloat16)
    branch_two = jnp.dot(inner_low, wide_down, preferred_element_type=jnp.float32)
    result, normed_two, inv_two = norm_parts(hidden + branch_two, norm_full[2], norm_full[3])
    output = (result * row_valid).astype(jnp.bfloat16).reshape(slot_count, span_len, width)
    back_qkv, back_out, back_gate, back_up, back_down, back_norm = (
        lax.all_gather(w_qkv, "seq", axis=0, tiled=True),
        lax.all_gather(w_out, "seq", axis=0, tiled=True),
        lax.all_gather(w_gate, "seq", axis=0, tiled=True),
        lax.all_gather(w_up, "seq", axis=0, tiled=True),
        lax.all_gather(w_down, "seq", axis=0, tiled=True),
        lax.all_gather(ln_params, "seq", axis=1, tiled=True),
    )
    wide_qkv, wide_out, wide_gate, wide_up, wide_down, wide_norm = (
        lax.all_gather(back_qkv, "dp", axis=1, tiled=True),
        lax.all_gather(back_out, "dp", axis=1, tiled=True),
        lax.all_gather(back_gate, "dp", axis=1, tiled=True),
        lax.all_gather(back_up, "dp", axis=1, tiled=True),
        lax.all_gather(back_down, "dp", axis=1, tiled=True),
        lax.all_gather(back_norm, "dp", axis=1, tiled=True),
    )
    norm_full = wide_norm.astype(jnp.float32)
    grad_out = cotangent.reshape(row_count, width).astype(jnp.float32) * row_valid
    gain_two_grad = jnp.sum(grad_out * normed_two, axis=0)
    bias_two_grad = jnp.sum(grad_out, axis=0)
    grad_res2 = norm_back(grad_out, normed_two, inv_two, norm_full[2])
    grad_branch2 = grad_res2.astype(jnp.bfloat16)
    grad_wdown = jnp.einsum(
        "rf,rd->fd", inner_low, grad_branch2, preferred_element_type=jnp.float32
    )
    grad_inner = jnp.einsum(
        "rd,fd->rf", grad_branch2, wide_down, preferred_element_type=jnp.float32
    )
    sigma = jax.nn.sigmoid(gate_pre)
    grad_gate = (grad_inner * up_proj * sigma * (1.0 + gate_pre * (1.0 - sigma))).astype(
        jnp.bfloat16
    )
    grad_up = (grad_inner * activated).astype(jnp.bfloat16)
    grad_wgate = jnp.einsum("rd,rf->df", hidden_low, grad_gate, preferred_element_type=jnp.float32)
    grad_wup = jnp.einsum("rd,rf->df", hidden_low, grad_up, preferred_element_type=jnp.float32)
    grad_hidden = (
        grad_res2
        + jnp.einsum("rf,df->rd", grad_gate, wide_gate, preferred_element_type=jnp.float32)
        + jnp.einsum("rf,df->rd", grad_up, wide_up, preferred_element_type=jnp.float32)
    )
    gain_one_grad = jnp.sum(grad_hidden * normed_one, axis=0)
    bias_one_grad = jnp.sum(grad_hidden, axis=0)
    grad_res1 = norm_back(grad_hidden, normed_one, inv_one, norm_full[0])
    grad_branch1 = grad_res1.astype(jnp.bfloat16)
    grad_wout = jnp.einsum("ri,rd->id", attn_low, grad_branch1, preferred_element_type=jnp.float32)
    grad_att = (
        jnp.einsum("rd,id->ri", grad_branch1, wide_out, preferred_element_type=jnp.float32)
        .astype(jnp.bfloat16)
        .reshape(slot_count, span_len, width)
    )
    zero_rows = jnp.zeros((slot_count, span_len, width), jnp.float32)
    delta_rows = jnp.einsum("sqhd,shqd->shq", heads_view(grad_att).astype(jnp.float32), attended)

    def key_turn(turn_id, run_state):
        key_cur, value_cur, grad_keys, grad_values, grad_query = run_state
        key_start = (my_index - turn_id) % cycle_size * span_len
        key_ok = (key_start + jnp.arange(span_len, dtype=jnp.int32))[None, :] < lengths[:, None]
        part_q, part_k, part_v = block_grads(
            queries, grad_att, log_total, delta_rows, key_cur, value_cur, key_ok
        )
        key_cur, value_cur = shifted((key_cur, value_cur), "seq", 1)
        grad_keys, grad_values = (
            shifted((grad_keys + part_k).astype(jnp.bfloat16), "seq", 1).astype(jnp.float32),
            shifted((grad_values + part_v).astype(jnp.bfloat16), "seq", 1).astype(jnp.float32),
        )
        return (key_cur, value_cur, grad_keys, grad_values, grad_query + part_q)

    key_cur, value_cur, grad_keys, grad_values, grad_query = lax.fori_loop(
        0, cycle_size - 1, key_turn, (keys_rot, values, zero_rows, zero_rows, zero_rows)
    )
    key_start = (my_index - (cycle_size - 1)) % cycle_size * span_len
    key_ok = (key_start + jnp.arange(span_len, dtype=jnp.int32))[None, :] < lengths[:, None]
    part_q, part_k, part_v = block_grads(
        queries, grad_att, log_total, delta_rows, key_cur, value_cur, key_ok
    )
    grad_query = grad_query + part_q
    grad_keys, grad_values = (
        shifted((grad_keys + part_k).astype(jnp.bfloat16), "seq", 1).astype(jnp.float32),
        shifted((grad_values + part_v).astype(jnp.bfloat16), "seq", 1).astype(jnp.float32),
    )
    query_back = rotate(heads_view(grad_query), cos_four, -sin_four)
    key_back = rotate(heads_view(grad_keys), cos_four, -sin_four)
    grad_qkv = jnp.stack([query_back, key_back, heads_view(grad_values)], axis=2)
    grad_qkv = grad_qkv.reshape(row_count, 3 * width).astype(jnp.bfloat16)
    grad_wqkv = jnp.einsum("rd,re->de", flat_tokens, grad_qkv, preferred_element_type=jnp.float32)
    grad_tokens = grad_res1 + jnp.einsum(
        "re,de->rd", grad_qkv, wide_qkv, preferred_element_type=jnp.float32
    )
    grad_tokens = grad_tokens.astype(jnp.bfloat16).reshape(slot_count, span_len, width)
    grad_norm = jnp.stack([gain_one_grad, bias_one_grad, gain_two_grad, bias_two_grad], axis=0)
    col_qkv, col_out, col_gate, col_up, col_down, col_norm = (
        lax.psum_scatter(
            grad_wqkv.astype(jnp.bfloat16), "dp", scatter_dimension=1, tiled=True
        ).astype(jnp.float32),
        lax.psum_scatter(
            grad_wout.astype(jnp.bfloat16), "dp", scatter_dimension=1, tiled=True
        ).astype(jnp.float32),
        lax.psum_scatter(
            grad_wgate.astype(jnp.bfloat16), "dp", scatter_dimension=1, tiled=True
        ).astype(jnp.float32),
        lax.psum_scatter(
            grad_wup.astype(jnp.bfloat16), "dp", scatter_dimension=1, tiled=True
        ).astype(jnp.float32),
        lax.psum_scatter(
            grad_wdown.astype(jnp.bfloat16), "dp", scatter_dimension=1, tiled=True
        ).astype(jnp.float32),
        lax.psum_scatter(
            grad_norm.astype(jnp.bfloat16), "dp", scatter_dimension=1, tiled=True
        ).astype(jnp.float32),
    )
    own_qkv, own_out, own_gate, own_up, own_down, own_norm = (
        lax.psum_scatter(
            col_qkv.astype(jnp.bfloat16), "seq", scatter_dimension=0, tiled=True
        ).astype(jnp.float32),
        lax.psum_scatter(
            col_out.astype(jnp.bfloat16), "seq", scatter_dimension=0, tiled=True
        ).astype(jnp.float32),
        lax.psum_scatter(
            col_gate.astype(jnp.bfloat16), "seq", scatter_dimension=0, tiled=True
        ).astype(jnp.float32),
        lax.psum_scatter(
            col_up.astype(jnp.bfloat16), "seq", scatter_dimension=0, tiled=True
        ).astype(jnp.float32),
        lax.psum_scatter(
            col_down.astype(jnp.bfloat16), "seq", scatter_dimension=0, tiled=True
        ).astype(jnp.float32),
        lax.psum_scatter(
            col_norm.astype(jnp.bfloat16), "seq", scatter_dimension=1, tiled=True
        ).astype(jnp.float32),
    )
    return (output, grad_tokens, own_qkv, own_out, own_gate, own_up, own_down, own_norm)


MESH = pl.DeviceIdType.MESH
CHIPS, ZS = 16, 4
OFFSETS = sorted(((dx, dy, dz) for dx in (0, 1) for dy in (0, 1) for dz in range(-3, 4)),
                 key=lambda o: (2 * (o[0] + o[1]) + abs(o[2]), abs(o[2]), o))


def pick(index, values):
    out = jnp.int32(0)
    for position, value in enumerate(values):
        if value:
            out = out + jnp.where(index == position, jnp.int32(value), 0)
    return out


def spread(order, dx, dy, dz):
    zero = {"x": dx == 0, "y": dy == 0, "z": dz == 0}
    flags = {}
    for position, axis in enumerate(order):
        flag = zero[axis] if axis != "z" else None
        for later in order[position + 1:]:
            flag = zero[later] if flag is None else flag & zero[later]
        flags[axis] = flag
    up, down = dz <= 0, dz >= 0
    if flags["z"] is not None:
        up, down = up & flags["z"], down & flags["z"]
    return flags["x"], flags["y"], up, down


def place():
    core, chip = lax.axis_index("dp"), lax.axis_index("seq")
    return core, chip, chip % 2, (chip // 2) % 2, chip // 4


def chip_at(x, y, z):
    return (z * 2 + y) * 2 + x


def meet_all(core, chip):
    barrier = pltpu.get_barrier_semaphore()
    me = core * CHIPS + chip

    def greet(step, carry):
        other = (me + step) % (2 * CHIPS)
        pl.semaphore_signal(barrier, inc=1, device_id={"dp": other // CHIPS, "seq": other % CHIPS}, device_id_type=MESH)
        return carry

    lax.fori_loop(1, 2 * CHIPS, greet, 0)
    pl.semaphore_wait(barrier, 2 * CHIPS - 1)


def onward(order, dx, dy, dz):
    zero = {"x": dx == 0, "y": dy == 0, "z": dz == 0}
    links = []
    for position, axis in enumerate(order):
        if all(zero[later] for later in order[position + 1:]):
            if axis == "z":
                links += [2] * (dz <= 0) + [3] * (dz >= 0)
            elif zero[axis]:
                links.append("xy".index(axis))
    return links


def when(condition, action):
    if condition is True:
        action()
    else:
        pl.when(condition)(action)


LOW, F32 = jnp.bfloat16, jnp.float32
EPS = 1e-12
HEAD = 64
LANES = 128
GROUP = 256
FULL = pl.BlockSpec(memory_space=pltpu.VMEM)


def nn(a, b):
    return jnp.dot(a, b, preferred_element_type=F32)


def nt(a, b):
    return lax.dot_general(a, b, (((1,), (1,)), ((), ())), preferred_element_type=F32)


def tn(a, b):
    return lax.dot_general(a, b, (((0,), (0,)), ((), ())), preferred_element_type=F32)


def lane_of(shape):
    return lax.broadcasted_iota(jnp.int32, shape, 1)


def turn(u):
    parts = []
    for start in range(0, u.shape[1], LANES):
        part = u[:, start:start + LANES]
        first = lane_of(part.shape) % HEAD < HEAD // 2
        parts.append(jnp.where(first, pltpu.roll(part, LANES - HEAD // 2, 1), pltpu.roll(part, HEAD // 2, 1)))
    return jnp.concatenate(parts, 1)


def ln_parts(u):
    center = u - jnp.mean(u, axis=1, keepdims=True)
    inv = lax.rsqrt(jnp.mean(center * center, axis=1, keepdims=True) + EPS)
    return center * inv, inv


def ln_back(g, n, inv):
    return inv * (g - jnp.mean(g, axis=1, keepdims=True) - n * jnp.mean(g * n, axis=1, keepdims=True))


def middle_kernel(tiles, x_ref, att_ref, wo_ref, wg_ref, wu_ref, wd_ref, cot_ref, ln_ref, bias_ref,
                  y_ref, dwg_ref, dwu_ref, dwd_ref, dwo_ref, gatt_ref, gres_ref, dln_ref,
                  n1_ref, inv1_ref, hid_ref, hidt_ref, gate_ref, up_ref, acc_ref, gb_ref):
    index = pl.program_id(0)
    width = x_ref.shape[1]
    half = width // 2
    rows = att_ref.shape[0]
    mine = pl.ds(pl.multiple_of(lax.axis_index("dp") * rows, rows), rows)

    def wide(ref):
        return jnp.concatenate([ref[0], ref[1]], 1)

    @pl.when(index == 0)
    def _():
        n1, inv1 = ln_parts(x_ref[mine, :].astype(F32) + nn(att_ref[...], wide(wo_ref)))
        hidden = n1 * ln_ref[0:1, :] + ln_ref[1:2, :]
        n1_ref[...] = n1
        inv1_ref[...] = jnp.broadcast_to(inv1, inv1_ref.shape)
        acc_ref[...] = hidden
        low = hidden.astype(LOW)
        hid_ref[...] = low
        hidt_ref[...] = low.T

    tile = wg_ref.shape[2]
    f = jnp.where(index < tiles, index, index - tiles)
    cols = pl.ds(pl.multiple_of(f * tile, tile), tile)

    @pl.when(index < tiles)
    def _():
        gate, up = nn(hid_ref[...], wg_ref[0]), nn(hid_ref[...], wu_ref[0])
        gate_ref[:, cols] = gate
        up_ref[:, cols] = up
        acc_ref[...] += nn((gate * jax.nn.sigmoid(gate) * up).astype(LOW), wide(wd_ref))

    @pl.when(index == tiles - 1)
    def _():
        n2, inv2 = ln_parts(acc_ref[...])
        valid = jnp.where(bias_ref[mine, 0:1] == 0.0, 1.0, 0.0)
        y_ref[...] = ((n2 * ln_ref[2:3, :] + ln_ref[3:4, :]) * valid).astype(LOW)
        g_y = cot_ref[...].astype(F32) * valid
        dln_ref[2:3, :] = jnp.sum(g_y * n2, axis=0, keepdims=True)
        dln_ref[3:4, :] = jnp.sum(g_y, axis=0, keepdims=True)
        g_res2 = ln_back(g_y * ln_ref[2:3, :], n2, inv2)
        acc_ref[...] = g_res2
        gb_ref[...] = g_res2.astype(LOW)

    @pl.when(index >= tiles)
    def _():
        gate, up = gate_ref[:, cols], up_ref[:, cols]
        sig = jax.nn.sigmoid(gate)
        act = gate * sig
        gb = gb_ref[...]
        dwd = tn((act * up).astype(LOW), gb)
        dwd_ref[0] = dwd[:, :half].astype(LOW)
        dwd_ref[1] = dwd[:, half:].astype(LOW)
        g_inner = nt(gb, wide(wd_ref))
        g_gate = (g_inner * up * sig * (1.0 + gate * (1.0 - sig))).astype(LOW)
        g_up = (g_inner * act).astype(LOW)
        dwg_ref[0] = nn(hidt_ref[...], g_gate).astype(LOW)
        dwu_ref[0] = nn(hidt_ref[...], g_up).astype(LOW)
        acc_ref[...] += nt(g_gate, wg_ref[0]) + nt(g_up, wu_ref[0])

    @pl.when(index == 2 * tiles - 1)
    def _():
        g_hidden, n1 = acc_ref[...], n1_ref[...]
        dln_ref[0:1, :] = jnp.sum(g_hidden * n1, axis=0, keepdims=True)
        dln_ref[1:2, :] = jnp.sum(g_hidden, axis=0, keepdims=True)
        g_res1 = ln_back(g_hidden * ln_ref[0:1, :], n1, inv1_ref[:, 0:1])
        gres_ref[...] = g_res1
        gb1 = g_res1.astype(LOW)
        dwo = tn(att_ref[...], gb1)
        dwo_ref[0] = dwo[:, :half].astype(LOW)
        dwo_ref[1] = dwo[:, half:].astype(LOW)
        gatt_ref[...] = nt(gb1, wide(wo_ref)).astype(LOW)


def middle(x, att, wo, wg, wu, wd, cot, ln, bias_col):
    rows, width = att.shape
    hidden = wd.shape[1]
    tile = 512
    tiles = hidden // tile
    per = wg.shape[2] // tile
    at = lambda i: jnp.where(i < tiles, i, i - tiles)
    late = lambda i: jnp.maximum(i - tiles, 0)
    cols = lambda pick: pl.BlockSpec((1, width, tile), lambda i: (pick(i) // per, 0, pick(i) % per))
    rowb = lambda pick: pl.BlockSpec((2, tile, wd.shape[2]), lambda i: (0, pick(i), 0))
    sds = jax.ShapeDtypeStruct
    return pl.pallas_call(
        functools.partial(middle_kernel, tiles), grid=(2 * tiles,),
        out_shape=[sds((rows, width), LOW), sds(wg.shape, LOW), sds(wu.shape, LOW), sds(wd.shape, LOW), sds((2, width, width // 2), LOW),
                   sds((rows, width), LOW), sds((rows, width), F32), sds((8, width), F32)],
        in_specs=[FULL, FULL, pl.BlockSpec((2, width, width // 2), lambda i: (0, 0, 3)), cols(at), cols(at), rowb(at), FULL, FULL, FULL],
        out_specs=[FULL, cols(late), cols(late), rowb(late), FULL, FULL, FULL, FULL],
        scratch_shapes=[pltpu.VMEM((rows, width), F32), pltpu.VMEM((rows, LANES), F32), pltpu.VMEM((rows, width), LOW),
                        pltpu.VMEM((width, rows), LOW), pltpu.VMEM((rows, hidden), F32), pltpu.VMEM((rows, hidden), F32),
                        pltpu.VMEM((rows, width), F32), pltpu.VMEM((rows, width), LOW)],
        compiler_params=pltpu.CompilerParams(vmem_limit_bytes=60 << 20),
        cost_estimate=pl.CostEstimate(flops=24 * 10**9, bytes_accessed=6 * 10**7, transcendentals=3 * 10**6),
        name="middle")(x, att, wo, wg, wu, wd, cot, ln, bias_col)


def finish_kernel(count, *refs):
    sources, targets, holds, (in_sem, out_sem) = refs[:count], refs[count:2 * count], refs[2 * count:3 * count], refs[3 * count:]
    loads = [pltpu.make_async_copy(source, hold, in_sem.at[n]) for n, (source, hold) in enumerate(zip(sources, holds))]
    stores = [pltpu.make_async_copy(hold, target, out_sem.at[n]) for n, (hold, target) in enumerate(zip(holds, targets))]
    for load in loads:
        load.start()
    for load, store in zip(loads, stores):
        load.wait()
        store.start()
    for store in stores:
        store.wait()


def finish(results):
    count = len(results)
    anywhere = pl.BlockSpec(memory_space=pl.ANY)
    return pl.pallas_call(
        functools.partial(finish_kernel, count), out_shape=[jax.ShapeDtypeStruct(r.shape, r.dtype) for r in results],
        in_specs=[anywhere] * count, out_specs=[anywhere] * count,
        scratch_shapes=[pltpu.VMEM(r.shape, r.dtype) for r in results] + [pltpu.SemaphoreType.DMA((count,))] * 2,
        name="finish")(*results)

FIRST_ORDERS = ("yzx", "xzy", "zyx", "zxy")
REST_ORDERS = ("xzy", "zyx", "zyx")
REST_STARTS = (12, 6, 0)
REST_MIXES = 20
TOKENS_AT = (1, 4, 7, 10, 13, 16, 18, 20)
COTS_AT = (2, 3, 4, 5, 6, 7, 8, 9)
CHUNK = 256


def front_kernel(tok, cot, w_qkv, w_out, w_gate, w_up, w_down, ln_in, len_in, turns_far, turns_near,
                 x_all, c_own, ln_out, w_first, wide_gate, wide_up, wide_down, q_out, k_out, v_out, att_out, cos_out, sin_out, bias_out, *refs):
    (xv, wv, qv, kv, vv, attv, cosv, sinv, biasv, rowv, small, smalls, lnv), refs = refs[:13], refs[13:]
    (first_send, first_recv, first_sib, rest_send, rest_recv, rest_sib, own_sem, tok_send, tok_recv, tok_sib, cot_recv,
     small_send, small_recv, out_sem) = refs
    core, chip, x, y, z = place()
    other = 1 - core
    slots, span = tok.shape[0], tok.shape[1]
    half = CHIPS // 2
    me = core * CHIPS + chip
    rows, width = qv.shape
    can = (True, True, z < ZS - 1, z > 0, True)
    neighbours = (
        {"dp": core, "seq": chip_at(1 - x, y, z)},
        {"dp": core, "seq": chip_at(x, 1 - y, z)},
        {"dp": core, "seq": chip_at(x, y, jnp.minimum(z + 1, ZS - 1))},
        {"dp": core, "seq": chip_at(x, y, jnp.maximum(z - 1, 0))},
        {"dp": other, "seq": chip},
    )
    shards, wides = (w_gate, w_up, w_down), (wide_gate, wide_up, wide_down)
    n_first = w_out.shape[0]
    c_first = w_out.shape[1]

    def first_region(n, owner, source):
        return wv.at[owner, pl.ds(pl.multiple_of(source * n_first, n_first), n_first), n * c_first:n * c_first + c_first]

    def first_own(n):
        return w_out if n == 3 else w_qkv.at[:, n * c_first:n * c_first + c_first]

    def rest_region(m, owner, source):
        size = shards[m].shape[0]
        return wides[m].at[owner, pl.ds(pl.multiple_of(source * size, size), size)]

    def first_piece(n, source, link, own=False):
        target = first_region(n, core, source)
        return pltpu.make_async_remote_copy(
            src_ref=first_own(n) if own else target, dst_ref=target, send_sem=first_send.at[n, link, source],
            recv_sem=first_sib.at[n, source] if link == 4 else first_recv.at[n, source],
            device_id=neighbours[link], device_id_type=MESH)

    def rest_piece(m, source, link, own=False):
        target = rest_region(m, core, source)
        return pltpu.make_async_remote_copy(
            src_ref=shards[m] if own else target, dst_ref=target, send_sem=rest_send.at[m, link, source],
            recv_sem=rest_sib.at[m, source] if link == 4 else rest_recv.at[m, source],
            device_id=neighbours[link], device_id_type=MESH)

    def valid(offset):
        dz = offset[2]
        return True if dz == 0 else (z < ZS - dz if dz > 0 else z >= -dz)

    def source_at(offset):
        return chip_at((x + offset[0]) % 2, (y + offset[1]) % 2, z + offset[2])

    def arrive(piece, orders, offset):
        def one():
            source = source_at(offset)
            for m, order in enumerate(orders):
                piece(m, source, 0).wait_recv()
                for link in onward(order, *offset) + [4]:
                    when(can[link], piece(m, source, link).start)
        when(valid(offset), one)

    def send_own(piece, orders, m):
        for link in onward(orders[m], 0, 0, 0) + [4]:
            when(can[link], piece(m, chip, link, own=True).start)

    def drain(piece, orders):
        for offset in OFFSETS:
            def one():
                source = source_at(offset)
                for m, order in enumerate(orders):
                    for link in onward(order, *offset) + [4]:
                        when(can[link], piece(m, source, link).wait_send)
            when(valid(offset), one)

    def rows_of(ref, index):
        return ref.at[pl.ds(pl.multiple_of(index * span, span), span)]

    def deliver(j, source, target, sends, recvs):
        slot = (chip + 1 + j) % half
        to = core * half + slot
        src, dst = source.at[slot], target
        self_copy = (chip // half == core) & (to == chip)

        @pl.when(self_copy)
        def _():
            pltpu.make_async_copy(src, dst, recvs.at[chip % half]).start()

        @pl.when(jnp.logical_not(self_copy))
        def _():
            pltpu.make_async_remote_copy(
                src_ref=src, dst_ref=dst, send_sem=sends.at[slot], recv_sem=recvs.at[chip % half],
                device_id={"dp": chip // half, "seq": to}, device_id_type=MESH).start()

    def small_to(step):
        to = (me + step) % (2 * CHIPS)
        return pltpu.make_async_remote_copy(
            src_ref=small, dst_ref=smalls.at[me], send_sem=small_send.at[step], recv_sem=small_recv.at[me],
            device_id={"dp": to // CHIPS, "seq": to % CHIPS}, device_id_type=MESH)

    lane = lax.broadcasted_iota(jnp.int32, (1, LANES), 1)
    counts = jnp.zeros((1, LANES), F32)
    for j in range(slots):
        counts = counts + jnp.where(lane == j, len_in[j].astype(F32), 0.0)
    small[...] = jnp.zeros_like(small)
    small[0:ln_in.shape[0], 0:ln_in.shape[1]] = ln_in[...].astype(F32)
    small[4:5, :] = counts
    meet_all(core, chip)

    for n in range(4):
        send_own(first_piece, FIRST_ORDERS, n)
        pltpu.make_async_copy(first_own(n), first_region(n, core, chip), own_sem.at[n]).start()
    lax.fori_loop(1, 2 * CHIPS, lambda s, c: (small_to(s).start(), c)[1], 0)
    own_small = pltpu.make_async_copy(small, smalls.at[me], small_recv.at[me])
    own_small.start()

    sign = jnp.where(lane % HEAD < HEAD // 2, -1.0, 1.0).astype(F32)
    near = turns_near.shape[1]
    for far in range(turns_far.shape[1]):
        part = slice(far * near, far * near + near)
        ca, sa = turns_far[0, far:far + 1, :], turns_far[1, far:far + 1, :]
        cosv[part, :] = ca * turns_near[0] - sa * turns_near[1]
        sinv[part, :] = (sa * turns_near[0] + ca * turns_near[1]) * sign

    def relay(i, carry):
        block = rows_of(xv, core * half + i)
        pltpu.make_async_copy(block, block, tok_recv.at[i]).wait()
        pltpu.make_async_remote_copy(
            src_ref=block, dst_ref=block, send_sem=tok_send.at[2, i], recv_sem=tok_sib.at[i],
            device_id=neighbours[4], device_id_type=MESH).start()
        return carry

    waiting = list(OFFSETS[1:])
    for index, offset in enumerate(OFFSETS[1:]):
        for j in range(half):
            if index == TOKENS_AT[j]:
                deliver(j, tok, rows_of(xv, chip), tok_send.at[0], tok_recv)
        for m in range(3):
            if index == REST_STARTS[m]:
                send_own(rest_piece, REST_ORDERS, m)
                pltpu.make_async_copy(shards[m], rest_region(m, core, chip), own_sem.at[4 + m]).start()
        arrive(first_piece, FIRST_ORDERS, offset)
        if index >= REST_MIXES:
            arrive(rest_piece, REST_ORDERS, waiting.pop(0))

    def first_in(source, carry):
        for n in range(4):
            block = first_region(n, other, source)
            pltpu.make_async_copy(block, block, first_sib.at[n, source]).wait()
        return carry

    def small_in(step, carry):
        source = (me + step) % (2 * CHIPS)
        pltpu.make_async_copy(smalls.at[source], smalls.at[source], small_recv.at[source]).wait()
        return carry

    def tok_in(i, carry):
        block = rows_of(xv, other * half + i)
        pltpu.make_async_copy(block, block, tok_sib.at[i]).wait()
        return carry

    lax.fori_loop(0, half, relay, 0)
    lax.fori_loop(0, half, tok_in, 0)
    lax.fori_loop(0, CHIPS, first_in, 0)
    for n in range(4):
        pltpu.make_async_copy(first_own(n), first_region(n, core, chip), own_sem.at[n]).wait()
    lax.fori_loop(1, 2 * CHIPS, small_in, 0)
    own_small.wait()
    norms, share = ln_in.shape
    lnv[...] = jnp.zeros_like(lnv)
    lnv[0:norms, :] = jnp.concatenate([smalls[device, 0:norms, 0:share] for device in range(2 * CHIPS)], 1)
    counted = smalls[chip // half * CHIPS, 4:5, :]
    length = jnp.sum(jnp.where(lane == chip % half, counted, 0.0), axis=1, keepdims=True)
    at_row = lax.broadcasted_iota(jnp.int32, biasv.shape, 0).astype(F32)
    biasv[...] = jnp.where(at_row < length, 0.0, masked_score)
    at_lane = lax.broadcasted_iota(jnp.int32, rowv.shape, 1).astype(F32)
    rowv[...] = jnp.where(at_lane < length, 0.0, masked_score)
    outs = [pltpu.make_async_copy(source, target, out_sem.at[n]) for n, (source, target) in enumerate((
        (xv, x_all), (wv, w_first), (lnv, ln_out), (cosv, cos_out), (sinv, sin_out), (biasv, bias_out),
        (qv, q_out), (kv, k_out), (vv, v_out), (attv, att_out)))]
    for copy in outs[:6]:
        copy.start()

    mine = pl.ds(pl.multiple_of(core * rows, rows), rows)
    blocks = width // LANES
    per = 3 * blocks // 2

    def weights(block):
        return jnp.concatenate([wv[b // per, :, pl.ds(pl.multiple_of(b % per * LANES, LANES), LANES)] for b in (block, block + 1)], 1)

    def turned(u, cos, sin):
        return u * jnp.concatenate([cos, cos], 1) + turn(u) * jnp.concatenate([sin, sin], 1)

    per_group = (GROUP // LANES) * (rows // CHUNK)
    chunks = width // GROUP * per_group

    def chunk(index, carry):
        group, inner = index // per_group, index % per_group
        cols = pl.ds(pl.multiple_of(group * GROUP, GROUP), GROUP)

        @pl.when(inner == 0)
        def _():
            q = turned(nn(xv[mine, :], weights(2 * group)), cosv[mine, :], sinv[mine, :]).astype(LOW)
            qv[:, cols] = q * jnp.asarray(0.125, LOW)
            kv[:, cols] = turned(nn(xv[...], weights(blocks + 2 * group)), cosv[...], sinv[...]).astype(LOW)
            vv[:, cols] = nn(xv[...], weights(2 * blocks + 2 * group)).astype(LOW)

        pair, block = inner // (rows // CHUNK), inner % (rows // CHUNK)
        here = pl.ds(pl.multiple_of(block * CHUNK, CHUNK), CHUNK)
        lanes = pl.ds(pl.multiple_of(group * GROUP + pair * LANES, LANES), LANES)
        qp, kp, vp = qv[here, lanes], kv[:, lanes], vv[:, lanes]
        low = lane_of(qp.shape) < HEAD
        parts = []
        for head in range(2):
            qm = jnp.where(low if head == 0 else jnp.logical_not(low), qp, jnp.zeros_like(qp))
            s = nt(qm, kp) + rowv[0:1, :]
            p = jnp.exp(s - jnp.max(s, axis=1, keepdims=True))
            total = jnp.sum(p, axis=1, keepdims=True)
            parts.append(nn(p.astype(LOW), vp) / total)
        attv[here, lanes] = jnp.where(low, parts[0], parts[1]).astype(LOW)

        for k in range(chunks):
            @pl.when(index == k)
            def _():
                for j in range(half):
                    if k == COTS_AT[j]:
                        deliver(j, cot, rows_of(c_own, chip % half), tok_send.at[1], cot_recv)
                if waiting:
                    arrive(rest_piece, REST_ORDERS, waiting.pop(0))
        return carry

    lax.fori_loop(0, chunks, chunk, 0)
    for copy in outs[6:]:
        copy.start()
    while waiting:
        arrive(rest_piece, REST_ORDERS, waiting.pop(0))

    def ends(i, carry):
        block = rows_of(c_own, i)
        pltpu.make_async_copy(block, block, cot_recv.at[i]).wait()
        block = rows_of(xv, core * half + i)
        pltpu.make_async_copy(block, block, tok_send.at[2, i]).wait()
        self_copy = (chip // half == core) & (core * half + i == chip)

        @pl.when(jnp.logical_not(self_copy))
        def _():
            pltpu.make_async_copy(tok.at[i], tok.at[i], tok_send.at[0, i]).wait()
            pltpu.make_async_copy(cot.at[i], cot.at[i], tok_send.at[1, i]).wait()
        return carry

    def rest_in(source, carry):
        for m in range(3):
            block = rest_region(m, other, source)
            pltpu.make_async_copy(block, block, rest_sib.at[m, source]).wait()
        return carry

    lax.fori_loop(1, 2 * CHIPS, lambda s, c: (small_to(s).wait_send(), c)[1], 0)
    lax.fori_loop(0, half, ends, 0)
    drain(first_piece, FIRST_ORDERS)
    drain(rest_piece, REST_ORDERS)
    lax.fori_loop(0, CHIPS, rest_in, 0)
    for m in range(3):
        pltpu.make_async_copy(shards[m], rest_region(m, core, chip), own_sem.at[4 + m]).wait()
    for copy in outs:
        copy.wait()


def front(tokens, cotangent, w_qkv, w_out, w_gate, w_up, w_down, ln_params, lengths, turns_far, turns_near):
    slots, span, width = tokens.shape
    total, rows = span * CHIPS, span * CHIPS // 2
    sds, mem, dma = jax.ShapeDtypeStruct, pltpu.VMEM, pltpu.SemaphoreType.DMA
    anywhere, vmem, smem = (pl.BlockSpec(memory_space=s) for s in (pl.ANY, pltpu.VMEM, pltpu.SMEM))
    wide = lambda w: sds((2, w.shape[0] * CHIPS, w.shape[1]), LOW)
    first = (2, width, w_qkv.shape[1] + w_out.shape[1])
    table, small = (total, LANES), (8, LANES)
    outs = [sds((total, width), LOW), sds((rows, width), LOW), sds((8, width), F32), sds(first, LOW),
            wide(w_gate), wide(w_up), wide(w_down), sds((rows, width), LOW), sds((total, width), LOW), sds((total, width), LOW),
            sds((rows, width), LOW), sds(table, F32), sds(table, F32), sds(table, F32)]
    return pl.pallas_call(
        front_kernel,
        out_shape=outs,
        in_specs=[anywhere] * 7 + [vmem, smem, vmem, vmem],
        out_specs=[anywhere] * len(outs),
        scratch_shapes=[
            mem((total, width), LOW), mem(first, LOW), mem((rows, width), LOW), mem((total, width), LOW), mem((total, width), LOW),
            mem((rows, width), LOW), mem(table, F32), mem(table, F32), mem(table, F32), mem((8, total), F32), mem(small, F32),
            mem((2 * CHIPS,) + small, F32), mem((8, width), F32),
            dma((4, 5, CHIPS)), dma((4, CHIPS)), dma((4, CHIPS)), dma((3, 5, CHIPS)), dma((3, CHIPS)), dma((3, CHIPS)), dma((7,)),
            dma((3, 8)), dma((8,)), dma((8,)), dma((8,)), dma((2 * CHIPS,)), dma((2 * CHIPS,)), dma((10,))],
        compiler_params=pltpu.CompilerParams(collective_id=0, has_side_effects=True, vmem_limit_bytes=60 << 20),
        name="front",
    )(tokens, cotangent, w_qkv, w_out, w_gate, w_up, w_down, ln_params, lengths, turns_far, turns_near)

BACK_ORDERS = ("xzy", "zyx", "zyx")
LATE_ORDERS = ("zxy", "zyx", "zxy")
FAR_FIRST = OFFSETS[::-1]
SIDES = {"x": 2, "y": 2, "z": ZS}


def landing_slots(order):
    sizes, room = {}, 1
    for axis in order:
        sizes[axis] = room * (ZS if axis == "z" else 1)
        room *= SIDES[axis]
    return sizes["x"], sizes["y"], sizes["z"], sizes["z"]


def landing_index(order, link, x, y, z):
    axis = "xyzz"[link]
    index = 0
    for before in order:
        if before == axis:
            break
        index = index * SIDES[before] + {"x": x, "y": y, "z": z}[before]
    return index * ZS + z if axis == "z" else index


def back_scatter_kernel(y_own, dwg, dwu, dwd, dwo, dsmall, x_in, w_in, q_in, k_in, v_in, g_in, res_in, cos_in, sin_in, bias_in,
                        y_out, gt_out, f_gate, f_up, f_down, f_out, f_qkv, f_small, *refs):
    (xv, wv, qv, kv, vv, gv, own_acc, cosv, sinv, biasv, xt, oth_acc, dq, dk, dv, dw), refs = refs[:16], refs[16:]
    owns, refs = refs[:3], refs[3:]
    sibs, refs = refs[:4], refs[4:]
    down_out, refs = refs[0], refs[1:]
    lands, refs = refs[:24], refs[24:]
    (gt_low, gt_sib, smalls), refs = refs[:3], refs[3:]
    (in_sem, send_sem, recv_sem, sib_send, sib_recv, own_sem, late_send, late_recv, late_sib_send, late_sib_recv,
     gt_sem, tok_send, y_recv, gt_recv, small_send, small_recv) = refs
    core, chip, x, y, z = place()
    other = 1 - core
    half = CHIPS // 2
    me = core * CHIPS + chip
    span = y_out.shape[1]
    rows = qv.shape[0]
    mine = pl.ds(pl.multiple_of(core * rows, rows), rows)
    theirs = pl.ds(pl.multiple_of(other * rows, rows), rows)
    neighbours = (
        {"dp": core, "seq": chip_at(1 - x, y, z)},
        {"dp": core, "seq": chip_at(x, 1 - y, z)},
        {"dp": core, "seq": chip_at(x, y, jnp.minimum(z + 1, ZS - 1))},
        {"dp": core, "seq": chip_at(x, y, jnp.maximum(z - 1, 0))},
    )
    sibling = {"dp": other, "seq": chip}

    loads = [pltpu.make_async_copy(source, target, in_sem.at[n]) for n, (source, target) in enumerate((
        (k_in, kv), (q_in, qv), (bias_in, biasv), (v_in, vv), (g_in, gv), (x_in, xv), (w_in, wv), (res_in, own_acc), (cos_in, cosv), (sin_in, sinv)))]
    for load in loads:
        load.start()

    def cut(ref, size, index):
        return ref.at[pl.ds(pl.multiple_of(index * size, size), size)]

    rows_gate, rows_down, rows_out = f_gate.shape[0], f_down.shape[0], f_out.shape[0]

    def parts(m, owner, dest):
        if m == 0:
            return [(cut(dwg.at[owner], rows_gate, dest), 0, rows_gate)]
        if m == 1:
            return [(cut(dwu.at[owner], rows_gate, dest), 0, rows_gate)]
        return [(cut(dwd.at[owner], rows_down, dest), 0, rows_down), (cut(dwo.at[owner], rows_out, dest), rows_down, rows_out)]

    def to_sibling(m, dest):
        return [pltpu.make_async_remote_copy(
            src_ref=source, dst_ref=sibs[m].at[dest, pl.ds(start, size)], send_sem=sib_send.at[m + n, dest],
            recv_sem=sib_recv.at[m + n, dest], device_id=sibling, device_id_type=MESH)
            for n, (source, start, size) in enumerate(parts(m, other, dest))]

    def own_load(m, dest, slot):
        return [pltpu.make_async_copy(source, owns[m].at[slot, pl.ds(start, size)], own_sem.at[m + n, slot])
                for n, (source, start, size) in enumerate(parts(m, core, dest))]

    def dest_of(index):
        dx = pick(index, [o[0] for o in FAR_FIRST])
        dy = pick(index, [o[1] for o in FAR_FIRST])
        dz = pick(index, [o[2] for o in FAR_FIRST])
        return dx, dy, dz, (z + dz >= 0) & (z + dz < ZS), (x + dx) % 2, (y + dy) % 2, jnp.clip(z + dz, 0, ZS - 1)

    meet_all(core, chip)

    def begin(index, carry):
        dx, dy, dz, valid, tx, ty, tz = dest_of(index)

        @pl.when(valid)
        def _():
            for m in range(3):
                for copy in to_sibling(m, chip_at(tx, ty, tz)):
                    copy.start()
        return carry

    lax.fori_loop(0, len(FAR_FIRST), begin, 0)

    def prefetch(index):
        dx, dy, dz, valid, tx, ty, tz = dest_of(index)

        @pl.when(valid & (index < len(FAR_FIRST)))
        def _():
            for m in range(3):
                for copy in own_load(m, chip_at(tx, ty, tz), index % 3):
                    copy.start()

    prefetch(jnp.int32(0))
    prefetch(jnp.int32(1))

    def deliver(source, target, k, recvs):
        def one(j, carry):
            i = (chip + 1 + j) % half
            to_core, to_chip = chip // half, core * half + i
            src, dst = cut(source, span, i), target.at[chip % half]
            self_copy = (to_core == core) & (to_chip == chip)

            @pl.when(self_copy)
            def _():
                pltpu.make_async_copy(src, dst, recvs.at[chip % half]).start()

            @pl.when(jnp.logical_not(self_copy))
            def _():
                pltpu.make_async_remote_copy(
                    src_ref=src, dst_ref=dst, send_sem=tok_send.at[k, i], recv_sem=recvs.at[chip % half],
                    device_id={"dp": to_core, "seq": to_chip}, device_id_type=MESH).start()
            return carry

        lax.fori_loop(0, half, one, 0)

    def small_to(step):
        to = (me + step) % (2 * CHIPS)
        return pltpu.make_async_remote_copy(
            src_ref=dsmall.at[to], dst_ref=smalls.at[me], send_sem=small_send.at[step], recv_sem=small_recv.at[me],
            device_id={"dp": to // CHIPS, "seq": to % CHIPS}, device_id_type=MESH)

    deliver(y_own, y_out, 0, y_recv)
    lax.fori_loop(1, 2 * CHIPS, lambda s, c: (small_to(s).start(), c)[1], 0)
    own_small = pltpu.make_async_copy(dsmall.at[me], smalls.at[me], small_recv.at[me])
    own_small.start()

    def reduce_piece(order, lands_m, send_at, recv_at, own, acc, offset, target, last, final):
        dx, dy, dz = offset
        tx, ty, tz = target
        fx, fy, up, down = spread(order, dx, dy, dz)
        flags = (fx, fy, up & (z < ZS - 1), down & (z > 0))

        @pl.when(jnp.logical_not(last))
        def _():
            acc[...] += own()

        @pl.when(last)
        def _():
            final[...] = acc[...].astype(F32) + own().astype(F32)

        for link in range(4):
            land = lands_m[link].at[landing_index(order, link, tx, ty, tz)]

            @pl.when(flags[link])
            def _():
                pltpu.make_async_copy(land, land, recv_at(link)).wait()

            @pl.when(flags[link] & jnp.logical_not(last))
            def _():
                acc[...] += land[...]

            @pl.when(flags[link] & last)
            def _():
                final[...] += land[...].astype(F32)

        away = {"x": dx != 0, "y": dy != 0, "z": dz != 0}
        taken = None
        for axis in order[::-1]:
            here = away[axis] if taken is None else away[axis] & jnp.logical_not(taken)
            taken = away[axis] if taken is None else taken | away[axis]
            for link in {"x": (0,), "y": (1,), "z": (2, 3)}[axis]:
                go = here if axis != "z" else (here & (dz > 0 if link == 2 else dz < 0))
                there = {0: 0, 1: 1, 2: 3, 3: 2}[link]

                @pl.when(go)
                def _():
                    pltpu.make_async_remote_copy(
                        src_ref=acc, dst_ref=lands_m[there].at[landing_index(order, there, tx, ty, tz)],
                        send_sem=send_at, recv_sem=recv_at(there), device_id=neighbours[link], device_id_type=MESH).start()

    def early(index):
        dx, dy, dz, valid, tx, ty, tz = dest_of(index)
        last = index == len(FAR_FIRST) - 1
        prefetch(index + 2)

        @pl.when(valid)
        def _():
            dest = chip_at(tx, ty, tz)
            for m in range(3):
                for copy in own_load(m, dest, index % 3):
                    copy.wait()
                for copy in to_sibling(m, dest):
                    copy.wait_recv()
                reduce_piece(BACK_ORDERS[m], lands[4 * m:4 * m + 4], send_sem.at[m, dest], lambda link: recv_sem.at[m, link, dest],
                             lambda: owns[m][index % 3], sibs[m].at[dest], (dx, dy, dz), (tx, ty, tz), last, (f_gate, f_up, down_out)[m])

    step = 256
    per_group = (GROUP // LANES) * (rows // step) * 2
    groups = xv.shape[1] // GROUP
    chunks = groups * per_group
    blocks = xv.shape[1] // LANES
    for load in loads[:5]:
        load.wait()

    def chunk(index):
        group, inner = index // per_group, index % per_group
        pair, block, head = inner // (per_group // 2), inner // 2 % (rows // step), inner % 2
        here = pl.ds(pl.multiple_of(block * step, step), step)
        lanes = pl.ds(pl.multiple_of(group * GROUP + pair * LANES, LANES), LANES)
        out_lanes = pl.ds(pl.multiple_of(pair * LANES, LANES), LANES)

        @pl.when(inner == 0)
        def _():
            dq[...] = jnp.zeros_like(dq)
            dk[...] = jnp.zeros_like(dk)
            dv[...] = jnp.zeros_like(dv)

        qp, gp = qv[here, lanes], gv[here, lanes]
        keep = lane_of(qp.shape) // HEAD == head
        qm, gm = jnp.where(keep, qp, jnp.zeros_like(qp)), jnp.where(keep, gp, jnp.zeros_like(gp))
        kp, vp = kv[:, lanes], vv[:, lanes]
        s = nt(kp, qm) + jnp.concatenate([biasv[...]] * (step // LANES), 1)
        e = jnp.exp(s - jnp.max(s, axis=0, keepdims=True))
        p = e * (1.0 / jnp.sum(e, axis=0, keepdims=True))
        dp = nt(vp, gm)
        delta = jnp.sum(p * dp, axis=0, keepdims=True)
        ds = (p * (dp - delta)).astype(LOW)
        dv[:, out_lanes] += nn(p.astype(LOW), gm)
        dk[:, out_lanes] += nn(ds, qm)
        dq[here, out_lanes] += jnp.where(keep, tn(ds, kp), 0.0)

        @pl.when(index == per_group - 1)
        def _():
            for load in loads[5:]:
                load.wait()
            xt[...] = xv[...].T
            oth_acc[...] = jnp.zeros_like(oth_acc)

        @pl.when(inner == per_group - 1)
        def _():
            finish(group)

    def finish(group):
        def back(u, cos, sin):
            return u * jnp.concatenate([cos, cos], 1) - turn(u) * jnp.concatenate([sin, sin], 1)

        def put(block, value):
            per = dw.shape[2] // LANES
            for i in range(2):
                b = block + i
                dw[b // per, :, pl.ds(pl.multiple_of(b % per * LANES, LANES), LANES)] = value[:, i * LANES:i * LANES + LANES].astype(LOW)

        def weights(block):
            per = dw.shape[2] // LANES
            return jnp.concatenate([wv[b // per, :, pl.ds(pl.multiple_of(b % per * LANES, LANES), LANES)] for b in (block, block + 1)], 1)

        gq = back(dq[...] * 0.125, cosv[mine, :], sinv[mine, :]).astype(LOW)
        dk[...] = back(dk[...], cosv[...], sinv[...])
        put(2 * group, nn(xt[:, mine], gq))
        put(blocks + 2 * group, nn(xt[...], dk[...].astype(LOW)))
        put(2 * blocks + 2 * group, nn(xt[...], dv[...].astype(LOW)))
        wq, wk, wvv = (weights(n * blocks + 2 * group) for n in range(3))
        own_acc[...] += nt(gq, wq) + nt(dk[mine, :].astype(LOW), wk) + nt(dv[mine, :].astype(LOW), wvv)
        oth_acc[...] += nt(dk[theirs, :].astype(LOW), wk) + nt(dv[theirs, :].astype(LOW), wvv)

    def turn_of(index, carry):
        chunk(index)

        @pl.when(index < mixed)
        def _():
            early(index)
        return carry

    mixed = min(chunks, len(FAR_FIRST) - 4)
    lax.fori_loop(0, chunks, turn_of, 0)

    gt_low[...] = oth_acc[...].astype(LOW)
    third = f_qkv.shape[1] // len(LATE_ORDERS)

    def late_to_sibling(dest):
        return pltpu.make_async_remote_copy(
            src_ref=cut(dw.at[other], rows_gate, dest), dst_ref=sibs[3].at[dest], send_sem=late_sib_send.at[dest],
            recv_sem=late_sib_recv.at[dest], device_id=sibling, device_id_type=MESH)

    def late_begin(index, carry):
        dx, dy, dz, valid, tx, ty, tz = dest_of(index)

        @pl.when(valid)
        def _():
            late_to_sibling(chip_at(tx, ty, tz)).start()
        return carry

    lax.fori_loop(0, len(FAR_FIRST), late_begin, 0)
    cross = pltpu.make_async_remote_copy(src_ref=gt_low, dst_ref=gt_sib, send_sem=gt_sem.at[0], recv_sem=gt_sem.at[1],
                                         device_id=sibling, device_id_type=MESH)
    cross.start()

    def late(index, carry):
        dx, dy, dz, valid, tx, ty, tz = dest_of(index)
        last = index == len(FAR_FIRST) - 1

        @pl.when(valid)
        def _():
            dest = chip_at(tx, ty, tz)
            late_to_sibling(dest).wait_recv()
            for n, order in enumerate(LATE_ORDERS):
                lanes = slice(n * third, n * third + third)
                acc = sibs[3].at[dest, :, lanes]
                reduce_piece(order, lands[12 + 4 * n:16 + 4 * n], late_send.at[n, dest], lambda link: late_recv.at[n, link, dest],
                             lambda: dw[core, pl.ds(pl.multiple_of(dest * rows_gate, rows_gate), rows_gate), lanes],
                             acc, (dx, dy, dz), (tx, ty, tz), last, f_qkv.at[:, lanes])

        @pl.when((index % 2 == 1) & (mixed + index // 2 < len(FAR_FIRST)))
        def _():
            early(mixed + index // 2)
        return carry

    early_steps = 8
    lax.fori_loop(0, early_steps, late, 0)
    cross.wait()
    gt_low[...] = (own_acc[...] + gt_sib[...].astype(F32)).astype(LOW)
    deliver(gt_low, gt_out, 1, gt_recv)
    lax.fori_loop(early_steps, len(FAR_FIRST), late, 0)
    f_down[...] = down_out[0:rows_down, :]
    f_out[...] = down_out[rows_down:rows_down + rows_out, :]

    def small_end(s, carry):
        small_to(s).wait_send()
        source = (me + s) % (2 * CHIPS)
        pltpu.make_async_copy(smalls.at[source], smalls.at[source], small_recv.at[source]).wait()
        return carry

    lax.fori_loop(1, 2 * CHIPS, small_end, 0)
    own_small.wait()
    f_small[...] = jnp.sum(smalls[...], axis=0)

    def ends(i, carry):
        for out, recvs, k in ((y_out, y_recv, 0), (gt_out, gt_recv, 1)):
            pltpu.make_async_copy(out.at[i], out.at[i], recvs.at[i]).wait()
            self_copy = (chip // half == core) & (core * half + i == chip)

            @pl.when(jnp.logical_not(self_copy))
            def _():
                pltpu.make_async_copy(out.at[i], out.at[i], tok_send.at[k, i]).wait()
        return carry

    lax.fori_loop(0, half, ends, 0)

    def sent(dest, carry):
        for m in range(3):
            for copy in to_sibling(m, dest):
                copy.wait_send()
        late_to_sibling(dest).wait_send()

        @pl.when(dest != chip)
        def _():
            for m in range(3):
                pltpu.make_async_copy(sibs[m].at[dest], sibs[m].at[dest], send_sem.at[m, dest]).wait()
            for n in range(len(LATE_ORDERS)):
                part = sibs[3].at[dest, :, pl.ds(n * third, third)]
                pltpu.make_async_copy(part, part, late_send.at[n, dest]).wait()
        return carry

    lax.fori_loop(0, CHIPS, sent, 0)


def back_scatter(y_own, dwg, dwu, dwd, dwo, dsmall, x, w, q, k, v, g_att, g_res1, cos, sin, bias_col):
    tokens, width = x.shape
    rows = tokens // 2
    span = rows // 8
    anywhere, vmem = pl.BlockSpec(memory_space=pl.ANY), pl.BlockSpec(memory_space=pltpu.VMEM)
    n_gate, n_down, n_out = width // CHIPS, dwd.shape[1] // CHIPS, dwo.shape[1] // CHIPS
    c_gate, c_down = dwg.shape[2], dwd.shape[2]
    c_qkv = 3 * width // 2
    third = c_qkv // len(LATE_ORDERS)
    sds, mem = jax.ShapeDtypeStruct, pltpu.VMEM
    out8 = sds((8, span, width), LOW)
    finals = [sds((n_gate, c_gate), F32), sds((n_gate, c_gate), F32), sds((n_down, c_down), F32), sds((n_out, c_down), F32),
              sds((n_gate, c_qkv), F32), sds(dsmall.shape[1:], F32)]
    pieces = [(n_gate, c_gate), (n_gate, c_gate), (n_down + n_out, c_down)]
    scratch = [mem((tokens, width), LOW), mem(w.shape, LOW), mem((rows, width), LOW), mem((tokens, width), LOW), mem((tokens, width), LOW),
               mem((rows, width), LOW), mem((rows, width), F32), mem(cos.shape, F32), mem(sin.shape, F32), mem(bias_col.shape, F32),
               mem((width, tokens), LOW), mem((rows, width), F32), mem((rows, GROUP), F32), mem((tokens, GROUP), F32), mem((tokens, GROUP), F32),
               mem((2, width, c_qkv), LOW)]
    scratch += [mem((3,) + piece, LOW) for piece in pieces]
    scratch += [mem((CHIPS,) + piece, LOW) for piece in pieces] + [mem((CHIPS, n_gate, c_qkv), LOW)]
    scratch += [mem(pieces[2], F32)]
    for order, piece in zip(BACK_ORDERS, pieces):
        scratch += [mem((n,) + piece, LOW) for n in landing_slots(order)]
    for order in LATE_ORDERS:
        scratch += [mem((n, n_gate, third), LOW) for n in landing_slots(order)]
    scratch += [mem((rows, width), LOW), mem((rows, width), LOW), mem(dsmall.shape, F32)]
    dma = pltpu.SemaphoreType.DMA
    scratch += [dma((10,)), dma((3, CHIPS)), dma((3, 4, CHIPS)), dma((4, CHIPS)), dma((4, CHIPS)), dma((4, 3)), dma((3, CHIPS)), dma((3, 4, CHIPS)),
                dma((CHIPS,)), dma((CHIPS,)), dma((2,)), dma((2, 8)), dma((8,)), dma((8,)), dma((2 * CHIPS,)), dma((2 * CHIPS,))]
    return pl.pallas_call(
        back_scatter_kernel,
        out_shape=[out8, out8] + finals,
        in_specs=[anywhere] * 16,
        out_specs=[anywhere] * 2 + [vmem] * len(finals),
        scratch_shapes=scratch,
        compiler_params=pltpu.CompilerParams(collective_id=1, has_side_effects=True, vmem_limit_bytes=67043328),
        name="back_scatter",
    )(y_own, dwg, dwu, dwd, dwo, dsmall, x, w, q, k, v, g_att, g_res1, cos, sin, bias_col)


def rotary_turns(tokens, near):
    lane = jnp.arange(LANES)
    inverse = jnp.power(jnp.float32(1000.0), -2.0 * (lane % (HEAD // 2)).astype(F32) / HEAD)

    def table(positions):
        angles = positions.astype(F32)[:, None] * inverse[None, :]
        return jnp.stack([jnp.cos(angles), jnp.sin(angles)])

    return table(jnp.arange(0, tokens, near)), table(jnp.arange(near))


def local_by_slot(tokens, lengths, w_qkv, w_out, w_gate, w_up, w_down, ln_params, cotangent):
    slots, span, width = tokens.shape
    share = ln_params.shape[1]
    turns_far, turns_near = rotary_turns(span * CHIPS, span)
    x, cot, ln, w_in, wg, wu, wd, q, k, v, att, cos, sin, bias_col = front(
        tokens, cotangent, w_qkv, w_out, w_gate, w_up, w_down, ln_params, lengths, turns_far, turns_near)
    y, dwg, dwu, dwd, dwo, g_att, g_res1, dln = middle(x, att, w_in, wg, wu, wd, cot, ln, bias_col)
    dsmall = dln[:4].reshape(4, 2 * CHIPS, share).transpose(1, 0, 2)
    dsmall = jnp.pad(dsmall, ((0, 0), (0, 4), (0, LANES - share)))
    output, grad_tokens, d_gate, d_up, d_down, d_out, d_qkv, d_small = finish(back_scatter(
        y, dwg, dwu, dwd, dwo, dsmall, x, w_in, q, k, v, g_att, g_res1, cos, sin, bias_col))
    return (output, grad_tokens, d_qkv, d_out, d_gate, d_up, d_down, d_small[:4, :share])


def solution(mesh):
    placed = (
        P("dp", "seq", None),
        P("dp"),
        P("seq", "dp"),
        P("seq", "dp"),
        P("seq", "dp"),
        P("seq", "dp"),
        P("seq", "dp"),
        P(None, ("dp", "seq")),
        P("dp", "seq", None),
    )

    def run(tokens, *rest):
        by_slot = mesh.shape["dp"] == 2 and mesh.shape["seq"] == CHIPS and tokens.shape[0] == CHIPS
        body = local_by_slot if by_slot else local
        return jax.shard_map(
            body,
            mesh=mesh,
            in_specs=placed,
            out_specs=(
                P("dp", "seq", None),
                P("dp", "seq", None),
                P("seq", "dp"),
                P("seq", "dp"),
                P("seq", "dp"),
                P("seq", "dp"),
                P("seq", "dp"),
                P(None, ("dp", "seq")),
            ),
            check_vma=False,
        )(tokens, *rest)

    return run
```

```python
import functools

import jax
import jax.numpy as jnp
from jax import lax
from jax.experimental import pallas as pl
from jax.experimental.pallas import tpu as pltpu
from jax.sharding import PartitionSpec as P

HEADS = 12
HEAD_DIM = 64


norm_epsilon = 1e-12
score_scale = 0.125
masked_score = -1e30


def shifted(shard, axis, by):
    count = lax.axis_size(axis)
    return lax.ppermute(shard, axis, [(i, (i + by) % count) for i in range(count)])


def rotary_tables(positions):
    pair_index = jnp.arange(HEAD_DIM // 2, dtype=jnp.float32)
    inverse = jnp.power(jnp.float32(1000.0), -2.0 * pair_index / HEAD_DIM)
    angles = positions.astype(jnp.float32)[:, None] * inverse[None, :]
    cos_tab = jnp.concatenate([jnp.cos(angles), jnp.cos(angles)], axis=-1)
    sin_tab = jnp.concatenate([jnp.sin(angles), jnp.sin(angles)], axis=-1)
    return (cos_tab, sin_tab)


def rotate(values, cos_tab, sin_tab):
    half_dim = values.shape[-1] // 2
    turned = jnp.concatenate([-values[..., half_dim:], values[..., :half_dim]], axis=-1)
    return values * cos_tab + turned * sin_tab


def norm_parts(values, gain_vec, bias_vec):
    center = values - jnp.mean(values, axis=-1, keepdims=True)
    inv_std = lax.rsqrt(jnp.mean(center * center, axis=-1, keepdims=True) + norm_epsilon)
    normed = center * inv_std
    return (normed * gain_vec + bias_vec, normed, inv_std)


def norm_back(grad_in, normed, inv_std, gain_vec):
    scaled = grad_in * gain_vec
    return inv_std * (
        scaled
        - jnp.mean(scaled, axis=-1, keepdims=True)
        - normed * jnp.mean(scaled * normed, axis=-1, keepdims=True)
    )


def heads_view(flat_rows):
    return flat_rows.reshape(flat_rows.shape[0], flat_rows.shape[1], HEADS, HEAD_DIM)


def attend_block(run_state, queries, key_blk, value_blk, key_start, lengths):
    run_max, run_sum, run_acc = run_state
    scores = (
        jnp.einsum(
            "sqhd,skhd->shqk",
            heads_view(queries),
            heads_view(key_blk),
            preferred_element_type=jnp.float32,
        )
        * score_scale
    )
    key_pos = key_start + jnp.arange(key_blk.shape[1], dtype=jnp.int32)
    key_mask = (key_pos[None, :] < lengths[:, None])[:, None, None, :]
    scores = jnp.where(key_mask, scores, masked_score)
    new_max = jnp.maximum(run_max, jnp.max(scores, axis=-1))
    exp_scores = jnp.where(key_mask, jnp.exp(scores - new_max[..., None]), 0.0)
    factor = jnp.exp(run_max - new_max)
    run_sum = run_sum * factor + jnp.sum(exp_scores, axis=-1)
    run_acc = run_acc * factor[..., None] + jnp.einsum(
        "shqk,skhd->shqd",
        exp_scores.astype(jnp.bfloat16),
        heads_view(value_blk),
        preferred_element_type=jnp.float32,
    )
    return (new_max, run_sum, run_acc)


def block_grads(queries, grad_att, log_total, delta_rows, key_blk, value_blk, key_ok):
    query_h = heads_view(queries)
    grad_h = heads_view(grad_att)
    key_h = heads_view(key_blk)
    scores = (
        jnp.einsum("sqhd,skhd->shqk", query_h, key_h, preferred_element_type=jnp.float32)
        * score_scale
    )
    key_mask = key_ok[:, None, None, :]
    soft_probs = jnp.where(key_mask, jnp.exp(scores - log_total[..., None]), 0.0)
    grad_probs = jnp.einsum(
        "sqhd,skhd->shqk", grad_h, heads_view(value_blk), preferred_element_type=jnp.float32
    )
    grad_scores = (soft_probs * (grad_probs - delta_rows[..., None])).astype(jnp.bfloat16)
    part_q = (
        jnp.einsum("shqk,skhd->sqhd", grad_scores, key_h, preferred_element_type=jnp.float32)
        * score_scale
    )
    part_k = (
        jnp.einsum("shqk,sqhd->skhd", grad_scores, query_h, preferred_element_type=jnp.float32)
        * score_scale
    )
    part_v = jnp.einsum(
        "shqk,sqhd->skhd",
        soft_probs.astype(jnp.bfloat16),
        grad_h,
        preferred_element_type=jnp.float32,
    )
    shape_out = queries.shape
    return (part_q.reshape(shape_out), part_k.reshape(key_blk.shape), part_v.reshape(key_blk.shape))


def local(tokens, lengths, w_qkv, w_out, w_gate, w_up, w_down, ln_params, cotangent):
    slot_count, span_len, width = tokens.shape
    row_count = slot_count * span_len
    cycle_size = lax.axis_size("seq")
    my_index = lax.axis_index("seq")
    row_qkv, row_out, row_gate, row_up, row_down, row_norm = (
        lax.all_gather(w_qkv, "seq", axis=0, tiled=True),
        lax.all_gather(w_out, "seq", axis=0, tiled=True),
        lax.all_gather(w_gate, "seq", axis=0, tiled=True),
        lax.all_gather(w_up, "seq", axis=0, tiled=True),
        lax.all_gather(w_down, "seq", axis=0, tiled=True),
        lax.all_gather(ln_params, "seq", axis=1, tiled=True),
    )
    wide_qkv, wide_out, wide_gate, wide_up, wide_down, wide_norm = (
        lax.all_gather(row_qkv, "dp", axis=1, tiled=True),
        lax.all_gather(row_out, "dp", axis=1, tiled=True),
        lax.all_gather(row_gate, "dp", axis=1, tiled=True),
        lax.all_gather(row_up, "dp", axis=1, tiled=True),
        lax.all_gather(row_down, "dp", axis=1, tiled=True),
        lax.all_gather(row_norm, "dp", axis=1, tiled=True),
    )
    norm_full = wide_norm.astype(jnp.float32)
    flat_tokens = tokens.reshape(row_count, width)
    token_f32 = flat_tokens.astype(jnp.float32)
    positions = my_index * span_len + jnp.arange(span_len, dtype=jnp.int32)
    row_valid = (positions[None, :] < lengths[:, None]).astype(jnp.float32).reshape(row_count, 1)
    cos_tab, sin_tab = rotary_tables(positions)
    cos_four = cos_tab[None, :, None, :]
    sin_four = sin_tab[None, :, None, :]
    qkv_pre = jnp.dot(flat_tokens, wide_qkv, preferred_element_type=jnp.float32)
    split_qkv = qkv_pre.reshape(slot_count, span_len, 3, HEADS, HEAD_DIM)
    queries = (
        rotate(split_qkv[:, :, 0], cos_four, sin_four)
        .astype(jnp.bfloat16)
        .reshape(slot_count, span_len, width)
    )
    keys_rot = (
        rotate(split_qkv[:, :, 1], cos_four, sin_four)
        .astype(jnp.bfloat16)
        .reshape(slot_count, span_len, width)
    )
    values = split_qkv[:, :, 2].astype(jnp.bfloat16).reshape(slot_count, span_len, width)
    start_state = (
        jnp.full((slot_count, HEADS, span_len), masked_score, jnp.float32),
        jnp.zeros((slot_count, HEADS, span_len), jnp.float32),
        jnp.zeros((slot_count, HEADS, span_len, HEAD_DIM), jnp.float32),
    )
    key_piece = lax.all_gather(keys_rot, "seq", axis=1, tiled=True)
    value_piece = lax.all_gather(values, "seq", axis=1, tiled=True)
    block_count = key_piece.shape[1] // span_len

    def one_block(block_id, inner_state):
        offset = block_id * span_len
        key_blk = lax.dynamic_slice_in_dim(key_piece, offset, span_len, axis=1)
        value_blk = lax.dynamic_slice_in_dim(value_piece, offset, span_len, axis=1)
        return attend_block(inner_state, queries, key_blk, value_blk, offset, lengths)

    run_max, run_sum, run_acc = lax.fori_loop(0, block_count, one_block, start_state)
    attended = run_acc / run_sum[..., None]
    log_total = run_max + jnp.log(run_sum)
    attn_low = attended.transpose(0, 2, 1, 3).reshape(row_count, width).astype(jnp.bfloat16)
    branch = jnp.dot(attn_low, wide_out, preferred_element_type=jnp.float32)
    hidden, normed_one, inv_one = norm_parts(token_f32 + branch, norm_full[0], norm_full[1])
    hidden_low = hidden.astype(jnp.bfloat16)
    gate_pre = jnp.dot(hidden_low, wide_gate, preferred_element_type=jnp.float32)
    up_proj = jnp.dot(hidden_low, wide_up, preferred_element_type=jnp.float32)
    activated = jax.nn.silu(gate_pre)
    inner_low = (activated * up_proj).astype(jnp.bfloat16)
    branch_two = jnp.dot(inner_low, wide_down, preferred_element_type=jnp.float32)
    result, normed_two, inv_two = norm_parts(hidden + branch_two, norm_full[2], norm_full[3])
    output = (result * row_valid).astype(jnp.bfloat16).reshape(slot_count, span_len, width)
    back_qkv, back_out, back_gate, back_up, back_down, back_norm = (
        lax.all_gather(w_qkv, "seq", axis=0, tiled=True),
        lax.all_gather(w_out, "seq", axis=0, tiled=True),
        lax.all_gather(w_gate, "seq", axis=0, tiled=True),
        lax.all_gather(w_up, "seq", axis=0, tiled=True),
        lax.all_gather(w_down, "seq", axis=0, tiled=True),
        lax.all_gather(ln_params, "seq", axis=1, tiled=True),
    )
    wide_qkv, wide_out, wide_gate, wide_up, wide_down, wide_norm = (
        lax.all_gather(back_qkv, "dp", axis=1, tiled=True),
        lax.all_gather(back_out, "dp", axis=1, tiled=True),
        lax.all_gather(back_gate, "dp", axis=1, tiled=True),
        lax.all_gather(back_up, "dp", axis=1, tiled=True),
        lax.all_gather(back_down, "dp", axis=1, tiled=True),
        lax.all_gather(back_norm, "dp", axis=1, tiled=True),
    )
    norm_full = wide_norm.astype(jnp.float32)
    grad_out = cotangent.reshape(row_count, width).astype(jnp.float32) * row_valid
    gain_two_grad = jnp.sum(grad_out * normed_two, axis=0)
    bias_two_grad = jnp.sum(grad_out, axis=0)
    grad_res2 = norm_back(grad_out, normed_two, inv_two, norm_full[2])
    grad_branch2 = grad_res2.astype(jnp.bfloat16)
    grad_wdown = jnp.einsum(
        "rf,rd->fd", inner_low, grad_branch2, preferred_element_type=jnp.float32
    )
    grad_inner = jnp.einsum(
        "rd,fd->rf", grad_branch2, wide_down, preferred_element_type=jnp.float32
    )
    sigma = jax.nn.sigmoid(gate_pre)
    grad_gate = (grad_inner * up_proj * sigma * (1.0 + gate_pre * (1.0 - sigma))).astype(
        jnp.bfloat16
    )
    grad_up = (grad_inner * activated).astype(jnp.bfloat16)
    grad_wgate = jnp.einsum("rd,rf->df", hidden_low, grad_gate, preferred_element_type=jnp.float32)
    grad_wup = jnp.einsum("rd,rf->df", hidden_low, grad_up, preferred_element_type=jnp.float32)
    grad_hidden = (
        grad_res2
        + jnp.einsum("rf,df->rd", grad_gate, wide_gate, preferred_element_type=jnp.float32)
        + jnp.einsum("rf,df->rd", grad_up, wide_up, preferred_element_type=jnp.float32)
    )
    gain_one_grad = jnp.sum(grad_hidden * normed_one, axis=0)
    bias_one_grad = jnp.sum(grad_hidden, axis=0)
    grad_res1 = norm_back(grad_hidden, normed_one, inv_one, norm_full[0])
    grad_branch1 = grad_res1.astype(jnp.bfloat16)
    grad_wout = jnp.einsum("ri,rd->id", attn_low, grad_branch1, preferred_element_type=jnp.float32)
    grad_att = (
        jnp.einsum("rd,id->ri", grad_branch1, wide_out, preferred_element_type=jnp.float32)
        .astype(jnp.bfloat16)
        .reshape(slot_count, span_len, width)
    )
    zero_rows = jnp.zeros((slot_count, span_len, width), jnp.float32)
    delta_rows = jnp.einsum("sqhd,shqd->shq", heads_view(grad_att).astype(jnp.float32), attended)

    def key_turn(turn_id, run_state):
        key_cur, value_cur, grad_keys, grad_values, grad_query = run_state
        key_start = (my_index - turn_id) % cycle_size * span_len
        key_ok = (key_start + jnp.arange(span_len, dtype=jnp.int32))[None, :] < lengths[:, None]
        part_q, part_k, part_v = block_grads(
            queries, grad_att, log_total, delta_rows, key_cur, value_cur, key_ok
        )
        key_cur, value_cur = shifted((key_cur, value_cur), "seq", 1)
        grad_keys, grad_values = (
            shifted((grad_keys + part_k).astype(jnp.bfloat16), "seq", 1).astype(jnp.float32),
            shifted((grad_values + part_v).astype(jnp.bfloat16), "seq", 1).astype(jnp.float32),
        )
        return (key_cur, value_cur, grad_keys, grad_values, grad_query + part_q)

    key_cur, value_cur, grad_keys, grad_values, grad_query = lax.fori_loop(
        0, cycle_size - 1, key_turn, (keys_rot, values, zero_rows, zero_rows, zero_rows)
    )
    key_start = (my_index - (cycle_size - 1)) % cycle_size * span_len
    key_ok = (key_start + jnp.arange(span_len, dtype=jnp.int32))[None, :] < lengths[:, None]
    part_q, part_k, part_v = block_grads(
        queries, grad_att, log_total, delta_rows, key_cur, value_cur, key_ok
    )
    grad_query = grad_query + part_q
    grad_keys, grad_values = (
        shifted((grad_keys + part_k).astype(jnp.bfloat16), "seq", 1).astype(jnp.float32),
        shifted((grad_values + part_v).astype(jnp.bfloat16), "seq", 1).astype(jnp.float32),
    )
    query_back = rotate(heads_view(grad_query), cos_four, -sin_four)
    key_back = rotate(heads_view(grad_keys), cos_four, -sin_four)
    grad_qkv = jnp.stack([query_back, key_back, heads_view(grad_values)], axis=2)
    grad_qkv = grad_qkv.reshape(row_count, 3 * width).astype(jnp.bfloat16)
    grad_wqkv = jnp.einsum("rd,re->de", flat_tokens, grad_qkv, preferred_element_type=jnp.float32)
    grad_tokens = grad_res1 + jnp.einsum(
        "re,de->rd", grad_qkv, wide_qkv, preferred_element_type=jnp.float32
    )
    grad_tokens = grad_tokens.astype(jnp.bfloat16).reshape(slot_count, span_len, width)
    grad_norm = jnp.stack([gain_one_grad, bias_one_grad, gain_two_grad, bias_two_grad], axis=0)
    col_qkv, col_out, col_gate, col_up, col_down, col_norm = (
        lax.psum_scatter(
            grad_wqkv.astype(jnp.bfloat16), "dp", scatter_dimension=1, tiled=True
        ).astype(jnp.float32),
        lax.psum_scatter(
            grad_wout.astype(jnp.bfloat16), "dp", scatter_dimension=1, tiled=True
        ).astype(jnp.float32),
        lax.psum_scatter(
            grad_wgate.astype(jnp.bfloat16), "dp", scatter_dimension=1, tiled=True
        ).astype(jnp.float32),
        lax.psum_scatter(
            grad_wup.astype(jnp.bfloat16), "dp", scatter_dimension=1, tiled=True
        ).astype(jnp.float32),
        lax.psum_scatter(
            grad_wdown.astype(jnp.bfloat16), "dp", scatter_dimension=1, tiled=True
        ).astype(jnp.float32),
        lax.psum_scatter(
            grad_norm.astype(jnp.bfloat16), "dp", scatter_dimension=1, tiled=True
        ).astype(jnp.float32),
    )
    own_qkv, own_out, own_gate, own_up, own_down, own_norm = (
        lax.psum_scatter(
            col_qkv.astype(jnp.bfloat16), "seq", scatter_dimension=0, tiled=True
        ).astype(jnp.float32),
        lax.psum_scatter(
            col_out.astype(jnp.bfloat16), "seq", scatter_dimension=0, tiled=True
        ).astype(jnp.float32),
        lax.psum_scatter(
            col_gate.astype(jnp.bfloat16), "seq", scatter_dimension=0, tiled=True
        ).astype(jnp.float32),
        lax.psum_scatter(
            col_up.astype(jnp.bfloat16), "seq", scatter_dimension=0, tiled=True
        ).astype(jnp.float32),
        lax.psum_scatter(
            col_down.astype(jnp.bfloat16), "seq", scatter_dimension=0, tiled=True
        ).astype(jnp.float32),
        lax.psum_scatter(
            col_norm.astype(jnp.bfloat16), "seq", scatter_dimension=1, tiled=True
        ).astype(jnp.float32),
    )
    return (output, grad_tokens, own_qkv, own_out, own_gate, own_up, own_down, own_norm)


MESH = pl.DeviceIdType.MESH
CHIPS, ZS = 16, 4
OFFSETS = sorted(((dx, dy, dz) for dx in (0, 1) for dy in (0, 1) for dz in range(-3, 4)),
                 key=lambda o: (2 * (o[0] + o[1]) + abs(o[2]), abs(o[2]), o))


def pick(index, values):
    out = jnp.int32(0)
    for position, value in enumerate(values):
        if value:
            out = out + jnp.where(index == position, jnp.int32(value), 0)
    return out


def spread(order, dx, dy, dz):
    zero = {"x": dx == 0, "y": dy == 0, "z": dz == 0}
    flags = {}
    for position, axis in enumerate(order):
        flag = zero[axis] if axis != "z" else None
        for later in order[position + 1:]:
            flag = zero[later] if flag is None else flag & zero[later]
        flags[axis] = flag
    up, down = dz <= 0, dz >= 0
    if flags["z"] is not None:
        up, down = up & flags["z"], down & flags["z"]
    return flags["x"], flags["y"], up, down


def place():
    core, chip = lax.axis_index("dp"), lax.axis_index("seq")
    return core, chip, chip % 2, (chip // 2) % 2, chip // 4


def chip_at(x, y, z):
    return (z * 2 + y) * 2 + x


def meet_all(core, chip):
    greet_all(core, chip)
    all_here()


def onward(order, dx, dy, dz):
    zero = {"x": dx == 0, "y": dy == 0, "z": dz == 0}
    links = []
    for position, axis in enumerate(order):
        if all(zero[later] for later in order[position + 1:]):
            if axis == "z":
                links += [2] * (dz <= 0) + [3] * (dz >= 0)
            elif zero[axis]:
                links.append("xy".index(axis))
    return links


def when(condition, action):
    if condition is True:
        action()
    else:
        pl.when(condition)(action)


def to_slot(core, chip, j, source, target, sends, recvs):
    half = CHIPS // 2
    slot = (chip + 1 + j) % half
    to = core * half + slot
    src = source.at[slot]
    self_copy = (chip // half == core) & (to == chip)

    @pl.when(self_copy)
    def _():
        pltpu.make_async_copy(src, target, recvs.at[chip % half]).start()

    @pl.when(jnp.logical_not(self_copy))
    def _():
        pltpu.make_async_remote_copy(
            src_ref=src, dst_ref=target, send_sem=sends.at[slot], recv_sem=recvs.at[chip % half],
            device_id={"dp": chip // half, "seq": to}, device_id_type=MESH).start()


def from_slot(core, chip, j, source, target, sends, recvs):
    half = CHIPS // 2
    i = (chip + 1 + j) % half
    to_core, to_chip = chip // half, core * half + i
    span = target.shape[1]
    src, dst = source.at[pl.ds(pl.multiple_of(i * span, span), span)], target.at[chip % half]
    self_copy = (to_core == core) & (to_chip == chip)

    @pl.when(self_copy)
    def _():
        pltpu.make_async_copy(src, dst, recvs.at[chip % half]).start()

    @pl.when(jnp.logical_not(self_copy))
    def _():
        pltpu.make_async_remote_copy(
            src_ref=src, dst_ref=dst, send_sem=sends.at[i], recv_sem=recvs.at[chip % half],
            device_id={"dp": to_core, "seq": to_chip}, device_id_type=MESH).start()


def sent_blocks(core, chip, part, sends):
    half = CHIPS // 2

    def one(i, carry):
        @pl.when(jnp.logical_not((chip // half == core) & (core * half + i == chip)))
        def _():
            pltpu.make_async_copy(part, part, sends.at[i]).wait()
        return carry

    lax.fori_loop(0, half, one, 0)


def greet_all(core, chip):
    barrier = pltpu.get_barrier_semaphore()
    me = core * CHIPS + chip

    def greet(step, carry):
        other = (me + step) % (2 * CHIPS)
        pl.semaphore_signal(barrier, inc=1, device_id={"dp": other // CHIPS, "seq": other % CHIPS}, device_id_type=MESH)
        return carry

    lax.fori_loop(1, 2 * CHIPS, greet, 0)


def all_here():
    pl.semaphore_wait(pltpu.get_barrier_semaphore(), 2 * CHIPS - 1)


LOW, F32 = jnp.bfloat16, jnp.float32
EPS = 1e-12
HEAD = 64
LANES = 128
GROUP = 256
FULL = pl.BlockSpec(memory_space=pltpu.VMEM)


def nn(a, b):
    return jnp.dot(a, b, preferred_element_type=F32)


def nt(a, b):
    return lax.dot_general(a, b, (((1,), (1,)), ((), ())), preferred_element_type=F32)


def tn(a, b):
    return lax.dot_general(a, b, (((0,), (0,)), ((), ())), preferred_element_type=F32)


def lane_of(shape):
    return lax.broadcasted_iota(jnp.int32, shape, 1)


def turn(u):
    parts = []
    for start in range(0, u.shape[1], LANES):
        part = u[:, start:start + LANES]
        first = lane_of(part.shape) % HEAD < HEAD // 2
        parts.append(jnp.where(first, pltpu.roll(part, LANES - HEAD // 2, 1), pltpu.roll(part, HEAD // 2, 1)))
    return jnp.concatenate(parts, 1)


def ln_parts(u):
    center = u - jnp.mean(u, axis=1, keepdims=True)
    inv = lax.rsqrt(jnp.mean(center * center, axis=1, keepdims=True) + EPS)
    return center * inv, inv


def ln_back(g, n, inv):
    return inv * (g - jnp.mean(g, axis=1, keepdims=True) - n * jnp.mean(g * n, axis=1, keepdims=True))


def middle_kernel(tiles, x_ref, att_ref, wo_ref, wg_ref, wu_ref, wd_ref, cot_ref, ln_ref, bias_ref,
                  y_out, dwg_ref, dwu_ref, dwd_ref, dwo_ref, gatt_ref, gres_ref, dln_ref,
                  n1_ref, inv1_ref, hid_ref, hidt_ref, gate_ref, up_ref, acc_ref, gb_ref, y_ref, y_send, y_recv):
    index = pl.program_id(0)
    width = x_ref.shape[1]
    half = width // 2
    rows = att_ref.shape[0]
    core, chip = lax.axis_index("dp"), lax.axis_index("seq")
    mine = pl.ds(pl.multiple_of(core * rows, rows), rows)
    eighth = CHIPS // 2

    def wide(ref):
        return jnp.concatenate([ref[0], ref[1]], 1)

    @pl.when(index == 0)
    def _():
        greet_all(core, chip)
        n1, inv1 = ln_parts(x_ref[mine, :].astype(F32) + nn(att_ref[...], wide(wo_ref)))
        hidden = n1 * ln_ref[0:1, :] + ln_ref[1:2, :]
        n1_ref[...] = n1
        inv1_ref[...] = jnp.broadcast_to(inv1, inv1_ref.shape)
        acc_ref[...] = hidden
        low = hidden.astype(LOW)
        hid_ref[...] = low
        hidt_ref[...] = low.T

    tile = wg_ref.shape[2]
    f = jnp.where(index < tiles, index, index - tiles)
    cols = pl.ds(pl.multiple_of(f * tile, tile), tile)

    @pl.when(index < tiles)
    def _():
        gate, up = nn(hid_ref[...], wg_ref[0]), nn(hid_ref[...], wu_ref[0])
        gate_ref[:, cols] = gate
        up_ref[:, cols] = up
        acc_ref[...] += nn((gate * jax.nn.sigmoid(gate) * up).astype(LOW), wide(wd_ref))

    @pl.when(index == tiles - 1)
    def _():
        n2, inv2 = ln_parts(acc_ref[...])
        all_here()
        valid = jnp.where(bias_ref[mine, 0:1] == 0.0, 1.0, 0.0)
        y_ref[...] = ((n2 * ln_ref[2:3, :] + ln_ref[3:4, :]) * valid).astype(LOW)
        for j in range(eighth):
            from_slot(core, chip, j, y_ref, y_out, y_send, y_recv)
        g_y = cot_ref[...].astype(F32) * valid
        dln_ref[2:3, :] = jnp.sum(g_y * n2, axis=0, keepdims=True)
        dln_ref[3:4, :] = jnp.sum(g_y, axis=0, keepdims=True)
        g_res2 = ln_back(g_y * ln_ref[2:3, :], n2, inv2)
        acc_ref[...] = g_res2
        gb_ref[...] = g_res2.astype(LOW)

    @pl.when(index >= tiles)
    def _():
        gate, up = gate_ref[:, cols], up_ref[:, cols]
        sig = jax.nn.sigmoid(gate)
        act = gate * sig
        gb = gb_ref[...]
        dwd = tn((act * up).astype(LOW), gb)
        dwd_ref[0] = dwd[:, :half].astype(LOW)
        dwd_ref[1] = dwd[:, half:].astype(LOW)
        g_inner = nt(gb, wide(wd_ref))
        g_gate = (g_inner * up * sig * (1.0 + gate * (1.0 - sig))).astype(LOW)
        g_up = (g_inner * act).astype(LOW)
        dwg_ref[0] = nn(hidt_ref[...], g_gate).astype(LOW)
        dwu_ref[0] = nn(hidt_ref[...], g_up).astype(LOW)
        acc_ref[...] += nt(g_gate, wg_ref[0]) + nt(g_up, wu_ref[0])

    @pl.when(index == 2 * tiles - 1)
    def _():
        g_hidden, n1 = acc_ref[...], n1_ref[...]
        dln_ref[0:1, :] = jnp.sum(g_hidden * n1, axis=0, keepdims=True)
        dln_ref[1:2, :] = jnp.sum(g_hidden, axis=0, keepdims=True)
        g_res1 = ln_back(g_hidden * ln_ref[0:1, :], n1, inv1_ref[:, 0:1])
        gres_ref[...] = g_res1
        gb1 = g_res1.astype(LOW)
        dwo = tn(att_ref[...], gb1)
        dwo_ref[0] = dwo[:, :half].astype(LOW)
        dwo_ref[1] = dwo[:, half:].astype(LOW)
        gatt_ref[...] = nt(gb1, wide(wo_ref)).astype(LOW)
        sent_blocks(core, chip, y_out.at[0], y_send)
        lax.fori_loop(0, eighth, lambda i, carry: (pltpu.make_async_copy(y_out.at[i], y_out.at[i], y_recv.at[i]).wait(), carry)[1], 0)


def middle(x, att, wo, wg, wu, wd, cot, ln, bias_col):
    rows, width = att.shape
    hidden = wd.shape[1]
    tile = 512
    tiles = hidden // tile
    anywhere = pl.BlockSpec(memory_space=pl.ANY)
    per = wg.shape[2] // tile
    at = lambda i: jnp.where(i < tiles, i, i - tiles)
    late = lambda i: jnp.maximum(i - tiles, 0)
    cols = lambda pick: pl.BlockSpec((1, width, tile), lambda i: (pick(i) // per, 0, pick(i) % per))
    rowb = lambda pick: pl.BlockSpec((2, tile, wd.shape[2]), lambda i: (0, pick(i), 0))
    sds = jax.ShapeDtypeStruct
    return pl.pallas_call(
        functools.partial(middle_kernel, tiles), grid=(2 * tiles,),
        out_shape=[sds((8, rows // 8, width), LOW), sds(wg.shape, LOW), sds(wu.shape, LOW), sds(wd.shape, LOW), sds((2, width, width // 2), LOW),
                   sds((rows, width), LOW), sds((rows, width), F32), sds((8, width), F32)],
        in_specs=[FULL, FULL, pl.BlockSpec((2, width, width // 2), lambda i: (0, 0, 3)), cols(at), cols(at), rowb(at), FULL, FULL, FULL],
        out_specs=[anywhere, cols(late), cols(late), rowb(late), FULL, FULL, FULL, FULL],
        scratch_shapes=[pltpu.VMEM((rows, width), F32), pltpu.VMEM((rows, LANES), F32), pltpu.VMEM((rows, width), LOW),
                        pltpu.VMEM((width, rows), LOW), pltpu.VMEM((rows, hidden), F32), pltpu.VMEM((rows, hidden), F32),
                        pltpu.VMEM((rows, width), F32), pltpu.VMEM((rows, width), LOW), pltpu.VMEM((rows, width), LOW)]
        + [pltpu.SemaphoreType.DMA((8,))] * 2,
        compiler_params=pltpu.CompilerParams(collective_id=2, has_side_effects=True, vmem_limit_bytes=60 << 20),
        cost_estimate=pl.CostEstimate(flops=24 * 10**9, bytes_accessed=6 * 10**7, transcendentals=3 * 10**6),
        name="middle")(x, att, wo, wg, wu, wd, cot, ln, bias_col)


def finish_kernel(count, share, *refs):
    sources, targets, holds, (in_sem, out_sem) = refs[:count], refs[count:2 * count], refs[2 * count:3 * count], refs[3 * count:]
    loads = [pltpu.make_async_copy(source, hold, in_sem.at[n]) for n, (source, hold) in enumerate(zip(sources, holds))]
    stores = [pltpu.make_async_copy(hold, target, out_sem.at[n]) for n, (hold, target) in enumerate(zip(holds[:-1], targets[:-1]))]
    for load in loads:
        load.start()
    for load, store in zip(loads[:-1], stores):
        load.wait()
        store.start()
    loads[-1].wait()
    targets[-1][...] = holds[-1][0:4, 0:share]
    for store in stores:
        store.wait()


def finish(results, share):
    count = len(results)
    anywhere = pl.BlockSpec(memory_space=pl.ANY)
    shapes = [jax.ShapeDtypeStruct(r.shape, r.dtype) for r in results]
    shapes[-1] = jax.ShapeDtypeStruct((4, share), results[-1].dtype)
    return pl.pallas_call(
        functools.partial(finish_kernel, count, share), out_shape=shapes,
        in_specs=[anywhere] * count, out_specs=[anywhere] * (count - 1) + [FULL],
        scratch_shapes=[pltpu.VMEM(r.shape, r.dtype) for r in results] + [pltpu.SemaphoreType.DMA((count,))] * 2,
        name="finish")(*results)

FIRST_ORDERS = ("yzx", "xzy", "zyx", "zxy")
REST_ORDERS = ("xzy", "zyx", "zyx")
REST_STARTS = (12, 6, 0)
REST_MIXES = 20
TOKENS_AT = (1, 4, 7, 10, 13, 16, 18, 20)
COTS_AT = (2, 3, 4, 5, 6, 7, 8, 9)
CHUNK = 256


def front_kernel(tok, cot, w_qkv, w_out, w_gate, w_up, w_down, ln_in, len_in, turns_far, turns_near,
                 x_all, c_own, ln_out, w_first, wide_gate, wide_up, wide_down, q_out, k_out, v_out, att_out, cos_out, sin_out, bias_out, lse_out, *refs):
    (xv, wv, qv, kv, vv, attv, cosv, sinv, biasv, rowv, small, smalls, lnv, lsev), refs = refs[:14], refs[14:]
    (first_send, first_recv, first_sib, rest_send, rest_recv, rest_sib, own_sem, tok_send, tok_recv, tok_sib, cot_recv,
     small_send, small_recv, out_sem) = refs
    core, chip, x, y, z = place()
    other = 1 - core
    slots, span = tok.shape[0], tok.shape[1]
    half = CHIPS // 2
    me = core * CHIPS + chip
    rows, width = qv.shape
    can = (True, True, z < ZS - 1, z > 0, True)
    neighbours = (
        {"dp": core, "seq": chip_at(1 - x, y, z)},
        {"dp": core, "seq": chip_at(x, 1 - y, z)},
        {"dp": core, "seq": chip_at(x, y, jnp.minimum(z + 1, ZS - 1))},
        {"dp": core, "seq": chip_at(x, y, jnp.maximum(z - 1, 0))},
        {"dp": other, "seq": chip},
    )
    shards, wides = (w_gate, w_up, w_down), (wide_gate, wide_up, wide_down)
    n_first = w_out.shape[0]
    c_first = w_out.shape[1]

    def first_region(n, owner, source):
        return wv.at[owner, pl.ds(pl.multiple_of(source * n_first, n_first), n_first), n * c_first:n * c_first + c_first]

    def first_own(n):
        return w_out if n == 3 else w_qkv.at[:, n * c_first:n * c_first + c_first]

    def rest_region(m, owner, source):
        size = shards[m].shape[0]
        return wides[m].at[owner, pl.ds(pl.multiple_of(source * size, size), size)]

    def first_piece(n, source, link, own=False):
        target = first_region(n, core, source)
        return pltpu.make_async_remote_copy(
            src_ref=first_own(n) if own else target, dst_ref=target, send_sem=first_send.at[n, link, source],
            recv_sem=first_sib.at[n, source] if link == 4 else first_recv.at[n, source],
            device_id=neighbours[link], device_id_type=MESH)

    def rest_piece(m, source, link, own=False):
        target = rest_region(m, core, source)
        return pltpu.make_async_remote_copy(
            src_ref=shards[m] if own else target, dst_ref=target, send_sem=rest_send.at[m, link, source],
            recv_sem=rest_sib.at[m, source] if link == 4 else rest_recv.at[m, source],
            device_id=neighbours[link], device_id_type=MESH)

    def valid(offset):
        dz = offset[2]
        return True if dz == 0 else (z < ZS - dz if dz > 0 else z >= -dz)

    def source_at(offset):
        return chip_at((x + offset[0]) % 2, (y + offset[1]) % 2, z + offset[2])

    def arrive(piece, orders, offset):
        def one():
            source = source_at(offset)
            for m, order in enumerate(orders):
                piece(m, source, 0).wait_recv()
                for link in onward(order, *offset) + [4]:
                    when(can[link], piece(m, source, link).start)
        when(valid(offset), one)

    def send_own(piece, orders, m):
        for link in onward(orders[m], 0, 0, 0) + [4]:
            when(can[link], piece(m, chip, link, own=True).start)

    def drain(piece, orders):
        for offset in OFFSETS:
            def one():
                source = source_at(offset)
                for m, order in enumerate(orders):
                    for link in onward(order, *offset) + [4]:
                        when(can[link], piece(m, source, link).wait_send)
            when(valid(offset), one)

    def rows_of(ref, index):
        return ref.at[pl.ds(pl.multiple_of(index * span, span), span)]

    def deliver(j, source, target, sends, recvs):
        slot = (chip + 1 + j) % half
        to = core * half + slot
        src, dst = source.at[slot], target
        self_copy = (chip // half == core) & (to == chip)

        @pl.when(self_copy)
        def _():
            pltpu.make_async_copy(src, dst, recvs.at[chip % half]).start()

        @pl.when(jnp.logical_not(self_copy))
        def _():
            pltpu.make_async_remote_copy(
                src_ref=src, dst_ref=dst, send_sem=sends.at[slot], recv_sem=recvs.at[chip % half],
                device_id={"dp": chip // half, "seq": to}, device_id_type=MESH).start()

    def small_to(step):
        to = (me + step) % (2 * CHIPS)
        return pltpu.make_async_remote_copy(
            src_ref=small, dst_ref=smalls.at[me], send_sem=small_send.at[step], recv_sem=small_recv.at[me],
            device_id={"dp": to // CHIPS, "seq": to % CHIPS}, device_id_type=MESH)

    lane = lax.broadcasted_iota(jnp.int32, (1, LANES), 1)
    counts = jnp.zeros((1, LANES), F32)
    for j in range(slots):
        counts = counts + jnp.where(lane == j, len_in[j].astype(F32), 0.0)
    small[...] = jnp.zeros_like(small)
    small[0:ln_in.shape[0], 0:ln_in.shape[1]] = ln_in[...].astype(F32)
    small[4:5, :] = counts
    meet_all(core, chip)

    for n in range(4):
        send_own(first_piece, FIRST_ORDERS, n)
        pltpu.make_async_copy(first_own(n), first_region(n, core, chip), own_sem.at[n]).start()
    lax.fori_loop(1, 2 * CHIPS, lambda s, c: (small_to(s).start(), c)[1], 0)
    own_small = pltpu.make_async_copy(small, smalls.at[me], small_recv.at[me])
    own_small.start()

    sign = jnp.where(lane % HEAD < HEAD // 2, -1.0, 1.0).astype(F32)
    near = turns_near.shape[1]
    for far in range(turns_far.shape[1]):
        part = slice(far * near, far * near + near)
        ca, sa = turns_far[0, far:far + 1, :], turns_far[1, far:far + 1, :]
        cosv[part, :] = ca * turns_near[0] - sa * turns_near[1]
        sinv[part, :] = (sa * turns_near[0] + ca * turns_near[1]) * sign

    def relay(i, carry):
        block = rows_of(xv, core * half + i)
        pltpu.make_async_copy(block, block, tok_recv.at[i]).wait()
        pltpu.make_async_remote_copy(
            src_ref=block, dst_ref=block, send_sem=tok_send.at[2, i], recv_sem=tok_sib.at[i],
            device_id=neighbours[4], device_id_type=MESH).start()
        return carry

    waiting = list(OFFSETS[1:])
    for index, offset in enumerate(OFFSETS[1:]):
        for j in range(half):
            if index == TOKENS_AT[j]:
                deliver(j, tok, rows_of(xv, chip), tok_send.at[0], tok_recv)
        for m in range(3):
            if index == REST_STARTS[m]:
                send_own(rest_piece, REST_ORDERS, m)
                pltpu.make_async_copy(shards[m], rest_region(m, core, chip), own_sem.at[4 + m]).start()
        arrive(first_piece, FIRST_ORDERS, offset)
        if index >= REST_MIXES:
            arrive(rest_piece, REST_ORDERS, waiting.pop(0))

    def first_in(source, carry):
        for n in range(4):
            block = first_region(n, other, source)
            pltpu.make_async_copy(block, block, first_sib.at[n, source]).wait()
        return carry

    def small_in(step, carry):
        source = (me + step) % (2 * CHIPS)
        pltpu.make_async_copy(smalls.at[source], smalls.at[source], small_recv.at[source]).wait()
        return carry

    def tok_in(i, carry):
        block = rows_of(xv, other * half + i)
        pltpu.make_async_copy(block, block, tok_sib.at[i]).wait()
        return carry

    lax.fori_loop(0, half, relay, 0)
    lax.fori_loop(0, half, tok_in, 0)
    lax.fori_loop(0, CHIPS, first_in, 0)
    for n in range(4):
        pltpu.make_async_copy(first_own(n), first_region(n, core, chip), own_sem.at[n]).wait()
    lax.fori_loop(1, 2 * CHIPS, small_in, 0)
    own_small.wait()
    norms, share = ln_in.shape
    lnv[...] = jnp.zeros_like(lnv)
    lnv[0:norms, :] = jnp.concatenate([smalls[device, 0:norms, 0:share] for device in range(2 * CHIPS)], 1)
    counted = smalls[chip // half * CHIPS, 4:5, :]
    length = jnp.sum(jnp.where(lane == chip % half, counted, 0.0), axis=1, keepdims=True)
    at_row = lax.broadcasted_iota(jnp.int32, biasv.shape, 0).astype(F32)
    biasv[...] = jnp.where(at_row < length, 0.0, masked_score)
    at_lane = lax.broadcasted_iota(jnp.int32, rowv.shape, 1).astype(F32)
    rowv[...] = jnp.where(at_lane < length, 0.0, masked_score)
    outs = [pltpu.make_async_copy(source, target, out_sem.at[n]) for n, (source, target) in enumerate((
        (xv, x_all), (wv, w_first), (lnv, ln_out), (cosv, cos_out), (sinv, sin_out), (biasv, bias_out),
        (qv, q_out), (kv, k_out), (vv, v_out), (attv, att_out), (lsev, lse_out)))]
    for copy in outs[:6]:
        copy.start()

    mine = pl.ds(pl.multiple_of(core * rows, rows), rows)
    blocks = width // LANES
    per = 3 * blocks // 2

    def weights(block):
        return jnp.concatenate([wv[b // per, :, pl.ds(pl.multiple_of(b % per * LANES, LANES), LANES)] for b in (block, block + 1)], 1)

    def turned(u, cos, sin):
        return u * jnp.concatenate([cos, cos], 1) + turn(u) * jnp.concatenate([sin, sin], 1)

    per_group = (GROUP // LANES) * (rows // CHUNK)
    chunks = width // GROUP * per_group

    def chunk(index, carry):
        group, inner = index // per_group, index % per_group
        cols = pl.ds(pl.multiple_of(group * GROUP, GROUP), GROUP)

        @pl.when(inner == 0)
        def _():
            q = turned(nn(xv[mine, :], weights(2 * group)), cosv[mine, :], sinv[mine, :]).astype(LOW)
            qv[:, cols] = q * jnp.asarray(0.125, LOW)
            kv[:, cols] = turned(nn(xv[...], weights(blocks + 2 * group)), cosv[...], sinv[...]).astype(LOW)
            vv[:, cols] = nn(xv[...], weights(2 * blocks + 2 * group)).astype(LOW)

        pair, block = inner // (rows // CHUNK), inner % (rows // CHUNK)
        here = pl.ds(pl.multiple_of(block * CHUNK, CHUNK), CHUNK)
        lanes = pl.ds(pl.multiple_of(group * GROUP + pair * LANES, LANES), LANES)
        qp, kp, vp = qv[here, lanes], kv[:, lanes], vv[:, lanes]
        low = lane_of(qp.shape) < HEAD
        parts = []
        for head in range(2):
            qm = jnp.where(low if head == 0 else jnp.logical_not(low), qp, jnp.zeros_like(qp))
            s = nt(qm, kp) + rowv[0:1, :]
            top = jnp.max(s, axis=1, keepdims=True)
            p = jnp.exp(s - top)
            total = jnp.sum(p, axis=1, keepdims=True)
            at_head = pl.ds(2 * (group * (GROUP // LANES) + pair) + head, 1)
            lsev[at_head, here] = jnp.broadcast_to(top + jnp.log(total), (CHUNK, LANES)).T[0:1, :]
            parts.append(nn(p.astype(LOW), vp) / total)
        attv[here, lanes] = jnp.where(low, parts[0], parts[1]).astype(LOW)

        for k in range(chunks):
            @pl.when(index == k)
            def _():
                for j in range(half):
                    if k == COTS_AT[j]:
                        deliver(j, cot, rows_of(c_own, chip % half), tok_send.at[1], cot_recv)
                if waiting:
                    arrive(rest_piece, REST_ORDERS, waiting.pop(0))
        return carry

    lax.fori_loop(0, chunks, chunk, 0)
    for copy in outs[6:]:
        copy.start()
    while waiting:
        arrive(rest_piece, REST_ORDERS, waiting.pop(0))

    def ends(i, carry):
        block = rows_of(c_own, i)
        pltpu.make_async_copy(block, block, cot_recv.at[i]).wait()
        block = rows_of(xv, core * half + i)
        pltpu.make_async_copy(block, block, tok_send.at[2, i]).wait()
        self_copy = (chip // half == core) & (core * half + i == chip)

        @pl.when(jnp.logical_not(self_copy))
        def _():
            pltpu.make_async_copy(tok.at[i], tok.at[i], tok_send.at[0, i]).wait()
            pltpu.make_async_copy(cot.at[i], cot.at[i], tok_send.at[1, i]).wait()
        return carry

    def rest_in(source, carry):
        for m in range(3):
            block = rest_region(m, other, source)
            pltpu.make_async_copy(block, block, rest_sib.at[m, source]).wait()
        return carry

    lax.fori_loop(1, 2 * CHIPS, lambda s, c: (small_to(s).wait_send(), c)[1], 0)
    lax.fori_loop(0, half, ends, 0)
    drain(first_piece, FIRST_ORDERS)
    drain(rest_piece, REST_ORDERS)
    lax.fori_loop(0, CHIPS, rest_in, 0)
    for m in range(3):
        pltpu.make_async_copy(shards[m], rest_region(m, core, chip), own_sem.at[4 + m]).wait()
    for copy in outs:
        copy.wait()


def front(tokens, cotangent, w_qkv, w_out, w_gate, w_up, w_down, ln_params, lengths, turns_far, turns_near):
    slots, span, width = tokens.shape
    total, rows = span * CHIPS, span * CHIPS // 2
    sds, mem, dma = jax.ShapeDtypeStruct, pltpu.VMEM, pltpu.SemaphoreType.DMA
    anywhere, vmem, smem = (pl.BlockSpec(memory_space=s) for s in (pl.ANY, pltpu.VMEM, pltpu.SMEM))
    wide = lambda w: sds((2, w.shape[0] * CHIPS, w.shape[1]), LOW)
    first = (2, width, w_qkv.shape[1] + w_out.shape[1])
    table, small = (total, LANES), (8, LANES)
    outs = [sds((total, width), LOW), sds((rows, width), LOW), sds((8, width), F32), sds(first, LOW),
            wide(w_gate), wide(w_up), wide(w_down), sds((rows, width), LOW), sds((total, width), LOW), sds((total, width), LOW),
            sds((rows, width), LOW), sds(table, F32), sds(table, F32), sds(table, F32), sds((16, rows), F32)]
    return pl.pallas_call(
        front_kernel,
        out_shape=outs,
        in_specs=[anywhere] * 7 + [vmem, smem, vmem, vmem],
        out_specs=[anywhere] * len(outs),
        scratch_shapes=[
            mem((total, width), LOW), mem(first, LOW), mem((rows, width), LOW), mem((total, width), LOW), mem((total, width), LOW),
            mem((rows, width), LOW), mem(table, F32), mem(table, F32), mem(table, F32), mem((8, total), F32), mem(small, F32),
            mem((2 * CHIPS,) + small, F32), mem((8, width), F32), mem((16, rows), F32),
            dma((4, 5, CHIPS)), dma((4, CHIPS)), dma((4, CHIPS)), dma((3, 5, CHIPS)), dma((3, CHIPS)), dma((3, CHIPS)), dma((7,)),
            dma((3, 8)), dma((8,)), dma((8,)), dma((8,)), dma((2 * CHIPS,)), dma((2 * CHIPS,)), dma((11,))],
        compiler_params=pltpu.CompilerParams(collective_id=0, has_side_effects=True, vmem_limit_bytes=60 << 20),
        name="front",
    )(tokens, cotangent, w_qkv, w_out, w_gate, w_up, w_down, ln_params, lengths, turns_far, turns_near)

BACK_ORDERS = ("xzy", "zyx", "zyx")
LATE_ORDERS = ("zxy", "zyx", "zxy")
FAR_FIRST = OFFSETS[::-1]
SIDES = {"x": 2, "y": 2, "z": ZS}


def far_first(index):
    words = [sum((o[0] + 2 * o[1] + 4 * (o[2] + 3)) << (5 * place) for place, o in enumerate(FAR_FIRST[start:start + 6]))
             for start in range(0, len(FAR_FIRST), 6)]
    word = jnp.int32(words[0])
    for place, value in enumerate(words[1:], 1):
        word = jnp.where(index >= 6 * place, jnp.int32(value), word)
    code = lax.shift_right_logical(word, 5 * (index % 6)) & 31
    return code & 1, lax.shift_right_logical(code, 1) & 1, lax.shift_right_logical(code, 2) - 3


def landing_slots(order):
    sizes, room = {}, 1
    for axis in order:
        sizes[axis] = room * (ZS if axis == "z" else 1)
        room *= SIDES[axis]
    return sizes["x"], sizes["y"], sizes["z"], sizes["z"]


def landing_index(order, link, x, y, z):
    axis = "xyzz"[link]
    index = 0
    for before in order:
        if before == axis:
            break
        index = index * SIDES[before] + {"x": x, "y": y, "z": z}[before]
    return index * ZS + z if axis == "z" else index


def back_scatter_kernel(dwg, dwu, dwd, dwo, dsmall, x_in, w_in, q_in, k_in, v_in, g_in, res_in, cos_in, sin_in, bias_in, att_in, lse_in,
                        gt_out, f_gate, f_up, f_down, f_out, f_qkv, f_small, *refs):
    (xv, wv, qv, kv, vv, gv, own_acc, cosv, sinv, biasv, xt, oth_acc, dq, dk, dv, dw, attv, lsev), refs = refs[:18], refs[18:]
    owns, refs = refs[:3], refs[3:]
    sibs, refs = refs[:4], refs[4:]
    down_out, refs = refs[0], refs[1:]
    lands, refs = refs[:24], refs[24:]
    (gt_low, gt_sib, smalls), refs = refs[:3], refs[3:]
    (in_sem, send_sem, recv_sem, sib_send, sib_recv, own_sem, late_send, late_recv, late_sib_send, late_sib_recv,
     gt_sem, tok_send, gt_recv, small_send, small_recv) = refs
    core, chip, x, y, z = place()
    other = 1 - core
    half = CHIPS // 2
    me = core * CHIPS + chip
    rows = qv.shape[0]
    mine = pl.ds(pl.multiple_of(core * rows, rows), rows)
    theirs = pl.ds(pl.multiple_of(other * rows, rows), rows)
    neighbours = (
        {"dp": core, "seq": chip_at(1 - x, y, z)},
        {"dp": core, "seq": chip_at(x, 1 - y, z)},
        {"dp": core, "seq": chip_at(x, y, jnp.minimum(z + 1, ZS - 1))},
        {"dp": core, "seq": chip_at(x, y, jnp.maximum(z - 1, 0))},
    )
    sibling = {"dp": other, "seq": chip}

    loads = [pltpu.make_async_copy(source, target, in_sem.at[n]) for n, (source, target) in enumerate((
        (k_in, kv), (q_in, qv), (bias_in, biasv), (v_in, vv), (g_in, gv), (att_in, attv), (lse_in, lsev), (x_in, xv), (w_in, wv), (res_in, own_acc), (cos_in, cosv), (sin_in, sinv)))]
    for load in loads:
        load.start()

    def cut(ref, size, index):
        return ref.at[pl.ds(pl.multiple_of(index * size, size), size)]

    rows_gate, rows_down, rows_out = f_gate.shape[0], f_down.shape[0], f_out.shape[0]

    def parts(m, owner, dest):
        if m == 0:
            return [(cut(dwg.at[owner], rows_gate, dest), 0, rows_gate)]
        if m == 1:
            return [(cut(dwu.at[owner], rows_gate, dest), 0, rows_gate)]
        return [(cut(dwd.at[owner], rows_down, dest), 0, rows_down), (cut(dwo.at[owner], rows_out, dest), rows_down, rows_out)]

    def to_sibling(m, dest):
        return [pltpu.make_async_remote_copy(
            src_ref=source, dst_ref=sibs[m].at[dest, pl.ds(start, size)], send_sem=sib_send.at[m + n, dest],
            recv_sem=sib_recv.at[m + n, dest], device_id=sibling, device_id_type=MESH)
            for n, (source, start, size) in enumerate(parts(m, other, dest))]

    def own_load(m, dest, slot):
        return [pltpu.make_async_copy(source, owns[m].at[slot, pl.ds(start, size)], own_sem.at[m + n, slot])
                for n, (source, start, size) in enumerate(parts(m, core, dest))]

    def dest_of(index):
        dx, dy, dz = far_first(index)
        return dx, dy, dz, (z + dz >= 0) & (z + dz < ZS), (x + dx) % 2, (y + dy) % 2, jnp.clip(z + dz, 0, ZS - 1)

    meet_all(core, chip)

    def begin(index, carry):
        dx, dy, dz, valid, tx, ty, tz = dest_of(index)

        @pl.when(valid)
        def _():
            for m in range(3):
                for copy in to_sibling(m, chip_at(tx, ty, tz)):
                    copy.start()
        return carry

    lax.fori_loop(0, len(FAR_FIRST), begin, 0)

    def prefetch(index):
        dx, dy, dz, valid, tx, ty, tz = dest_of(index)

        @pl.when(valid & (index < len(FAR_FIRST)))
        def _():
            for m in range(3):
                for copy in own_load(m, chip_at(tx, ty, tz), index % 3):
                    copy.start()

    prefetch(jnp.int32(0))
    prefetch(jnp.int32(1))

    def small_to(step):
        to = (me + step) % (2 * CHIPS)
        return pltpu.make_async_remote_copy(
            src_ref=dsmall.at[to], dst_ref=smalls.at[me], send_sem=small_send.at[step], recv_sem=small_recv.at[me],
            device_id={"dp": to // CHIPS, "seq": to % CHIPS}, device_id_type=MESH)

    lax.fori_loop(1, 2 * CHIPS, lambda s, c: (small_to(s).start(), c)[1], 0)
    own_small = pltpu.make_async_copy(dsmall.at[me], smalls.at[me], small_recv.at[me])
    own_small.start()

    def reduce_piece(order, lands_m, send_at, recv_at, own, acc, offset, target, last, final):
        dx, dy, dz = offset
        tx, ty, tz = target
        fx, fy, up, down = spread(order, dx, dy, dz)
        flags = (fx, fy, up & (z < ZS - 1), down & (z > 0))

        @pl.when(jnp.logical_not(last))
        def _():
            acc[...] += own()

        @pl.when(last)
        def _():
            final[...] = acc[...].astype(F32) + own().astype(F32)

        for link in range(4):
            land = lands_m[link].at[landing_index(order, link, tx, ty, tz)]

            @pl.when(flags[link])
            def _():
                pltpu.make_async_copy(land, land, recv_at(link)).wait()

            @pl.when(flags[link] & jnp.logical_not(last))
            def _():
                acc[...] += land[...]

            @pl.when(flags[link] & last)
            def _():
                final[...] += land[...].astype(F32)

        away = {"x": dx != 0, "y": dy != 0, "z": dz != 0}
        taken = None
        for axis in order[::-1]:
            here = away[axis] if taken is None else away[axis] & jnp.logical_not(taken)
            taken = away[axis] if taken is None else taken | away[axis]
            for link in {"x": (0,), "y": (1,), "z": (2, 3)}[axis]:
                go = here if axis != "z" else (here & (dz > 0 if link == 2 else dz < 0))
                there = {0: 0, 1: 1, 2: 3, 3: 2}[link]

                @pl.when(go)
                def _():
                    pltpu.make_async_remote_copy(
                        src_ref=acc, dst_ref=lands_m[there].at[landing_index(order, there, tx, ty, tz)],
                        send_sem=send_at, recv_sem=recv_at(there), device_id=neighbours[link], device_id_type=MESH).start()

    def early(index):
        dx, dy, dz, valid, tx, ty, tz = dest_of(index)
        last = index == len(FAR_FIRST) - 1
        prefetch(index + 2)

        @pl.when(valid)
        def _():
            dest = chip_at(tx, ty, tz)
            for m in range(3):
                for copy in own_load(m, dest, index % 3):
                    copy.wait()
                for copy in to_sibling(m, dest):
                    copy.wait_recv()
                reduce_piece(BACK_ORDERS[m], lands[4 * m:4 * m + 4], send_sem.at[m, dest], lambda link: recv_sem.at[m, link, dest],
                             lambda: owns[m][index % 3], sibs[m].at[dest], (dx, dy, dz), (tx, ty, tz), last, (f_gate, f_up, down_out)[m])

    step = 256
    per_group = (GROUP // LANES) * (rows // step) * 2
    groups = xv.shape[1] // GROUP
    chunks = groups * per_group
    blocks = xv.shape[1] // LANES
    for load in loads[:7]:
        load.wait()

    def chunk(index):
        group, inner = index // per_group, index % per_group
        pair, block, head = inner // (per_group // 2), inner // 2 % (rows // step), inner % 2
        here = pl.ds(pl.multiple_of(block * step, step), step)
        lanes = pl.ds(pl.multiple_of(group * GROUP + pair * LANES, LANES), LANES)
        out_lanes = pl.ds(pl.multiple_of(pair * LANES, LANES), LANES)

        @pl.when(inner == 0)
        def _():
            dq[...] = jnp.zeros_like(dq)
            dk[...] = jnp.zeros_like(dk)
            dv[...] = jnp.zeros_like(dv)

        qp, gp = qv[here, lanes], gv[here, lanes]
        keep = lane_of(qp.shape) // HEAD == head
        qm, gm = jnp.where(keep, qp, jnp.zeros_like(qp)), jnp.where(keep, gp, jnp.zeros_like(gp))
        kp, vp = kv[:, lanes], vv[:, lanes]
        s = nt(kp, qm) + jnp.concatenate([biasv[...]] * (step // LANES), 1)
        p = jnp.exp(s - lsev[pl.ds(2 * (group * (GROUP // LANES) + pair) + head, 1), here])
        dp = nt(vp, gm)
        shares = gm.astype(F32) * attv[here, lanes].astype(F32)
        delta = lax.dot_general(jnp.ones((8, LANES), F32), shares, (((1,), (1,)), ((), ())),
                                precision=lax.Precision.HIGHEST, preferred_element_type=F32)[0:1, :]
        ds = (p * (dp - delta)).astype(LOW)
        dv[:, out_lanes] += nn(p.astype(LOW), gm)
        dk[:, out_lanes] += nn(ds, qm)
        dq[here, out_lanes] += jnp.where(keep, tn(ds, kp), 0.0)

        @pl.when(index == per_group - 1)
        def _():
            for load in loads[7:]:
                load.wait()
            xt[...] = xv[...].T
            oth_acc[...] = jnp.zeros_like(oth_acc)

        @pl.when(inner == per_group - 1)
        def _():
            finish(group)

    def finish(group):
        def back(u, cos, sin):
            return u * jnp.concatenate([cos, cos], 1) - turn(u) * jnp.concatenate([sin, sin], 1)

        def put(block, value):
            per = dw.shape[2] // LANES
            for i in range(2):
                b = block + i
                dw[b // per, :, pl.ds(pl.multiple_of(b % per * LANES, LANES), LANES)] = value[:, i * LANES:i * LANES + LANES].astype(LOW)

        def weights(block):
            per = dw.shape[2] // LANES
            return jnp.concatenate([wv[b // per, :, pl.ds(pl.multiple_of(b % per * LANES, LANES), LANES)] for b in (block, block + 1)], 1)

        gq = back(dq[...] * 0.125, cosv[mine, :], sinv[mine, :]).astype(LOW)
        dk[...] = back(dk[...], cosv[...], sinv[...])
        put(2 * group, nn(xt[:, mine], gq))
        put(blocks + 2 * group, nn(xt[...], dk[...].astype(LOW)))
        put(2 * blocks + 2 * group, nn(xt[...], dv[...].astype(LOW)))
        wq, wk, wvv = (weights(n * blocks + 2 * group) for n in range(3))
        own_acc[...] += nt(gq, wq) + nt(dk[mine, :].astype(LOW), wk) + nt(dv[mine, :].astype(LOW), wvv)
        oth_acc[...] += nt(dk[theirs, :].astype(LOW), wk) + nt(dv[theirs, :].astype(LOW), wvv)

    def turn_of(index, carry):
        chunk(index)

        @pl.when(index < mixed)
        def _():
            early(index)
        return carry

    mixed = min(chunks, len(FAR_FIRST) - 4)
    lax.fori_loop(0, chunks, turn_of, 0)

    gt_low[...] = oth_acc[...].astype(LOW)
    third = f_qkv.shape[1] // len(LATE_ORDERS)

    def late_to_sibling(dest):
        return pltpu.make_async_remote_copy(
            src_ref=cut(dw.at[other], rows_gate, dest), dst_ref=sibs[3].at[dest], send_sem=late_sib_send.at[dest],
            recv_sem=late_sib_recv.at[dest], device_id=sibling, device_id_type=MESH)

    def late_begin(index, carry):
        dx, dy, dz, valid, tx, ty, tz = dest_of(index)

        @pl.when(valid)
        def _():
            late_to_sibling(chip_at(tx, ty, tz)).start()
        return carry

    lax.fori_loop(0, len(FAR_FIRST), late_begin, 0)
    cross = pltpu.make_async_remote_copy(src_ref=gt_low, dst_ref=gt_sib, send_sem=gt_sem.at[0], recv_sem=gt_sem.at[1],
                                         device_id=sibling, device_id_type=MESH)
    cross.start()

    def late(offset):
        dx, dy, dz = offset
        final_step = offset == (0, 0, 0)

        def one():
            tx, ty, tz = (x + dx) % 2, (y + dy) % 2, z + dz
            dest = chip_at(tx, ty, tz)
            late_to_sibling(dest).wait_recv()
            for n, order in enumerate(LATE_ORDERS):
                lanes = slice(n * third, n * third + third)
                acc = sibs[3].at[dest, :, lanes]
                own = dw[core, pl.ds(pl.multiple_of(dest * rows_gate, rows_gate), rows_gate), lanes]
                total = f_qkv.at[:, lanes] if final_step else acc
                total[...] = (acc[...].astype(F32) + own.astype(F32)).astype(total.dtype)
                for link in onward(order, dx, dy, dz):
                    land = lands[12 + 4 * n + link].at[landing_index(order, link, tx, ty, tz)]

                    def add():
                        pltpu.make_async_copy(land, land, late_recv.at[n, link, dest]).wait()
                        total[...] += land[...].astype(total.dtype)
                    when({2: z < ZS - 1, 3: z > 0}.get(link, True), add)
                if not final_step:
                    link = next({"x": 0, "y": 1, "z": 2 if dz > 0 else 3}[axis] for axis in order[::-1] if {"x": dx, "y": dy, "z": dz}[axis])
                    there = {0: 0, 1: 1, 2: 3, 3: 2}[link]
                    pltpu.make_async_remote_copy(
                        src_ref=acc, dst_ref=lands[12 + 4 * n + there].at[landing_index(order, there, tx, ty, tz)],
                        send_sem=late_send.at[n, dest], recv_sem=late_recv.at[n, there, dest],
                        device_id=neighbours[link], device_id_type=MESH).start()
        when(True if dz == 0 else (z < ZS - dz if dz > 0 else z >= -dz), one)

    early_steps, left = 4, mixed
    for step_index, offset in enumerate(FAR_FIRST):
        if step_index == early_steps:
            cross.wait()
            gt_low[...] = (own_acc[...] + gt_sib[...].astype(F32)).astype(LOW)
            for j in range(half):
                from_slot(core, chip, j, gt_low, gt_out, tok_send, gt_recv)
        late(offset)
        if step_index % 2 == 1 and left < len(FAR_FIRST):
            early(jnp.int32(left))
            left += 1
    f_down[...] = down_out[0:rows_down, :]
    f_out[...] = down_out[rows_down:rows_down + rows_out, :]

    def small_end(s, carry):
        small_to(s).wait_send()
        source = (me + s) % (2 * CHIPS)
        pltpu.make_async_copy(smalls.at[source], smalls.at[source], small_recv.at[source]).wait()
        return carry

    lax.fori_loop(1, 2 * CHIPS, small_end, 0)
    own_small.wait()
    f_small[...] = jnp.sum(smalls[...], axis=0)

    sent_blocks(core, chip, gt_out.at[0], tok_send)
    lax.fori_loop(0, half, lambda i, c: (pltpu.make_async_copy(gt_out.at[i], gt_out.at[i], gt_recv.at[i]).wait(), c)[1], 0)

    def sent(dest, carry):
        for m in range(3):
            for copy in to_sibling(m, dest):
                copy.wait_send()
        late_to_sibling(dest).wait_send()

        @pl.when(dest != chip)
        def _():
            for m in range(3):
                pltpu.make_async_copy(sibs[m].at[dest], sibs[m].at[dest], send_sem.at[m, dest]).wait()
            for n in range(len(LATE_ORDERS)):
                part = sibs[3].at[dest, :, pl.ds(n * third, third)]
                pltpu.make_async_copy(part, part, late_send.at[n, dest]).wait()
        return carry

    lax.fori_loop(0, CHIPS, sent, 0)


def back_scatter(dwg, dwu, dwd, dwo, dsmall, x, w, q, k, v, g_att, g_res1, cos, sin, bias_col, att, lse):
    tokens, width = x.shape
    rows = tokens // 2
    span = rows // 8
    anywhere, vmem = pl.BlockSpec(memory_space=pl.ANY), pl.BlockSpec(memory_space=pltpu.VMEM)
    n_gate, n_down, n_out = width // CHIPS, dwd.shape[1] // CHIPS, dwo.shape[1] // CHIPS
    c_gate, c_down = dwg.shape[2], dwd.shape[2]
    c_qkv = 3 * width // 2
    third = c_qkv // len(LATE_ORDERS)
    sds, mem = jax.ShapeDtypeStruct, pltpu.VMEM
    out8 = sds((8, span, width), LOW)
    finals = [sds((n_gate, c_gate), F32), sds((n_gate, c_gate), F32), sds((n_down, c_down), F32), sds((n_out, c_down), F32),
              sds((n_gate, c_qkv), F32), sds(dsmall.shape[1:], F32)]
    pieces = [(n_gate, c_gate), (n_gate, c_gate), (n_down + n_out, c_down)]
    scratch = [mem((tokens, width), LOW), mem(w.shape, LOW), mem((rows, width), LOW), mem((tokens, width), LOW), mem((tokens, width), LOW),
               mem((rows, width), LOW), mem((rows, width), F32), mem(cos.shape, F32), mem(sin.shape, F32), mem(bias_col.shape, F32),
               mem((width, tokens), LOW), mem((rows, width), F32), mem((rows, GROUP), F32), mem((tokens, GROUP), F32), mem((tokens, GROUP), F32),
               mem((2, width, c_qkv), LOW), mem((rows, width), LOW), mem(lse.shape, F32)]
    scratch += [mem((3,) + piece, LOW) for piece in pieces]
    scratch += [mem((CHIPS,) + piece, LOW) for piece in pieces] + [mem((CHIPS, n_gate, c_qkv), LOW)]
    scratch += [mem(pieces[2], F32)]
    for order, piece in zip(BACK_ORDERS, pieces):
        scratch += [mem((n,) + piece, LOW) for n in landing_slots(order)]
    for order in LATE_ORDERS:
        scratch += [mem((n, n_gate, third), LOW) for n in landing_slots(order)]
    scratch += [mem((rows, width), LOW), mem((rows, width), LOW), mem(dsmall.shape, F32)]
    dma = pltpu.SemaphoreType.DMA
    scratch += [dma((12,)), dma((3, CHIPS)), dma((3, 4, CHIPS)), dma((4, CHIPS)), dma((4, CHIPS)), dma((4, 3)), dma((3, CHIPS)), dma((3, 4, CHIPS)),
                dma((CHIPS,)), dma((CHIPS,)), dma((2,)), dma((8,)), dma((8,)), dma((2 * CHIPS,)), dma((2 * CHIPS,))]
    return pl.pallas_call(
        back_scatter_kernel,
        out_shape=[out8] + finals,
        in_specs=[anywhere] * 17,
        out_specs=[anywhere] + [vmem] * len(finals),
        scratch_shapes=scratch,
        compiler_params=pltpu.CompilerParams(collective_id=1, has_side_effects=True, vmem_limit_bytes=67043328),
        name="back_scatter",
    )(dwg, dwu, dwd, dwo, dsmall, x, w, q, k, v, g_att, g_res1, cos, sin, bias_col, att, lse)


def rotary_turns(tokens, near):
    lane = jnp.arange(LANES)
    inverse = jnp.power(jnp.float32(1000.0), -2.0 * (lane % (HEAD // 2)).astype(F32) / HEAD)

    def table(positions):
        angles = positions.astype(F32)[:, None] * inverse[None, :]
        return jnp.stack([jnp.cos(angles), jnp.sin(angles)])

    return table(jnp.arange(0, tokens, near)), table(jnp.arange(near))


def local_by_slot(tokens, lengths, w_qkv, w_out, w_gate, w_up, w_down, ln_params, cotangent):
    slots, span, width = tokens.shape
    share = ln_params.shape[1]
    turns_far, turns_near = rotary_turns(span * CHIPS, span)
    x, cot, ln, w_in, wg, wu, wd, q, k, v, att, cos, sin, bias_col, lse = front(
        tokens, cotangent, w_qkv, w_out, w_gate, w_up, w_down, ln_params, lengths, turns_far, turns_near)
    y, dwg, dwu, dwd, dwo, g_att, g_res1, dln = middle(x, att, w_in, wg, wu, wd, cot, ln, bias_col)
    dsmall = dln[:4].reshape(4, 2 * CHIPS, share).transpose(1, 0, 2)
    dsmall = jnp.pad(dsmall, ((0, 0), (0, 4), (0, LANES - share)))
    results = back_scatter(dwg, dwu, dwd, dwo, dsmall, x, w_in, q, k, v, g_att, g_res1, cos, sin, bias_col, att, lse)
    output, grad_tokens, d_gate, d_up, d_down, d_out, d_qkv, d_small = finish([y, *results], share)
    return (output, grad_tokens, d_qkv, d_out, d_gate, d_up, d_down, d_small)


def solution(mesh):
    placed = (
        P("dp", "seq", None),
        P("dp"),
        P("seq", "dp"),
        P("seq", "dp"),
        P("seq", "dp"),
        P("seq", "dp"),
        P("seq", "dp"),
        P(None, ("dp", "seq")),
        P("dp", "seq", None),
    )

    def run(tokens, *rest):
        by_slot = mesh.shape["dp"] == 2 and mesh.shape["seq"] == CHIPS and tokens.shape[0] == CHIPS
        body = local_by_slot if by_slot else local
        return jax.shard_map(
            body,
            mesh=mesh,
            in_specs=placed,
            out_specs=(
                P("dp", "seq", None),
                P("dp", "seq", None),
                P("seq", "dp"),
                P("seq", "dp"),
                P("seq", "dp"),
                P("seq", "dp"),
                P("seq", "dp"),
                P(None, ("dp", "seq")),
            ),
            check_vma=False,
        )(tokens, *rest)

    return run
```

```python
import functools

import jax
import jax.numpy as jnp
import numpy as np
from jax import lax
from jax.experimental import pallas as pl
from jax.experimental.pallas import tpu as pltpu
from jax.sharding import PartitionSpec as P

HEADS = 12
HEAD_DIM = 64


norm_epsilon = 1e-12
score_scale = 0.125
masked_score = -1e30


def shifted(shard, axis, by):
    count = lax.axis_size(axis)
    return lax.ppermute(shard, axis, [(i, (i + by) % count) for i in range(count)])


def rotary_tables(positions):
    pair_index = jnp.arange(HEAD_DIM // 2, dtype=jnp.float32)
    inverse = jnp.power(jnp.float32(1000.0), -2.0 * pair_index / HEAD_DIM)
    angles = positions.astype(jnp.float32)[:, None] * inverse[None, :]
    cos_tab = jnp.concatenate([jnp.cos(angles), jnp.cos(angles)], axis=-1)
    sin_tab = jnp.concatenate([jnp.sin(angles), jnp.sin(angles)], axis=-1)
    return (cos_tab, sin_tab)


def rotate(values, cos_tab, sin_tab):
    half_dim = values.shape[-1] // 2
    turned = jnp.concatenate([-values[..., half_dim:], values[..., :half_dim]], axis=-1)
    return values * cos_tab + turned * sin_tab


def norm_parts(values, gain_vec, bias_vec):
    center = values - jnp.mean(values, axis=-1, keepdims=True)
    inv_std = lax.rsqrt(jnp.mean(center * center, axis=-1, keepdims=True) + norm_epsilon)
    normed = center * inv_std
    return (normed * gain_vec + bias_vec, normed, inv_std)


def norm_back(grad_in, normed, inv_std, gain_vec):
    scaled = grad_in * gain_vec
    return inv_std * (
        scaled
        - jnp.mean(scaled, axis=-1, keepdims=True)
        - normed * jnp.mean(scaled * normed, axis=-1, keepdims=True)
    )


def heads_view(flat_rows):
    return flat_rows.reshape(flat_rows.shape[0], flat_rows.shape[1], HEADS, HEAD_DIM)


def attend_block(run_state, queries, key_blk, value_blk, key_start, lengths):
    run_max, run_sum, run_acc = run_state
    scores = (
        jnp.einsum(
            "sqhd,skhd->shqk",
            heads_view(queries),
            heads_view(key_blk),
            preferred_element_type=jnp.float32,
        )
        * score_scale
    )
    key_pos = key_start + jnp.arange(key_blk.shape[1], dtype=jnp.int32)
    key_mask = (key_pos[None, :] < lengths[:, None])[:, None, None, :]
    scores = jnp.where(key_mask, scores, masked_score)
    new_max = jnp.maximum(run_max, jnp.max(scores, axis=-1))
    exp_scores = jnp.where(key_mask, jnp.exp(scores - new_max[..., None]), 0.0)
    factor = jnp.exp(run_max - new_max)
    run_sum = run_sum * factor + jnp.sum(exp_scores, axis=-1)
    run_acc = run_acc * factor[..., None] + jnp.einsum(
        "shqk,skhd->shqd",
        exp_scores.astype(jnp.bfloat16),
        heads_view(value_blk),
        preferred_element_type=jnp.float32,
    )
    return (new_max, run_sum, run_acc)


def block_grads(queries, grad_att, log_total, delta_rows, key_blk, value_blk, key_ok):
    query_h = heads_view(queries)
    grad_h = heads_view(grad_att)
    key_h = heads_view(key_blk)
    scores = (
        jnp.einsum("sqhd,skhd->shqk", query_h, key_h, preferred_element_type=jnp.float32)
        * score_scale
    )
    key_mask = key_ok[:, None, None, :]
    soft_probs = jnp.where(key_mask, jnp.exp(scores - log_total[..., None]), 0.0)
    grad_probs = jnp.einsum(
        "sqhd,skhd->shqk", grad_h, heads_view(value_blk), preferred_element_type=jnp.float32
    )
    grad_scores = (soft_probs * (grad_probs - delta_rows[..., None])).astype(jnp.bfloat16)
    part_q = (
        jnp.einsum("shqk,skhd->sqhd", grad_scores, key_h, preferred_element_type=jnp.float32)
        * score_scale
    )
    part_k = (
        jnp.einsum("shqk,sqhd->skhd", grad_scores, query_h, preferred_element_type=jnp.float32)
        * score_scale
    )
    part_v = jnp.einsum(
        "shqk,sqhd->skhd",
        soft_probs.astype(jnp.bfloat16),
        grad_h,
        preferred_element_type=jnp.float32,
    )
    shape_out = queries.shape
    return (part_q.reshape(shape_out), part_k.reshape(key_blk.shape), part_v.reshape(key_blk.shape))


def local(tokens, lengths, w_qkv, w_out, w_gate, w_up, w_down, ln_params, cotangent):
    slot_count, span_len, width = tokens.shape
    row_count = slot_count * span_len
    cycle_size = lax.axis_size("seq")
    my_index = lax.axis_index("seq")
    row_qkv, row_out, row_gate, row_up, row_down, row_norm = (
        lax.all_gather(w_qkv, "seq", axis=0, tiled=True),
        lax.all_gather(w_out, "seq", axis=0, tiled=True),
        lax.all_gather(w_gate, "seq", axis=0, tiled=True),
        lax.all_gather(w_up, "seq", axis=0, tiled=True),
        lax.all_gather(w_down, "seq", axis=0, tiled=True),
        lax.all_gather(ln_params, "seq", axis=1, tiled=True),
    )
    wide_qkv, wide_out, wide_gate, wide_up, wide_down, wide_norm = (
        lax.all_gather(row_qkv, "dp", axis=1, tiled=True),
        lax.all_gather(row_out, "dp", axis=1, tiled=True),
        lax.all_gather(row_gate, "dp", axis=1, tiled=True),
        lax.all_gather(row_up, "dp", axis=1, tiled=True),
        lax.all_gather(row_down, "dp", axis=1, tiled=True),
        lax.all_gather(row_norm, "dp", axis=1, tiled=True),
    )
    norm_full = wide_norm.astype(jnp.float32)
    flat_tokens = tokens.reshape(row_count, width)
    token_f32 = flat_tokens.astype(jnp.float32)
    positions = my_index * span_len + jnp.arange(span_len, dtype=jnp.int32)
    row_valid = (positions[None, :] < lengths[:, None]).astype(jnp.float32).reshape(row_count, 1)
    cos_tab, sin_tab = rotary_tables(positions)
    cos_four = cos_tab[None, :, None, :]
    sin_four = sin_tab[None, :, None, :]
    qkv_pre = jnp.dot(flat_tokens, wide_qkv, preferred_element_type=jnp.float32)
    split_qkv = qkv_pre.reshape(slot_count, span_len, 3, HEADS, HEAD_DIM)
    queries = (
        rotate(split_qkv[:, :, 0], cos_four, sin_four)
        .astype(jnp.bfloat16)
        .reshape(slot_count, span_len, width)
    )
    keys_rot = (
        rotate(split_qkv[:, :, 1], cos_four, sin_four)
        .astype(jnp.bfloat16)
        .reshape(slot_count, span_len, width)
    )
    values = split_qkv[:, :, 2].astype(jnp.bfloat16).reshape(slot_count, span_len, width)
    start_state = (
        jnp.full((slot_count, HEADS, span_len), masked_score, jnp.float32),
        jnp.zeros((slot_count, HEADS, span_len), jnp.float32),
        jnp.zeros((slot_count, HEADS, span_len, HEAD_DIM), jnp.float32),
    )
    key_piece = lax.all_gather(keys_rot, "seq", axis=1, tiled=True)
    value_piece = lax.all_gather(values, "seq", axis=1, tiled=True)
    block_count = key_piece.shape[1] // span_len

    def one_block(block_id, inner_state):
        offset = block_id * span_len
        key_blk = lax.dynamic_slice_in_dim(key_piece, offset, span_len, axis=1)
        value_blk = lax.dynamic_slice_in_dim(value_piece, offset, span_len, axis=1)
        return attend_block(inner_state, queries, key_blk, value_blk, offset, lengths)

    run_max, run_sum, run_acc = lax.fori_loop(0, block_count, one_block, start_state)
    attended = run_acc / run_sum[..., None]
    log_total = run_max + jnp.log(run_sum)
    attn_low = attended.transpose(0, 2, 1, 3).reshape(row_count, width).astype(jnp.bfloat16)
    branch = jnp.dot(attn_low, wide_out, preferred_element_type=jnp.float32)
    hidden, normed_one, inv_one = norm_parts(token_f32 + branch, norm_full[0], norm_full[1])
    hidden_low = hidden.astype(jnp.bfloat16)
    gate_pre = jnp.dot(hidden_low, wide_gate, preferred_element_type=jnp.float32)
    up_proj = jnp.dot(hidden_low, wide_up, preferred_element_type=jnp.float32)
    activated = jax.nn.silu(gate_pre)
    inner_low = (activated * up_proj).astype(jnp.bfloat16)
    branch_two = jnp.dot(inner_low, wide_down, preferred_element_type=jnp.float32)
    result, normed_two, inv_two = norm_parts(hidden + branch_two, norm_full[2], norm_full[3])
    output = (result * row_valid).astype(jnp.bfloat16).reshape(slot_count, span_len, width)
    back_qkv, back_out, back_gate, back_up, back_down, back_norm = (
        lax.all_gather(w_qkv, "seq", axis=0, tiled=True),
        lax.all_gather(w_out, "seq", axis=0, tiled=True),
        lax.all_gather(w_gate, "seq", axis=0, tiled=True),
        lax.all_gather(w_up, "seq", axis=0, tiled=True),
        lax.all_gather(w_down, "seq", axis=0, tiled=True),
        lax.all_gather(ln_params, "seq", axis=1, tiled=True),
    )
    wide_qkv, wide_out, wide_gate, wide_up, wide_down, wide_norm = (
        lax.all_gather(back_qkv, "dp", axis=1, tiled=True),
        lax.all_gather(back_out, "dp", axis=1, tiled=True),
        lax.all_gather(back_gate, "dp", axis=1, tiled=True),
        lax.all_gather(back_up, "dp", axis=1, tiled=True),
        lax.all_gather(back_down, "dp", axis=1, tiled=True),
        lax.all_gather(back_norm, "dp", axis=1, tiled=True),
    )
    norm_full = wide_norm.astype(jnp.float32)
    grad_out = cotangent.reshape(row_count, width).astype(jnp.float32) * row_valid
    gain_two_grad = jnp.sum(grad_out * normed_two, axis=0)
    bias_two_grad = jnp.sum(grad_out, axis=0)
    grad_res2 = norm_back(grad_out, normed_two, inv_two, norm_full[2])
    grad_branch2 = grad_res2.astype(jnp.bfloat16)
    grad_wdown = jnp.einsum(
        "rf,rd->fd", inner_low, grad_branch2, preferred_element_type=jnp.float32
    )
    grad_inner = jnp.einsum(
        "rd,fd->rf", grad_branch2, wide_down, preferred_element_type=jnp.float32
    )
    sigma = jax.nn.sigmoid(gate_pre)
    grad_gate = (grad_inner * up_proj * sigma * (1.0 + gate_pre * (1.0 - sigma))).astype(
        jnp.bfloat16
    )
    grad_up = (grad_inner * activated).astype(jnp.bfloat16)
    grad_wgate = jnp.einsum("rd,rf->df", hidden_low, grad_gate, preferred_element_type=jnp.float32)
    grad_wup = jnp.einsum("rd,rf->df", hidden_low, grad_up, preferred_element_type=jnp.float32)
    grad_hidden = (
        grad_res2
        + jnp.einsum("rf,df->rd", grad_gate, wide_gate, preferred_element_type=jnp.float32)
        + jnp.einsum("rf,df->rd", grad_up, wide_up, preferred_element_type=jnp.float32)
    )
    gain_one_grad = jnp.sum(grad_hidden * normed_one, axis=0)
    bias_one_grad = jnp.sum(grad_hidden, axis=0)
    grad_res1 = norm_back(grad_hidden, normed_one, inv_one, norm_full[0])
    grad_branch1 = grad_res1.astype(jnp.bfloat16)
    grad_wout = jnp.einsum("ri,rd->id", attn_low, grad_branch1, preferred_element_type=jnp.float32)
    grad_att = (
        jnp.einsum("rd,id->ri", grad_branch1, wide_out, preferred_element_type=jnp.float32)
        .astype(jnp.bfloat16)
        .reshape(slot_count, span_len, width)
    )
    zero_rows = jnp.zeros((slot_count, span_len, width), jnp.float32)
    delta_rows = jnp.einsum("sqhd,shqd->shq", heads_view(grad_att).astype(jnp.float32), attended)

    def key_turn(turn_id, run_state):
        key_cur, value_cur, grad_keys, grad_values, grad_query = run_state
        key_start = (my_index - turn_id) % cycle_size * span_len
        key_ok = (key_start + jnp.arange(span_len, dtype=jnp.int32))[None, :] < lengths[:, None]
        part_q, part_k, part_v = block_grads(
            queries, grad_att, log_total, delta_rows, key_cur, value_cur, key_ok
        )
        key_cur, value_cur = shifted((key_cur, value_cur), "seq", 1)
        grad_keys, grad_values = (
            shifted((grad_keys + part_k).astype(jnp.bfloat16), "seq", 1).astype(jnp.float32),
            shifted((grad_values + part_v).astype(jnp.bfloat16), "seq", 1).astype(jnp.float32),
        )
        return (key_cur, value_cur, grad_keys, grad_values, grad_query + part_q)

    key_cur, value_cur, grad_keys, grad_values, grad_query = lax.fori_loop(
        0, cycle_size - 1, key_turn, (keys_rot, values, zero_rows, zero_rows, zero_rows)
    )
    key_start = (my_index - (cycle_size - 1)) % cycle_size * span_len
    key_ok = (key_start + jnp.arange(span_len, dtype=jnp.int32))[None, :] < lengths[:, None]
    part_q, part_k, part_v = block_grads(
        queries, grad_att, log_total, delta_rows, key_cur, value_cur, key_ok
    )
    grad_query = grad_query + part_q
    grad_keys, grad_values = (
        shifted((grad_keys + part_k).astype(jnp.bfloat16), "seq", 1).astype(jnp.float32),
        shifted((grad_values + part_v).astype(jnp.bfloat16), "seq", 1).astype(jnp.float32),
    )
    query_back = rotate(heads_view(grad_query), cos_four, -sin_four)
    key_back = rotate(heads_view(grad_keys), cos_four, -sin_four)
    grad_qkv = jnp.stack([query_back, key_back, heads_view(grad_values)], axis=2)
    grad_qkv = grad_qkv.reshape(row_count, 3 * width).astype(jnp.bfloat16)
    grad_wqkv = jnp.einsum("rd,re->de", flat_tokens, grad_qkv, preferred_element_type=jnp.float32)
    grad_tokens = grad_res1 + jnp.einsum(
        "re,de->rd", grad_qkv, wide_qkv, preferred_element_type=jnp.float32
    )
    grad_tokens = grad_tokens.astype(jnp.bfloat16).reshape(slot_count, span_len, width)
    grad_norm = jnp.stack([gain_one_grad, bias_one_grad, gain_two_grad, bias_two_grad], axis=0)
    col_qkv, col_out, col_gate, col_up, col_down, col_norm = (
        lax.psum_scatter(
            grad_wqkv.astype(jnp.bfloat16), "dp", scatter_dimension=1, tiled=True
        ).astype(jnp.float32),
        lax.psum_scatter(
            grad_wout.astype(jnp.bfloat16), "dp", scatter_dimension=1, tiled=True
        ).astype(jnp.float32),
        lax.psum_scatter(
            grad_wgate.astype(jnp.bfloat16), "dp", scatter_dimension=1, tiled=True
        ).astype(jnp.float32),
        lax.psum_scatter(
            grad_wup.astype(jnp.bfloat16), "dp", scatter_dimension=1, tiled=True
        ).astype(jnp.float32),
        lax.psum_scatter(
            grad_wdown.astype(jnp.bfloat16), "dp", scatter_dimension=1, tiled=True
        ).astype(jnp.float32),
        lax.psum_scatter(
            grad_norm.astype(jnp.bfloat16), "dp", scatter_dimension=1, tiled=True
        ).astype(jnp.float32),
    )
    own_qkv, own_out, own_gate, own_up, own_down, own_norm = (
        lax.psum_scatter(
            col_qkv.astype(jnp.bfloat16), "seq", scatter_dimension=0, tiled=True
        ).astype(jnp.float32),
        lax.psum_scatter(
            col_out.astype(jnp.bfloat16), "seq", scatter_dimension=0, tiled=True
        ).astype(jnp.float32),
        lax.psum_scatter(
            col_gate.astype(jnp.bfloat16), "seq", scatter_dimension=0, tiled=True
        ).astype(jnp.float32),
        lax.psum_scatter(
            col_up.astype(jnp.bfloat16), "seq", scatter_dimension=0, tiled=True
        ).astype(jnp.float32),
        lax.psum_scatter(
            col_down.astype(jnp.bfloat16), "seq", scatter_dimension=0, tiled=True
        ).astype(jnp.float32),
        lax.psum_scatter(
            col_norm.astype(jnp.bfloat16), "seq", scatter_dimension=1, tiled=True
        ).astype(jnp.float32),
    )
    return (output, grad_tokens, own_qkv, own_out, own_gate, own_up, own_down, own_norm)


MESH = pl.DeviceIdType.MESH
CHIPS, ZS = 16, 4
OFFSETS = sorted(((dx, dy, dz) for dx in (0, 1) for dy in (0, 1) for dz in range(-3, 4)),
                 key=lambda o: (2 * (o[0] + o[1]) + abs(o[2]), abs(o[2]), o))


def pick(index, values):
    out = jnp.int32(0)
    for position, value in enumerate(values):
        if value:
            out = out + jnp.where(index == position, jnp.int32(value), 0)
    return out


def spread(order, dx, dy, dz):
    zero = {"x": dx == 0, "y": dy == 0, "z": dz == 0}
    flags = {}
    for position, axis in enumerate(order):
        flag = zero[axis] if axis != "z" else None
        for later in order[position + 1:]:
            flag = zero[later] if flag is None else flag & zero[later]
        flags[axis] = flag
    up, down = dz <= 0, dz >= 0
    if flags["z"] is not None:
        up, down = up & flags["z"], down & flags["z"]
    return flags["x"], flags["y"], up, down


def place():
    core, chip = lax.axis_index("dp"), lax.axis_index("seq")
    return core, chip, chip % 2, (chip // 2) % 2, chip // 4


def chip_at(x, y, z):
    return (z * 2 + y) * 2 + x


def meet_all(core, chip):
    greet_all(core, chip)
    all_here()


def onward(order, dx, dy, dz):
    zero = {"x": dx == 0, "y": dy == 0, "z": dz == 0}
    links = []
    for position, axis in enumerate(order):
        if all(zero[later] for later in order[position + 1:]):
            if axis == "z":
                links += [2] * (dz <= 0) + [3] * (dz >= 0)
            elif zero[axis]:
                links.append("xy".index(axis))
    return links


def when(condition, action):
    if condition is True:
        action()
    else:
        pl.when(condition)(action)


def to_slot(core, chip, j, source, target, sends, recvs):
    half = CHIPS // 2
    slot = (chip + 1 + j) % half
    to = core * half + slot
    src = source.at[slot]
    self_copy = (chip // half == core) & (to == chip)

    @pl.when(self_copy)
    def _():
        pltpu.make_async_copy(src, target, recvs.at[chip % half]).start()

    @pl.when(jnp.logical_not(self_copy))
    def _():
        pltpu.make_async_remote_copy(
            src_ref=src, dst_ref=target, send_sem=sends.at[slot], recv_sem=recvs.at[chip % half],
            device_id={"dp": chip // half, "seq": to}, device_id_type=MESH).start()


def from_slot(core, chip, j, source, target, sends, recvs):
    half = CHIPS // 2
    i = (chip + 1 + j) % half
    to_core, to_chip = chip // half, core * half + i
    span = target.shape[1]
    src, dst = source.at[pl.ds(pl.multiple_of(i * span, span), span)], target.at[chip % half]
    self_copy = (to_core == core) & (to_chip == chip)

    @pl.when(self_copy)
    def _():
        pltpu.make_async_copy(src, dst, recvs.at[chip % half]).start()

    @pl.when(jnp.logical_not(self_copy))
    def _():
        pltpu.make_async_remote_copy(
            src_ref=src, dst_ref=dst, send_sem=sends.at[i], recv_sem=recvs.at[chip % half],
            device_id={"dp": to_core, "seq": to_chip}, device_id_type=MESH).start()


def sent_blocks(core, chip, part, sends):
    half = CHIPS // 2

    def one(i, carry):
        @pl.when(jnp.logical_not((chip // half == core) & (core * half + i == chip)))
        def _():
            pltpu.make_async_copy(part, part, sends.at[i]).wait()
        return carry

    lax.fori_loop(0, half, one, 0)


def greet_all(core, chip):
    barrier = pltpu.get_barrier_semaphore()
    me = core * CHIPS + chip

    def greet(step, carry):
        other = (me + step) % (2 * CHIPS)
        pl.semaphore_signal(barrier, inc=1, device_id={"dp": other // CHIPS, "seq": other % CHIPS}, device_id_type=MESH)
        return carry

    lax.fori_loop(1, 2 * CHIPS, greet, 0)


def all_here():
    pl.semaphore_wait(pltpu.get_barrier_semaphore(), 2 * CHIPS - 1)


LOW, F32 = jnp.bfloat16, jnp.float32
EPS = 1e-12
HEAD = 64
LANES = 128
GROUP = 256
FULL = pl.BlockSpec(memory_space=pltpu.VMEM)


def nn(a, b):
    return jnp.dot(a, b, preferred_element_type=F32)


def nt(a, b):
    return lax.dot_general(a, b, (((1,), (1,)), ((), ())), preferred_element_type=F32)


def tn(a, b):
    return lax.dot_general(a, b, (((0,), (0,)), ((), ())), preferred_element_type=F32)


def lane_of(shape):
    return lax.broadcasted_iota(jnp.int32, shape, 1)


def turn(u):
    parts = []
    for start in range(0, u.shape[1], LANES):
        part = u[:, start:start + LANES]
        first = lane_of(part.shape) % HEAD < HEAD // 2
        parts.append(jnp.where(first, pltpu.roll(part, LANES - HEAD // 2, 1), pltpu.roll(part, HEAD // 2, 1)))
    return jnp.concatenate(parts, 1)


def ln_parts(u):
    center = u - jnp.mean(u, axis=1, keepdims=True)
    inv = lax.rsqrt(jnp.mean(center * center, axis=1, keepdims=True) + EPS)
    return center * inv, inv


def ln_back(g, n, inv):
    return inv * (g - jnp.mean(g, axis=1, keepdims=True) - n * jnp.mean(g * n, axis=1, keepdims=True))


def middle_kernel(tiles, x_ref, att_ref, wo_ref, wg_ref, wu_ref, wd_ref, cot_ref, ln_ref, bias_ref,
                  y_out, dwg_ref, dwu_ref, dwd_ref, dwo_ref, gatt_ref, gres_ref, small_ref,
                  n1_ref, inv1_ref, hid_ref, hidt_ref, gate_ref, up_ref, acc_ref, gb_ref, y_ref, dln_ref, y_send, y_recv):
    index = pl.program_id(0)
    width = x_ref.shape[1]
    half = width // 2
    rows = att_ref.shape[0]
    core, chip = lax.axis_index("dp"), lax.axis_index("seq")
    mine = pl.ds(pl.multiple_of(core * rows, rows), rows)
    eighth = CHIPS // 2

    def wide(ref):
        return jnp.concatenate([ref[0], ref[1]], 1)

    @pl.when(index == 0)
    def _():
        greet_all(core, chip)
        n1, inv1 = ln_parts(x_ref[mine, :].astype(F32) + nn(att_ref[...], wide(wo_ref)))
        hidden = n1 * ln_ref[0:1, :] + ln_ref[1:2, :]
        n1_ref[...] = n1
        inv1_ref[...] = jnp.broadcast_to(inv1, inv1_ref.shape)
        acc_ref[...] = hidden
        low = hidden.astype(LOW)
        hid_ref[...] = low
        hidt_ref[...] = low.T

    tile = wg_ref.shape[2]
    f = jnp.where(index < tiles, index, index - tiles)
    cols = pl.ds(pl.multiple_of(f * tile, tile), tile)

    @pl.when(index < tiles)
    def _():
        gate, up = nn(hid_ref[...], wg_ref[0]), nn(hid_ref[...], wu_ref[0])
        gate_ref[:, cols] = gate
        up_ref[:, cols] = up
        acc_ref[...] += nn((gate * jax.nn.sigmoid(gate) * up).astype(LOW), wide(wd_ref))

    @pl.when(index == tiles - 1)
    def _():
        n2, inv2 = ln_parts(acc_ref[...])
        all_here()
        valid = jnp.where(bias_ref[mine, 0:1] == 0.0, 1.0, 0.0)
        y_ref[...] = ((n2 * ln_ref[2:3, :] + ln_ref[3:4, :]) * valid).astype(LOW)
        for j in range(eighth):
            from_slot(core, chip, j, y_ref, y_out, y_send, y_recv)
        g_y = cot_ref[...].astype(F32) * valid
        dln_ref[2:3, :] = jnp.sum(g_y * n2, axis=0, keepdims=True)
        dln_ref[3:4, :] = jnp.sum(g_y, axis=0, keepdims=True)
        g_res2 = ln_back(g_y * ln_ref[2:3, :], n2, inv2)
        acc_ref[...] = g_res2
        gb_ref[...] = g_res2.astype(LOW)

    @pl.when(index >= tiles)
    def _():
        gate, up = gate_ref[:, cols], up_ref[:, cols]
        sig = jax.nn.sigmoid(gate)
        act = gate * sig
        gb = gb_ref[...]
        dwd = tn((act * up).astype(LOW), gb)
        dwd_ref[0] = dwd[:, :half].astype(LOW)
        dwd_ref[1] = dwd[:, half:].astype(LOW)
        g_inner = nt(gb, wide(wd_ref))
        g_gate = (g_inner * up * sig * (1.0 + gate * (1.0 - sig))).astype(LOW)
        g_up = (g_inner * act).astype(LOW)
        dwg_ref[0] = nn(hidt_ref[...], g_gate).astype(LOW)
        dwu_ref[0] = nn(hidt_ref[...], g_up).astype(LOW)
        acc_ref[...] += nt(g_gate, wg_ref[0]) + nt(g_up, wu_ref[0])

    @pl.when(index == 2 * tiles - 1)
    def _():
        g_hidden, n1 = acc_ref[...], n1_ref[...]
        dln_ref[0:1, :] = jnp.sum(g_hidden * n1, axis=0, keepdims=True)
        dln_ref[1:2, :] = jnp.sum(g_hidden, axis=0, keepdims=True)
        g_res1 = ln_back(g_hidden * ln_ref[0:1, :], n1, inv1_ref[:, 0:1])
        gres_ref[...] = g_res1
        gb1 = g_res1.astype(LOW)
        dwo = tn(att_ref[...], gb1)
        dwo_ref[0] = dwo[:, :half].astype(LOW)
        dwo_ref[1] = dwo[:, half:].astype(LOW)
        gatt_ref[...] = nt(gb1, wide(wo_ref)).astype(LOW)
        small_ref[...] = jnp.zeros_like(small_ref)
        share = width // (2 * CHIPS)
        for device in range(2 * CHIPS):
            small_ref[device, 0:4, 0:share] = dln_ref[0:4, device * share:device * share + share]
        sent_blocks(core, chip, y_out.at[0], y_send)
        lax.fori_loop(0, eighth, lambda i, carry: (pltpu.make_async_copy(y_out.at[i], y_out.at[i], y_recv.at[i]).wait(), carry)[1], 0)


def middle(x, att, wo, wg, wu, wd, cot, ln, bias_col):
    rows, width = att.shape
    hidden = wd.shape[1]
    tile = 512
    tiles = hidden // tile
    anywhere = pl.BlockSpec(memory_space=pl.ANY)
    per = wg.shape[2] // tile
    at = lambda i: jnp.where(i < tiles, i, i - tiles)
    late = lambda i: jnp.maximum(i - tiles, 0)
    cols = lambda pick: pl.BlockSpec((1, width, tile), lambda i: (pick(i) // per, 0, pick(i) % per))
    rowb = lambda pick: pl.BlockSpec((2, tile, wd.shape[2]), lambda i: (0, pick(i), 0))
    sds = jax.ShapeDtypeStruct
    return pl.pallas_call(
        functools.partial(middle_kernel, tiles), grid=(2 * tiles,),
        out_shape=[sds((8, rows // 8, width), LOW), sds(wg.shape, LOW), sds(wu.shape, LOW), sds(wd.shape, LOW), sds((2, width, width // 2), LOW),
                   sds((rows, width), LOW), sds((rows, width), F32), sds((2 * CHIPS, 8, LANES), F32)],
        in_specs=[FULL, FULL, pl.BlockSpec((2, width, width // 2), lambda i: (0, 0, 3)), cols(at), cols(at), rowb(at), FULL, FULL, FULL],
        out_specs=[anywhere, cols(late), cols(late), rowb(late), FULL, FULL, FULL, FULL],
        scratch_shapes=[pltpu.VMEM((rows, width), F32), pltpu.VMEM((rows, LANES), F32), pltpu.VMEM((rows, width), LOW),
                        pltpu.VMEM((width, rows), LOW), pltpu.VMEM((rows, hidden), F32), pltpu.VMEM((rows, hidden), F32),
                        pltpu.VMEM((rows, width), F32), pltpu.VMEM((rows, width), LOW), pltpu.VMEM((rows, width), LOW), pltpu.VMEM((8, width), F32)]
        + [pltpu.SemaphoreType.DMA((8,))] * 2,
        compiler_params=pltpu.CompilerParams(collective_id=2, has_side_effects=True, vmem_limit_bytes=60 << 20),
        cost_estimate=pl.CostEstimate(flops=24 * 10**9, bytes_accessed=6 * 10**7, transcendentals=3 * 10**6),
        name="middle")(x, att, wo, wg, wu, wd, cot, ln, bias_col)


def finish_kernel(count, share, *refs):
    sources, targets, holds, (in_sem, out_sem) = refs[:count], refs[count:2 * count], refs[2 * count:3 * count], refs[3 * count:]
    loads = [pltpu.make_async_copy(source, hold, in_sem.at[n]) for n, (source, hold) in enumerate(zip(sources, holds))]
    stores = [pltpu.make_async_copy(hold, target, out_sem.at[n]) for n, (hold, target) in enumerate(zip(holds[:-1], targets[:-1]))]
    for load in loads:
        load.start()
    for load, store in zip(loads[:-1], stores):
        load.wait()
        store.start()
    loads[-1].wait()
    targets[-1][...] = holds[-1][0:4, 0:share]
    for store in stores:
        store.wait()


def finish(results, share):
    count = len(results)
    anywhere = pl.BlockSpec(memory_space=pl.ANY)
    shapes = [jax.ShapeDtypeStruct(r.shape, r.dtype) for r in results]
    shapes[-1] = jax.ShapeDtypeStruct((4, share), results[-1].dtype)
    return pl.pallas_call(
        functools.partial(finish_kernel, count, share), out_shape=shapes,
        in_specs=[anywhere] * count, out_specs=[anywhere] * (count - 1) + [FULL],
        scratch_shapes=[pltpu.VMEM(r.shape, r.dtype) for r in results] + [pltpu.SemaphoreType.DMA((count,))] * 2,
        name="finish")(*results)

FIRST_ORDERS = ("yzx", "xzy", "zyx", "zxy")
REST_ORDERS = ("xzy", "zyx", "zyx")
REST_STARTS = (12, 6, 0)
REST_MIXES = 20
TOKENS_AT = (1, 4, 7, 10, 13, 16, 18, 20)
COTS_AT = (2, 3, 4, 5, 6, 7, 8, 9)
CHUNK = 256


def front_kernel(tok, cot, w_qkv, w_out, w_gate, w_up, w_down, ln_in, len_in, turns_far, turns_near,
                 x_all, c_own, ln_out, w_first, wide_gate, wide_up, wide_down, q_out, k_out, v_out, att_out, cos_out, sin_out, bias_out, lse_out, *refs):
    (xv, wv, qv, kv, vv, attv, cosv, sinv, biasv, rowv, small, smalls, lnv, lsev), refs = refs[:14], refs[14:]
    (first_send, first_recv, first_sib, rest_send, rest_recv, rest_sib, own_sem, tok_send, tok_recv, tok_sib, cot_recv,
     small_send, small_recv, out_sem) = refs
    core, chip, x, y, z = place()
    other = 1 - core
    slots, span = tok.shape[0], tok.shape[1]
    half = CHIPS // 2
    me = core * CHIPS + chip
    rows, width = qv.shape
    can = (True, True, z < ZS - 1, z > 0, True)
    neighbours = (
        {"dp": core, "seq": chip_at(1 - x, y, z)},
        {"dp": core, "seq": chip_at(x, 1 - y, z)},
        {"dp": core, "seq": chip_at(x, y, jnp.minimum(z + 1, ZS - 1))},
        {"dp": core, "seq": chip_at(x, y, jnp.maximum(z - 1, 0))},
        {"dp": other, "seq": chip},
    )
    shards, wides = (w_gate, w_up, w_down), (wide_gate, wide_up, wide_down)
    n_first = w_out.shape[0]
    c_first = w_out.shape[1]

    def first_region(n, owner, source):
        return wv.at[owner, pl.ds(pl.multiple_of(source * n_first, n_first), n_first), n * c_first:n * c_first + c_first]

    def first_own(n):
        return w_out if n == 3 else w_qkv.at[:, n * c_first:n * c_first + c_first]

    def rest_region(m, owner, source):
        size = shards[m].shape[0]
        return wides[m].at[owner, pl.ds(pl.multiple_of(source * size, size), size)]

    def first_piece(n, source, link, own=False):
        target = first_region(n, core, source)
        return pltpu.make_async_remote_copy(
            src_ref=first_own(n) if own else target, dst_ref=target, send_sem=first_send.at[n, link, source],
            recv_sem=first_sib.at[n, source] if link == 4 else first_recv.at[n, source],
            device_id=neighbours[link], device_id_type=MESH)

    def rest_piece(m, source, link, own=False):
        target = rest_region(m, core, source)
        return pltpu.make_async_remote_copy(
            src_ref=shards[m] if own else target, dst_ref=target, send_sem=rest_send.at[m, link, source],
            recv_sem=rest_sib.at[m, source] if link == 4 else rest_recv.at[m, source],
            device_id=neighbours[link], device_id_type=MESH)

    def valid(offset):
        dz = offset[2]
        return True if dz == 0 else (z < ZS - dz if dz > 0 else z >= -dz)

    def source_at(offset):
        return chip_at((x + offset[0]) % 2, (y + offset[1]) % 2, z + offset[2])

    def arrive(piece, orders, offset):
        def one():
            source = source_at(offset)
            for m, order in enumerate(orders):
                piece(m, source, 0).wait_recv()
                for link in onward(order, *offset) + [4]:
                    when(can[link], piece(m, source, link).start)
        when(valid(offset), one)

    def send_own(piece, orders, m):
        for link in onward(orders[m], 0, 0, 0) + [4]:
            when(can[link], piece(m, chip, link, own=True).start)

    def drain(piece, orders):
        for offset in OFFSETS:
            def one():
                source = source_at(offset)
                for m, order in enumerate(orders):
                    for link in onward(order, *offset) + [4]:
                        when(can[link], piece(m, source, link).wait_send)
            when(valid(offset), one)

    def rows_of(ref, index):
        return ref.at[pl.ds(pl.multiple_of(index * span, span), span)]

    def deliver(j, source, target, sends, recvs):
        slot = (chip + 1 + j) % half
        to = core * half + slot
        src, dst = source.at[slot], target
        self_copy = (chip // half == core) & (to == chip)

        @pl.when(self_copy)
        def _():
            pltpu.make_async_copy(src, dst, recvs.at[chip % half]).start()

        @pl.when(jnp.logical_not(self_copy))
        def _():
            pltpu.make_async_remote_copy(
                src_ref=src, dst_ref=dst, send_sem=sends.at[slot], recv_sem=recvs.at[chip % half],
                device_id={"dp": chip // half, "seq": to}, device_id_type=MESH).start()

    def small_to(step):
        to = (me + step) % (2 * CHIPS)
        return pltpu.make_async_remote_copy(
            src_ref=small, dst_ref=smalls.at[me], send_sem=small_send.at[step], recv_sem=small_recv.at[me],
            device_id={"dp": to // CHIPS, "seq": to % CHIPS}, device_id_type=MESH)

    lane = lax.broadcasted_iota(jnp.int32, (1, LANES), 1)
    counts = jnp.zeros((1, LANES), F32)
    for j in range(slots):
        counts = counts + jnp.where(lane == j, len_in[j].astype(F32), 0.0)
    small[...] = jnp.zeros_like(small)
    small[0:ln_in.shape[0], 0:ln_in.shape[1]] = ln_in[...].astype(F32)
    small[4:5, :] = counts
    meet_all(core, chip)

    for n in range(4):
        send_own(first_piece, FIRST_ORDERS, n)
        pltpu.make_async_copy(first_own(n), first_region(n, core, chip), own_sem.at[n]).start()
    lax.fori_loop(1, 2 * CHIPS, lambda s, c: (small_to(s).start(), c)[1], 0)
    own_small = pltpu.make_async_copy(small, smalls.at[me], small_recv.at[me])
    own_small.start()

    sign = jnp.where(lane % HEAD < HEAD // 2, -1.0, 1.0).astype(F32)
    near = turns_near.shape[1]
    for far in range(turns_far.shape[1]):
        part = slice(far * near, far * near + near)
        ca, sa = turns_far[0, far:far + 1, :], turns_far[1, far:far + 1, :]
        cosv[part, :] = ca * turns_near[0] - sa * turns_near[1]
        sinv[part, :] = (sa * turns_near[0] + ca * turns_near[1]) * sign

    def relay(i, carry):
        block = rows_of(xv, core * half + i)
        pltpu.make_async_copy(block, block, tok_recv.at[i]).wait()
        pltpu.make_async_remote_copy(
            src_ref=block, dst_ref=block, send_sem=tok_send.at[2, i], recv_sem=tok_sib.at[i],
            device_id=neighbours[4], device_id_type=MESH).start()
        return carry

    waiting = list(OFFSETS[1:])
    for index, offset in enumerate(OFFSETS[1:]):
        for j in range(half):
            if index == TOKENS_AT[j]:
                deliver(j, tok, rows_of(xv, chip), tok_send.at[0], tok_recv)
        for m in range(3):
            if index == REST_STARTS[m]:
                send_own(rest_piece, REST_ORDERS, m)
                pltpu.make_async_copy(shards[m], rest_region(m, core, chip), own_sem.at[4 + m]).start()
        arrive(first_piece, FIRST_ORDERS, offset)
        if index >= REST_MIXES:
            arrive(rest_piece, REST_ORDERS, waiting.pop(0))

    def first_in(source, carry):
        for n in range(4):
            block = first_region(n, other, source)
            pltpu.make_async_copy(block, block, first_sib.at[n, source]).wait()
        return carry

    def small_in(step, carry):
        source = (me + step) % (2 * CHIPS)
        pltpu.make_async_copy(smalls.at[source], smalls.at[source], small_recv.at[source]).wait()
        return carry

    def tok_in(i, carry):
        block = rows_of(xv, other * half + i)
        pltpu.make_async_copy(block, block, tok_sib.at[i]).wait()
        return carry

    lax.fori_loop(0, half, relay, 0)
    lax.fori_loop(0, half, tok_in, 0)
    lax.fori_loop(0, CHIPS, first_in, 0)
    for n in range(4):
        pltpu.make_async_copy(first_own(n), first_region(n, core, chip), own_sem.at[n]).wait()
    lax.fori_loop(1, 2 * CHIPS, small_in, 0)
    own_small.wait()
    norms, share = ln_in.shape
    lnv[...] = jnp.zeros_like(lnv)
    lnv[0:norms, :] = jnp.concatenate([smalls[device, 0:norms, 0:share] for device in range(2 * CHIPS)], 1)
    counted = smalls[chip // half * CHIPS, 4:5, :]
    length = jnp.sum(jnp.where(lane == chip % half, counted, 0.0), axis=1, keepdims=True)
    at_row = lax.broadcasted_iota(jnp.int32, biasv.shape, 0).astype(F32)
    biasv[...] = jnp.where(at_row < length, 0.0, masked_score)
    at_lane = lax.broadcasted_iota(jnp.int32, rowv.shape, 1).astype(F32)
    rowv[...] = jnp.where(at_lane < length, 0.0, masked_score)
    outs = [pltpu.make_async_copy(source, target, out_sem.at[n]) for n, (source, target) in enumerate((
        (xv, x_all), (wv, w_first), (lnv, ln_out), (cosv, cos_out), (sinv, sin_out), (biasv, bias_out),
        (qv, q_out), (kv, k_out), (vv, v_out), (attv, att_out), (lsev, lse_out)))]
    for copy in outs[:6]:
        copy.start()

    mine = pl.ds(pl.multiple_of(core * rows, rows), rows)
    blocks = width // LANES
    per = 3 * blocks // 2

    def weights(block):
        return jnp.concatenate([wv[b // per, :, pl.ds(pl.multiple_of(b % per * LANES, LANES), LANES)] for b in (block, block + 1)], 1)

    def turned(u, cos, sin):
        return u * jnp.concatenate([cos, cos], 1) + turn(u) * jnp.concatenate([sin, sin], 1)

    per_group = (GROUP // LANES) * (rows // CHUNK)
    chunks = width // GROUP * per_group

    def chunk(index, carry):
        group, inner = index // per_group, index % per_group
        cols = pl.ds(pl.multiple_of(group * GROUP, GROUP), GROUP)

        @pl.when(inner == 0)
        def _():
            q = turned(nn(xv[mine, :], weights(2 * group)), cosv[mine, :], sinv[mine, :]).astype(LOW)
            qv[:, cols] = q * jnp.asarray(0.125, LOW)
            kv[:, cols] = turned(nn(xv[...], weights(blocks + 2 * group)), cosv[...], sinv[...]).astype(LOW)
            vv[:, cols] = nn(xv[...], weights(2 * blocks + 2 * group)).astype(LOW)

        pair, block = inner // (rows // CHUNK), inner % (rows // CHUNK)
        here = pl.ds(pl.multiple_of(block * CHUNK, CHUNK), CHUNK)
        lanes = pl.ds(pl.multiple_of(group * GROUP + pair * LANES, LANES), LANES)
        qp, kp, vp = qv[here, lanes], kv[:, lanes], vv[:, lanes]
        low = lane_of(qp.shape) < HEAD
        parts = []
        for head in range(2):
            qm = jnp.where(low if head == 0 else jnp.logical_not(low), qp, jnp.zeros_like(qp))
            s = nt(qm, kp) + rowv[0:1, :]
            top = jnp.max(s, axis=1, keepdims=True)
            p = jnp.exp(s - top)
            total = jnp.sum(p, axis=1, keepdims=True)
            at_head = pl.ds(2 * (group * (GROUP // LANES) + pair) + head, 1)
            lsev[at_head, here] = jnp.broadcast_to(top + jnp.log(total), (CHUNK, LANES)).T[0:1, :]
            parts.append(nn(p.astype(LOW), vp) / total)
        attv[here, lanes] = jnp.where(low, parts[0], parts[1]).astype(LOW)

        for k in range(chunks):
            @pl.when(index == k)
            def _():
                for j in range(half):
                    if k == COTS_AT[j]:
                        deliver(j, cot, rows_of(c_own, chip % half), tok_send.at[1], cot_recv)
                if waiting:
                    arrive(rest_piece, REST_ORDERS, waiting.pop(0))
        return carry

    lax.fori_loop(0, chunks, chunk, 0)
    for copy in outs[6:]:
        copy.start()
    while waiting:
        arrive(rest_piece, REST_ORDERS, waiting.pop(0))

    def ends(i, carry):
        block = rows_of(c_own, i)
        pltpu.make_async_copy(block, block, cot_recv.at[i]).wait()
        block = rows_of(xv, core * half + i)
        pltpu.make_async_copy(block, block, tok_send.at[2, i]).wait()
        self_copy = (chip // half == core) & (core * half + i == chip)

        @pl.when(jnp.logical_not(self_copy))
        def _():
            pltpu.make_async_copy(tok.at[i], tok.at[i], tok_send.at[0, i]).wait()
            pltpu.make_async_copy(cot.at[i], cot.at[i], tok_send.at[1, i]).wait()
        return carry

    def rest_in(source, carry):
        for m in range(3):
            block = rest_region(m, other, source)
            pltpu.make_async_copy(block, block, rest_sib.at[m, source]).wait()
        return carry

    lax.fori_loop(1, 2 * CHIPS, lambda s, c: (small_to(s).wait_send(), c)[1], 0)
    lax.fori_loop(0, half, ends, 0)
    drain(first_piece, FIRST_ORDERS)
    drain(rest_piece, REST_ORDERS)
    lax.fori_loop(0, CHIPS, rest_in, 0)
    for m in range(3):
        pltpu.make_async_copy(shards[m], rest_region(m, core, chip), own_sem.at[4 + m]).wait()
    for copy in outs:
        copy.wait()


def front(tokens, cotangent, w_qkv, w_out, w_gate, w_up, w_down, ln_params, lengths, turns_far, turns_near):
    slots, span, width = tokens.shape
    total, rows = span * CHIPS, span * CHIPS // 2
    sds, mem, dma = jax.ShapeDtypeStruct, pltpu.VMEM, pltpu.SemaphoreType.DMA
    anywhere, vmem, smem = (pl.BlockSpec(memory_space=s) for s in (pl.ANY, pltpu.VMEM, pltpu.SMEM))
    wide = lambda w: sds((2, w.shape[0] * CHIPS, w.shape[1]), LOW)
    first = (2, width, w_qkv.shape[1] + w_out.shape[1])
    table, small = (total, LANES), (8, LANES)
    outs = [sds((total, width), LOW), sds((rows, width), LOW), sds((8, width), F32), sds(first, LOW),
            wide(w_gate), wide(w_up), wide(w_down), sds((rows, width), LOW), sds((total, width), LOW), sds((total, width), LOW),
            sds((rows, width), LOW), sds(table, F32), sds(table, F32), sds(table, F32), sds((16, rows), F32)]
    return pl.pallas_call(
        front_kernel,
        out_shape=outs,
        in_specs=[anywhere] * 7 + [vmem, smem, vmem, vmem],
        out_specs=[anywhere] * len(outs),
        scratch_shapes=[
            mem((total, width), LOW), mem(first, LOW), mem((rows, width), LOW), mem((total, width), LOW), mem((total, width), LOW),
            mem((rows, width), LOW), mem(table, F32), mem(table, F32), mem(table, F32), mem((8, total), F32), mem(small, F32),
            mem((2 * CHIPS,) + small, F32), mem((8, width), F32), mem((16, rows), F32),
            dma((4, 5, CHIPS)), dma((4, CHIPS)), dma((4, CHIPS)), dma((3, 5, CHIPS)), dma((3, CHIPS)), dma((3, CHIPS)), dma((7,)),
            dma((3, 8)), dma((8,)), dma((8,)), dma((8,)), dma((2 * CHIPS,)), dma((2 * CHIPS,)), dma((11,))],
        compiler_params=pltpu.CompilerParams(collective_id=0, has_side_effects=True, vmem_limit_bytes=60 << 20),
        name="front",
    )(tokens, cotangent, w_qkv, w_out, w_gate, w_up, w_down, ln_params, lengths, turns_far, turns_near)

BACK_ORDERS = ("xzy", "zyx", "zyx")
LATE_ORDERS = ("zxy", "zyx", "zxy")
FAR_FIRST = OFFSETS[::-1]
SIDES = {"x": 2, "y": 2, "z": ZS}


def far_first(index):
    words = [sum((o[0] + 2 * o[1] + 4 * (o[2] + 3)) << (5 * place) for place, o in enumerate(FAR_FIRST[start:start + 6]))
             for start in range(0, len(FAR_FIRST), 6)]
    word = jnp.int32(words[0])
    for place, value in enumerate(words[1:], 1):
        word = jnp.where(index >= 6 * place, jnp.int32(value), word)
    code = lax.shift_right_logical(word, 5 * (index % 6)) & 31
    return code & 1, lax.shift_right_logical(code, 1) & 1, lax.shift_right_logical(code, 2) - 3


def landing_slots(order):
    sizes, room = {}, 1
    for axis in order:
        sizes[axis] = room * (ZS if axis == "z" else 1)
        room *= SIDES[axis]
    return sizes["x"], sizes["y"], sizes["z"], sizes["z"]


def landing_index(order, link, x, y, z):
    axis = "xyzz"[link]
    index = 0
    for before in order:
        if before == axis:
            break
        index = index * SIDES[before] + {"x": x, "y": y, "z": z}[before]
    return index * ZS + z if axis == "z" else index


def back_scatter_kernel(dwg, dwu, dwd, dwo, dsmall, x_in, w_in, q_in, k_in, v_in, g_in, res_in, cos_in, sin_in, bias_in, att_in, lse_in,
                        gt_out, f_gate, f_up, f_down, f_out, f_qkv, f_small, *refs):
    (xv, wv, qv, kv, vv, gv, own_acc, cosv, sinv, biasv, xt, oth_acc, dq, dk, dv, dw, attv, lsev), refs = refs[:18], refs[18:]
    owns, refs = refs[:3], refs[3:]
    sibs, refs = refs[:4], refs[4:]
    down_out, refs = refs[0], refs[1:]
    lands, refs = refs[:24], refs[24:]
    (gt_low, gt_sib, smalls), refs = refs[:3], refs[3:]
    (in_sem, send_sem, recv_sem, sib_send, sib_recv, own_sem, late_send, late_recv, late_sib_send, late_sib_recv,
     gt_sem, tok_send, gt_recv, small_send, small_recv) = refs
    core, chip, x, y, z = place()
    other = 1 - core
    half = CHIPS // 2
    me = core * CHIPS + chip
    rows = qv.shape[0]
    mine = pl.ds(pl.multiple_of(core * rows, rows), rows)
    theirs = pl.ds(pl.multiple_of(other * rows, rows), rows)
    neighbours = (
        {"dp": core, "seq": chip_at(1 - x, y, z)},
        {"dp": core, "seq": chip_at(x, 1 - y, z)},
        {"dp": core, "seq": chip_at(x, y, jnp.minimum(z + 1, ZS - 1))},
        {"dp": core, "seq": chip_at(x, y, jnp.maximum(z - 1, 0))},
    )
    sibling = {"dp": other, "seq": chip}

    loads = [pltpu.make_async_copy(source, target, in_sem.at[n]) for n, (source, target) in enumerate((
        (k_in, kv), (q_in, qv), (bias_in, biasv), (v_in, vv), (g_in, gv), (att_in, attv), (lse_in, lsev), (x_in, xv), (w_in, wv), (res_in, own_acc), (cos_in, cosv), (sin_in, sinv)))]
    for load in loads:
        load.start()

    def cut(ref, size, index):
        return ref.at[pl.ds(pl.multiple_of(index * size, size), size)]

    rows_gate, rows_down, rows_out = f_gate.shape[0], f_down.shape[0], f_out.shape[0]

    def parts(m, owner, dest):
        if m == 0:
            return [(cut(dwg.at[owner], rows_gate, dest), 0, rows_gate)]
        if m == 1:
            return [(cut(dwu.at[owner], rows_gate, dest), 0, rows_gate)]
        return [(cut(dwd.at[owner], rows_down, dest), 0, rows_down), (cut(dwo.at[owner], rows_out, dest), rows_down, rows_out)]

    def to_sibling(m, dest):
        return [pltpu.make_async_remote_copy(
            src_ref=source, dst_ref=sibs[m].at[dest, pl.ds(start, size)], send_sem=sib_send.at[m + n, dest],
            recv_sem=sib_recv.at[m + n, dest], device_id=sibling, device_id_type=MESH)
            for n, (source, start, size) in enumerate(parts(m, other, dest))]

    def own_load(m, dest, slot):
        return [pltpu.make_async_copy(source, owns[m].at[slot, pl.ds(start, size)], own_sem.at[m + n, slot])
                for n, (source, start, size) in enumerate(parts(m, core, dest))]

    def dest_of(index):
        dx, dy, dz = far_first(index)
        return dx, dy, dz, (z + dz >= 0) & (z + dz < ZS), (x + dx) % 2, (y + dy) % 2, jnp.clip(z + dz, 0, ZS - 1)

    greet_all(core, chip)

    def reduce_piece(order, lands_m, send_at, recv_at, own, acc, offset, target, last, final):
        dx, dy, dz = offset
        tx, ty, tz = target
        fx, fy, up, down = spread(order, dx, dy, dz)
        flags = (fx, fy, up & (z < ZS - 1), down & (z > 0))

        @pl.when(jnp.logical_not(last))
        def _():
            acc[...] += own()

        @pl.when(last)
        def _():
            final[...] = acc[...].astype(F32) + own().astype(F32)

        for link in range(4):
            land = lands_m[link].at[landing_index(order, link, tx, ty, tz)]

            @pl.when(flags[link])
            def _():
                pltpu.make_async_copy(land, land, recv_at(link)).wait()

            @pl.when(flags[link] & jnp.logical_not(last))
            def _():
                acc[...] += land[...]

            @pl.when(flags[link] & last)
            def _():
                final[...] += land[...].astype(F32)

        away = {"x": dx != 0, "y": dy != 0, "z": dz != 0}
        taken = None
        for axis in order[::-1]:
            here = away[axis] if taken is None else away[axis] & jnp.logical_not(taken)
            taken = away[axis] if taken is None else taken | away[axis]
            for link in {"x": (0,), "y": (1,), "z": (2, 3)}[axis]:
                go = here if axis != "z" else (here & (dz > 0 if link == 2 else dz < 0))
                there = {0: 0, 1: 1, 2: 3, 3: 2}[link]

                @pl.when(go)
                def _():
                    pltpu.make_async_remote_copy(
                        src_ref=acc, dst_ref=lands_m[there].at[landing_index(order, there, tx, ty, tz)],
                        send_sem=send_at, recv_sem=recv_at(there), device_id=neighbours[link], device_id_type=MESH).start()

    def early(index):
        dx, dy, dz, valid, tx, ty, tz = dest_of(index)
        last = index == len(FAR_FIRST) - 1
        prefetch(index + 2)

        @pl.when(valid)
        def _():
            dest = chip_at(tx, ty, tz)
            for m in range(3):
                for copy in own_load(m, dest, index % 3):
                    copy.wait()
                for copy in to_sibling(m, dest):
                    copy.wait_recv()
                reduce_piece(BACK_ORDERS[m], lands[4 * m:4 * m + 4], send_sem.at[m, dest], lambda link: recv_sem.at[m, link, dest],
                             lambda: owns[m][index % 3], sibs[m].at[dest], (dx, dy, dz), (tx, ty, tz), last, (f_gate, f_up, down_out)[m])

    step = 256
    per_group = (GROUP // LANES) * (rows // step) * 2
    groups = xv.shape[1] // GROUP
    chunks = groups * per_group
    blocks = xv.shape[1] // LANES
    for load in loads[:7]:
        load.wait()

    def chunk(index):
        group, inner = index // per_group, index % per_group
        pair, block, head = inner // (per_group // 2), inner // 2 % (rows // step), inner % 2
        here = pl.ds(pl.multiple_of(block * step, step), step)
        lanes = pl.ds(pl.multiple_of(group * GROUP + pair * LANES, LANES), LANES)
        out_lanes = pl.ds(pl.multiple_of(pair * LANES, LANES), LANES)

        @pl.when(inner == 0)
        def _():
            dq[...] = jnp.zeros_like(dq)
            dk[...] = jnp.zeros_like(dk)
            dv[...] = jnp.zeros_like(dv)

        qp, gp = qv[here, lanes], gv[here, lanes]
        keep = lane_of(qp.shape) // HEAD == head
        qm, gm = jnp.where(keep, qp, jnp.zeros_like(qp)), jnp.where(keep, gp, jnp.zeros_like(gp))
        kp, vp = kv[:, lanes], vv[:, lanes]
        s = nt(kp, qm) + jnp.concatenate([biasv[...]] * (step // LANES), 1)
        p = jnp.exp(s - lsev[pl.ds(2 * (group * (GROUP // LANES) + pair) + head, 1), here])
        dp = nt(vp, gm)
        shares = gm.astype(F32) * attv[here, lanes].astype(F32)
        delta = lax.dot_general(jnp.ones((8, LANES), F32), shares, (((1,), (1,)), ((), ())),
                                precision=lax.Precision.HIGHEST, preferred_element_type=F32)[0:1, :]
        ds = (p * (dp - delta)).astype(LOW)
        dv[:, out_lanes] += nn(p.astype(LOW), gm)
        dk[:, out_lanes] += nn(ds, qm)
        dq[here, out_lanes] += jnp.where(keep, tn(ds, kp), 0.0)

        @pl.when(index == per_group - 1)
        def _():
            for load in loads[7:]:
                load.wait()
            xt[...] = xv[...].T
            oth_acc[...] = jnp.zeros_like(oth_acc)

        @pl.when(inner == per_group - 1)
        def _():
            finish(group)

    def finish(group):
        def back(u, cos, sin):
            return u * jnp.concatenate([cos, cos], 1) - turn(u) * jnp.concatenate([sin, sin], 1)

        def put(block, value):
            per = dw.shape[2] // LANES
            for i in range(2):
                b = block + i
                dw[b // per, :, pl.ds(pl.multiple_of(b % per * LANES, LANES), LANES)] = value[:, i * LANES:i * LANES + LANES].astype(LOW)

        def weights(block):
            per = dw.shape[2] // LANES
            return jnp.concatenate([wv[b // per, :, pl.ds(pl.multiple_of(b % per * LANES, LANES), LANES)] for b in (block, block + 1)], 1)

        gq = back(dq[...] * 0.125, cosv[mine, :], sinv[mine, :]).astype(LOW)
        dk[...] = back(dk[...], cosv[...], sinv[...])
        put(2 * group, nn(xt[:, mine], gq))
        put(blocks + 2 * group, nn(xt[...], dk[...].astype(LOW)))
        put(2 * blocks + 2 * group, nn(xt[...], dv[...].astype(LOW)))
        wq, wk, wvv = (weights(n * blocks + 2 * group) for n in range(3))
        own_acc[...] += nt(gq, wq) + nt(dk[mine, :].astype(LOW), wk) + nt(dv[mine, :].astype(LOW), wvv)
        oth_acc[...] += nt(dk[theirs, :].astype(LOW), wk) + nt(dv[theirs, :].astype(LOW), wvv)

    def turn_of(index, carry):
        chunk(index)

        @pl.when(index - ahead < mixed)
        def _():
            early(index - ahead)
        return carry

    ahead = 1
    lax.fori_loop(0, ahead, lambda index, c: (chunk(index), c)[1], 0)
    all_here()

    def begin(index, carry):
        dx, dy, dz, valid, tx, ty, tz = dest_of(index)

        @pl.when(valid)
        def _():
            for m in range(3):
                for copy in to_sibling(m, chip_at(tx, ty, tz)):
                    copy.start()
        return carry

    lax.fori_loop(0, len(FAR_FIRST), begin, 0)

    def prefetch(index):
        dx, dy, dz, valid, tx, ty, tz = dest_of(index)

        @pl.when(valid & (index < len(FAR_FIRST)))
        def _():
            for m in range(3):
                for copy in own_load(m, chip_at(tx, ty, tz), index % 3):
                    copy.start()

    prefetch(jnp.int32(0))
    prefetch(jnp.int32(1))

    def small_to(step):
        to = (me + step) % (2 * CHIPS)
        return pltpu.make_async_remote_copy(
            src_ref=dsmall.at[to], dst_ref=smalls.at[me], send_sem=small_send.at[step], recv_sem=small_recv.at[me],
            device_id={"dp": to // CHIPS, "seq": to % CHIPS}, device_id_type=MESH)

    lax.fori_loop(1, 2 * CHIPS, lambda s, c: (small_to(s).start(), c)[1], 0)
    own_small = pltpu.make_async_copy(dsmall.at[me], smalls.at[me], small_recv.at[me])
    own_small.start()

    mixed = min(chunks - ahead, len(FAR_FIRST) - 4)
    lax.fori_loop(ahead, chunks, turn_of, 0)

    gt_low[...] = oth_acc[...].astype(LOW)
    third = f_qkv.shape[1] // len(LATE_ORDERS)

    def late_to_sibling(dest):
        return pltpu.make_async_remote_copy(
            src_ref=cut(dw.at[other], rows_gate, dest), dst_ref=sibs[3].at[dest], send_sem=late_sib_send.at[dest],
            recv_sem=late_sib_recv.at[dest], device_id=sibling, device_id_type=MESH)

    def late_begin(index, carry):
        dx, dy, dz, valid, tx, ty, tz = dest_of(index)

        @pl.when(valid)
        def _():
            late_to_sibling(chip_at(tx, ty, tz)).start()
        return carry

    lax.fori_loop(0, len(FAR_FIRST), late_begin, 0)
    cross = pltpu.make_async_remote_copy(src_ref=gt_low, dst_ref=gt_sib, send_sem=gt_sem.at[0], recv_sem=gt_sem.at[1],
                                         device_id=sibling, device_id_type=MESH)
    cross.start()

    def late(offset):
        dx, dy, dz = offset
        final_step = offset == (0, 0, 0)

        def one():
            tx, ty, tz = (x + dx) % 2, (y + dy) % 2, z + dz
            dest = chip_at(tx, ty, tz)
            late_to_sibling(dest).wait_recv()
            for n, order in enumerate(LATE_ORDERS):
                lanes = slice(n * third, n * third + third)
                acc = sibs[3].at[dest, :, lanes]
                own = dw[core, pl.ds(pl.multiple_of(dest * rows_gate, rows_gate), rows_gate), lanes]
                total = f_qkv.at[:, lanes] if final_step else acc
                total[...] = (acc[...].astype(F32) + own.astype(F32)).astype(total.dtype)
                for link in onward(order, dx, dy, dz):
                    land = lands[12 + 4 * n + link].at[landing_index(order, link, tx, ty, tz)]

                    def add():
                        pltpu.make_async_copy(land, land, late_recv.at[n, link, dest]).wait()
                        total[...] += land[...].astype(total.dtype)
                    when({2: z < ZS - 1, 3: z > 0}.get(link, True), add)
                if not final_step:
                    link = next({"x": 0, "y": 1, "z": 2 if dz > 0 else 3}[axis] for axis in order[::-1] if {"x": dx, "y": dy, "z": dz}[axis])
                    there = {0: 0, 1: 1, 2: 3, 3: 2}[link]
                    pltpu.make_async_remote_copy(
                        src_ref=acc, dst_ref=lands[12 + 4 * n + there].at[landing_index(order, there, tx, ty, tz)],
                        send_sem=late_send.at[n, dest], recv_sem=late_recv.at[n, there, dest],
                        device_id=neighbours[link], device_id_type=MESH).start()
        when(True if dz == 0 else (z < ZS - dz if dz > 0 else z >= -dz), one)

    early_steps, left = 4, mixed
    for step_index, offset in enumerate(FAR_FIRST):
        if step_index == early_steps:
            cross.wait()
            gt_low[...] = (own_acc[...] + gt_sib[...].astype(F32)).astype(LOW)
            for j in range(half):
                from_slot(core, chip, j, gt_low, gt_out, tok_send, gt_recv)
        late(offset)
        if step_index % 2 == 1 and left < len(FAR_FIRST):
            early(jnp.int32(left))
            left += 1
    f_down[...] = down_out[0:rows_down, :]
    f_out[...] = down_out[rows_down:rows_down + rows_out, :]

    def small_end(s, carry):
        small_to(s).wait_send()
        source = (me + s) % (2 * CHIPS)
        pltpu.make_async_copy(smalls.at[source], smalls.at[source], small_recv.at[source]).wait()
        return carry

    lax.fori_loop(1, 2 * CHIPS, small_end, 0)
    own_small.wait()
    f_small[...] = jnp.sum(smalls[...], axis=0)

    sent_blocks(core, chip, gt_out.at[0], tok_send)
    lax.fori_loop(0, half, lambda i, c: (pltpu.make_async_copy(gt_out.at[i], gt_out.at[i], gt_recv.at[i]).wait(), c)[1], 0)

    def sent(dest, carry):
        for m in range(3):
            for copy in to_sibling(m, dest):
                copy.wait_send()
        late_to_sibling(dest).wait_send()

        @pl.when(dest != chip)
        def _():
            for m in range(3):
                pltpu.make_async_copy(sibs[m].at[dest], sibs[m].at[dest], send_sem.at[m, dest]).wait()
            for n in range(len(LATE_ORDERS)):
                part = sibs[3].at[dest, :, pl.ds(n * third, third)]
                pltpu.make_async_copy(part, part, late_send.at[n, dest]).wait()
        return carry

    lax.fori_loop(0, CHIPS, sent, 0)


def back_scatter(dwg, dwu, dwd, dwo, dsmall, x, w, q, k, v, g_att, g_res1, cos, sin, bias_col, att, lse):
    tokens, width = x.shape
    rows = tokens // 2
    span = rows // 8
    anywhere, vmem = pl.BlockSpec(memory_space=pl.ANY), pl.BlockSpec(memory_space=pltpu.VMEM)
    n_gate, n_down, n_out = width // CHIPS, dwd.shape[1] // CHIPS, dwo.shape[1] // CHIPS
    c_gate, c_down = dwg.shape[2], dwd.shape[2]
    c_qkv = 3 * width // 2
    third = c_qkv // len(LATE_ORDERS)
    sds, mem = jax.ShapeDtypeStruct, pltpu.VMEM
    out8 = sds((8, span, width), LOW)
    finals = [sds((n_gate, c_gate), F32), sds((n_gate, c_gate), F32), sds((n_down, c_down), F32), sds((n_out, c_down), F32),
              sds((n_gate, c_qkv), F32), sds(dsmall.shape[1:], F32)]
    pieces = [(n_gate, c_gate), (n_gate, c_gate), (n_down + n_out, c_down)]
    scratch = [mem((tokens, width), LOW), mem(w.shape, LOW), mem((rows, width), LOW), mem((tokens, width), LOW), mem((tokens, width), LOW),
               mem((rows, width), LOW), mem((rows, width), F32), mem(cos.shape, F32), mem(sin.shape, F32), mem(bias_col.shape, F32),
               mem((width, tokens), LOW), mem((rows, width), F32), mem((rows, GROUP), F32), mem((tokens, GROUP), F32), mem((tokens, GROUP), F32),
               mem((2, width, c_qkv), LOW), mem((rows, width), LOW), mem(lse.shape, F32)]
    scratch += [mem((3,) + piece, LOW) for piece in pieces]
    scratch += [mem((CHIPS,) + piece, LOW) for piece in pieces] + [mem((CHIPS, n_gate, c_qkv), LOW)]
    scratch += [mem(pieces[2], F32)]
    for order, piece in zip(BACK_ORDERS, pieces):
        scratch += [mem((n,) + piece, LOW) for n in landing_slots(order)]
    for order in LATE_ORDERS:
        scratch += [mem((n, n_gate, third), LOW) for n in landing_slots(order)]
    scratch += [mem((rows, width), LOW), mem((rows, width), LOW), mem(dsmall.shape, F32)]
    dma = pltpu.SemaphoreType.DMA
    scratch += [dma((12,)), dma((3, CHIPS)), dma((3, 4, CHIPS)), dma((4, CHIPS)), dma((4, CHIPS)), dma((4, 3)), dma((3, CHIPS)), dma((3, 4, CHIPS)),
                dma((CHIPS,)), dma((CHIPS,)), dma((2,)), dma((8,)), dma((8,)), dma((2 * CHIPS,)), dma((2 * CHIPS,))]
    return pl.pallas_call(
        back_scatter_kernel,
        out_shape=[out8] + finals,
        in_specs=[anywhere] * 17,
        out_specs=[anywhere] + [vmem] * len(finals),
        scratch_shapes=scratch,
        compiler_params=pltpu.CompilerParams(collective_id=1, has_side_effects=True, vmem_limit_bytes=67043328),
        name="back_scatter",
    )(dwg, dwu, dwd, dwo, dsmall, x, w, q, k, v, g_att, g_res1, cos, sin, bias_col, att, lse)


def rotary_turns(tokens, near):
    pair_index = (np.arange(LANES) % (HEAD // 2)).astype(np.float32)
    inverse = np.power(np.float32(1000.0), np.float32(-2.0) * pair_index / np.float32(HEAD))

    def table(positions):
        angles = positions.astype(np.float32)[:, None] * inverse[None, :]
        return jnp.asarray(np.stack([np.cos(angles), np.sin(angles)]), F32)

    return table(np.arange(0, tokens, near)), table(np.arange(near))


def local_by_slot(tokens, lengths, w_qkv, w_out, w_gate, w_up, w_down, ln_params, cotangent):
    slots, span, width = tokens.shape
    share = ln_params.shape[1]
    turns_far, turns_near = rotary_turns(span * CHIPS, span)
    x, cot, ln, w_in, wg, wu, wd, q, k, v, att, cos, sin, bias_col, lse = front(
        tokens, cotangent, w_qkv, w_out, w_gate, w_up, w_down, ln_params, lengths, turns_far, turns_near)
    y, dwg, dwu, dwd, dwo, g_att, g_res1, dsmall = middle(x, att, w_in, wg, wu, wd, cot, ln, bias_col)
    results = back_scatter(dwg, dwu, dwd, dwo, dsmall, x, w_in, q, k, v, g_att, g_res1, cos, sin, bias_col, att, lse)
    output, grad_tokens, d_gate, d_up, d_down, d_out, d_qkv, d_small = finish([y, *results], share)
    return (output, grad_tokens, d_qkv, d_out, d_gate, d_up, d_down, d_small)


def solution(mesh):
    placed = (
        P("dp", "seq", None),
        P("dp"),
        P("seq", "dp"),
        P("seq", "dp"),
        P("seq", "dp"),
        P("seq", "dp"),
        P("seq", "dp"),
        P(None, ("dp", "seq")),
        P("dp", "seq", None),
    )

    def run(tokens, *rest):
        by_slot = mesh.shape["dp"] == 2 and mesh.shape["seq"] == CHIPS and tokens.shape[0] == CHIPS
        body = local_by_slot if by_slot else local
        return jax.shard_map(
            body,
            mesh=mesh,
            in_specs=placed,
            out_specs=(
                P("dp", "seq", None),
                P("dp", "seq", None),
                P("seq", "dp"),
                P("seq", "dp"),
                P("seq", "dp"),
                P("seq", "dp"),
                P("seq", "dp"),
                P(None, ("dp", "seq")),
            ),
            check_vma=False,
        )(tokens, *rest)

    return run
```

```python
import functools

import jax
import jax.numpy as jnp
import numpy as np
from jax import lax
from jax.experimental import pallas as pl
from jax.experimental.pallas import tpu as pltpu
from jax.sharding import PartitionSpec as P

HEADS = 12
HEAD_DIM = 64


norm_epsilon = 1e-12
score_scale = 0.125
masked_score = -1e30


def shifted(shard, axis, by):
    count = lax.axis_size(axis)
    return lax.ppermute(shard, axis, [(i, (i + by) % count) for i in range(count)])


def rotary_tables(positions):
    pair_index = jnp.arange(HEAD_DIM // 2, dtype=jnp.float32)
    inverse = jnp.power(jnp.float32(1000.0), -2.0 * pair_index / HEAD_DIM)
    angles = positions.astype(jnp.float32)[:, None] * inverse[None, :]
    cos_tab = jnp.concatenate([jnp.cos(angles), jnp.cos(angles)], axis=-1)
    sin_tab = jnp.concatenate([jnp.sin(angles), jnp.sin(angles)], axis=-1)
    return (cos_tab, sin_tab)


def rotate(values, cos_tab, sin_tab):
    half_dim = values.shape[-1] // 2
    turned = jnp.concatenate([-values[..., half_dim:], values[..., :half_dim]], axis=-1)
    return values * cos_tab + turned * sin_tab


def norm_parts(values, gain_vec, bias_vec):
    center = values - jnp.mean(values, axis=-1, keepdims=True)
    inv_std = lax.rsqrt(jnp.mean(center * center, axis=-1, keepdims=True) + norm_epsilon)
    normed = center * inv_std
    return (normed * gain_vec + bias_vec, normed, inv_std)


def norm_back(grad_in, normed, inv_std, gain_vec):
    scaled = grad_in * gain_vec
    return inv_std * (
        scaled
        - jnp.mean(scaled, axis=-1, keepdims=True)
        - normed * jnp.mean(scaled * normed, axis=-1, keepdims=True)
    )


def heads_view(flat_rows):
    return flat_rows.reshape(flat_rows.shape[0], flat_rows.shape[1], HEADS, HEAD_DIM)


def attend_block(run_state, queries, key_blk, value_blk, key_start, lengths):
    run_max, run_sum, run_acc = run_state
    scores = (
        jnp.einsum(
            "sqhd,skhd->shqk",
            heads_view(queries),
            heads_view(key_blk),
            preferred_element_type=jnp.float32,
        )
        * score_scale
    )
    key_pos = key_start + jnp.arange(key_blk.shape[1], dtype=jnp.int32)
    key_mask = (key_pos[None, :] < lengths[:, None])[:, None, None, :]
    scores = jnp.where(key_mask, scores, masked_score)
    new_max = jnp.maximum(run_max, jnp.max(scores, axis=-1))
    exp_scores = jnp.where(key_mask, jnp.exp(scores - new_max[..., None]), 0.0)
    factor = jnp.exp(run_max - new_max)
    run_sum = run_sum * factor + jnp.sum(exp_scores, axis=-1)
    run_acc = run_acc * factor[..., None] + jnp.einsum(
        "shqk,skhd->shqd",
        exp_scores.astype(jnp.bfloat16),
        heads_view(value_blk),
        preferred_element_type=jnp.float32,
    )
    return (new_max, run_sum, run_acc)


def block_grads(queries, grad_att, log_total, delta_rows, key_blk, value_blk, key_ok):
    query_h = heads_view(queries)
    grad_h = heads_view(grad_att)
    key_h = heads_view(key_blk)
    scores = (
        jnp.einsum("sqhd,skhd->shqk", query_h, key_h, preferred_element_type=jnp.float32)
        * score_scale
    )
    key_mask = key_ok[:, None, None, :]
    soft_probs = jnp.where(key_mask, jnp.exp(scores - log_total[..., None]), 0.0)
    grad_probs = jnp.einsum(
        "sqhd,skhd->shqk", grad_h, heads_view(value_blk), preferred_element_type=jnp.float32
    )
    grad_scores = (soft_probs * (grad_probs - delta_rows[..., None])).astype(jnp.bfloat16)
    part_q = (
        jnp.einsum("shqk,skhd->sqhd", grad_scores, key_h, preferred_element_type=jnp.float32)
        * score_scale
    )
    part_k = (
        jnp.einsum("shqk,sqhd->skhd", grad_scores, query_h, preferred_element_type=jnp.float32)
        * score_scale
    )
    part_v = jnp.einsum(
        "shqk,sqhd->skhd",
        soft_probs.astype(jnp.bfloat16),
        grad_h,
        preferred_element_type=jnp.float32,
    )
    shape_out = queries.shape
    return (part_q.reshape(shape_out), part_k.reshape(key_blk.shape), part_v.reshape(key_blk.shape))


def local(tokens, lengths, w_qkv, w_out, w_gate, w_up, w_down, ln_params, cotangent):
    slot_count, span_len, width = tokens.shape
    row_count = slot_count * span_len
    cycle_size = lax.axis_size("seq")
    my_index = lax.axis_index("seq")
    row_qkv, row_out, row_gate, row_up, row_down, row_norm = (
        lax.all_gather(w_qkv, "seq", axis=0, tiled=True),
        lax.all_gather(w_out, "seq", axis=0, tiled=True),
        lax.all_gather(w_gate, "seq", axis=0, tiled=True),
        lax.all_gather(w_up, "seq", axis=0, tiled=True),
        lax.all_gather(w_down, "seq", axis=0, tiled=True),
        lax.all_gather(ln_params, "seq", axis=1, tiled=True),
    )
    wide_qkv, wide_out, wide_gate, wide_up, wide_down, wide_norm = (
        lax.all_gather(row_qkv, "dp", axis=1, tiled=True),
        lax.all_gather(row_out, "dp", axis=1, tiled=True),
        lax.all_gather(row_gate, "dp", axis=1, tiled=True),
        lax.all_gather(row_up, "dp", axis=1, tiled=True),
        lax.all_gather(row_down, "dp", axis=1, tiled=True),
        lax.all_gather(row_norm, "dp", axis=1, tiled=True),
    )
    norm_full = wide_norm.astype(jnp.float32)
    flat_tokens = tokens.reshape(row_count, width)
    token_f32 = flat_tokens.astype(jnp.float32)
    positions = my_index * span_len + jnp.arange(span_len, dtype=jnp.int32)
    row_valid = (positions[None, :] < lengths[:, None]).astype(jnp.float32).reshape(row_count, 1)
    cos_tab, sin_tab = rotary_tables(positions)
    cos_four = cos_tab[None, :, None, :]
    sin_four = sin_tab[None, :, None, :]
    qkv_pre = jnp.dot(flat_tokens, wide_qkv, preferred_element_type=jnp.float32)
    split_qkv = qkv_pre.reshape(slot_count, span_len, 3, HEADS, HEAD_DIM)
    queries = (
        rotate(split_qkv[:, :, 0], cos_four, sin_four)
        .astype(jnp.bfloat16)
        .reshape(slot_count, span_len, width)
    )
    keys_rot = (
        rotate(split_qkv[:, :, 1], cos_four, sin_four)
        .astype(jnp.bfloat16)
        .reshape(slot_count, span_len, width)
    )
    values = split_qkv[:, :, 2].astype(jnp.bfloat16).reshape(slot_count, span_len, width)
    start_state = (
        jnp.full((slot_count, HEADS, span_len), masked_score, jnp.float32),
        jnp.zeros((slot_count, HEADS, span_len), jnp.float32),
        jnp.zeros((slot_count, HEADS, span_len, HEAD_DIM), jnp.float32),
    )
    key_piece = lax.all_gather(keys_rot, "seq", axis=1, tiled=True)
    value_piece = lax.all_gather(values, "seq", axis=1, tiled=True)
    block_count = key_piece.shape[1] // span_len

    def one_block(block_id, inner_state):
        offset = block_id * span_len
        key_blk = lax.dynamic_slice_in_dim(key_piece, offset, span_len, axis=1)
        value_blk = lax.dynamic_slice_in_dim(value_piece, offset, span_len, axis=1)
        return attend_block(inner_state, queries, key_blk, value_blk, offset, lengths)

    run_max, run_sum, run_acc = lax.fori_loop(0, block_count, one_block, start_state)
    attended = run_acc / run_sum[..., None]
    log_total = run_max + jnp.log(run_sum)
    attn_low = attended.transpose(0, 2, 1, 3).reshape(row_count, width).astype(jnp.bfloat16)
    branch = jnp.dot(attn_low, wide_out, preferred_element_type=jnp.float32)
    hidden, normed_one, inv_one = norm_parts(token_f32 + branch, norm_full[0], norm_full[1])
    hidden_low = hidden.astype(jnp.bfloat16)
    gate_pre = jnp.dot(hidden_low, wide_gate, preferred_element_type=jnp.float32)
    up_proj = jnp.dot(hidden_low, wide_up, preferred_element_type=jnp.float32)
    activated = jax.nn.silu(gate_pre)
    inner_low = (activated * up_proj).astype(jnp.bfloat16)
    branch_two = jnp.dot(inner_low, wide_down, preferred_element_type=jnp.float32)
    result, normed_two, inv_two = norm_parts(hidden + branch_two, norm_full[2], norm_full[3])
    output = (result * row_valid).astype(jnp.bfloat16).reshape(slot_count, span_len, width)
    back_qkv, back_out, back_gate, back_up, back_down, back_norm = (
        lax.all_gather(w_qkv, "seq", axis=0, tiled=True),
        lax.all_gather(w_out, "seq", axis=0, tiled=True),
        lax.all_gather(w_gate, "seq", axis=0, tiled=True),
        lax.all_gather(w_up, "seq", axis=0, tiled=True),
        lax.all_gather(w_down, "seq", axis=0, tiled=True),
        lax.all_gather(ln_params, "seq", axis=1, tiled=True),
    )
    wide_qkv, wide_out, wide_gate, wide_up, wide_down, wide_norm = (
        lax.all_gather(back_qkv, "dp", axis=1, tiled=True),
        lax.all_gather(back_out, "dp", axis=1, tiled=True),
        lax.all_gather(back_gate, "dp", axis=1, tiled=True),
        lax.all_gather(back_up, "dp", axis=1, tiled=True),
        lax.all_gather(back_down, "dp", axis=1, tiled=True),
        lax.all_gather(back_norm, "dp", axis=1, tiled=True),
    )
    norm_full = wide_norm.astype(jnp.float32)
    grad_out = cotangent.reshape(row_count, width).astype(jnp.float32) * row_valid
    gain_two_grad = jnp.sum(grad_out * normed_two, axis=0)
    bias_two_grad = jnp.sum(grad_out, axis=0)
    grad_res2 = norm_back(grad_out, normed_two, inv_two, norm_full[2])
    grad_branch2 = grad_res2.astype(jnp.bfloat16)
    grad_wdown = jnp.einsum(
        "rf,rd->fd", inner_low, grad_branch2, preferred_element_type=jnp.float32
    )
    grad_inner = jnp.einsum(
        "rd,fd->rf", grad_branch2, wide_down, preferred_element_type=jnp.float32
    )
    sigma = jax.nn.sigmoid(gate_pre)
    grad_gate = (grad_inner * up_proj * sigma * (1.0 + gate_pre * (1.0 - sigma))).astype(
        jnp.bfloat16
    )
    grad_up = (grad_inner * activated).astype(jnp.bfloat16)
    grad_wgate = jnp.einsum("rd,rf->df", hidden_low, grad_gate, preferred_element_type=jnp.float32)
    grad_wup = jnp.einsum("rd,rf->df", hidden_low, grad_up, preferred_element_type=jnp.float32)
    grad_hidden = (
        grad_res2
        + jnp.einsum("rf,df->rd", grad_gate, wide_gate, preferred_element_type=jnp.float32)
        + jnp.einsum("rf,df->rd", grad_up, wide_up, preferred_element_type=jnp.float32)
    )
    gain_one_grad = jnp.sum(grad_hidden * normed_one, axis=0)
    bias_one_grad = jnp.sum(grad_hidden, axis=0)
    grad_res1 = norm_back(grad_hidden, normed_one, inv_one, norm_full[0])
    grad_branch1 = grad_res1.astype(jnp.bfloat16)
    grad_wout = jnp.einsum("ri,rd->id", attn_low, grad_branch1, preferred_element_type=jnp.float32)
    grad_att = (
        jnp.einsum("rd,id->ri", grad_branch1, wide_out, preferred_element_type=jnp.float32)
        .astype(jnp.bfloat16)
        .reshape(slot_count, span_len, width)
    )
    zero_rows = jnp.zeros((slot_count, span_len, width), jnp.float32)
    delta_rows = jnp.einsum("sqhd,shqd->shq", heads_view(grad_att).astype(jnp.float32), attended)

    def key_turn(turn_id, run_state):
        key_cur, value_cur, grad_keys, grad_values, grad_query = run_state
        key_start = (my_index - turn_id) % cycle_size * span_len
        key_ok = (key_start + jnp.arange(span_len, dtype=jnp.int32))[None, :] < lengths[:, None]
        part_q, part_k, part_v = block_grads(
            queries, grad_att, log_total, delta_rows, key_cur, value_cur, key_ok
        )
        key_cur, value_cur = shifted((key_cur, value_cur), "seq", 1)
        grad_keys, grad_values = (
            shifted((grad_keys + part_k).astype(jnp.bfloat16), "seq", 1).astype(jnp.float32),
            shifted((grad_values + part_v).astype(jnp.bfloat16), "seq", 1).astype(jnp.float32),
        )
        return (key_cur, value_cur, grad_keys, grad_values, grad_query + part_q)

    key_cur, value_cur, grad_keys, grad_values, grad_query = lax.fori_loop(
        0, cycle_size - 1, key_turn, (keys_rot, values, zero_rows, zero_rows, zero_rows)
    )
    key_start = (my_index - (cycle_size - 1)) % cycle_size * span_len
    key_ok = (key_start + jnp.arange(span_len, dtype=jnp.int32))[None, :] < lengths[:, None]
    part_q, part_k, part_v = block_grads(
        queries, grad_att, log_total, delta_rows, key_cur, value_cur, key_ok
    )
    grad_query = grad_query + part_q
    grad_keys, grad_values = (
        shifted((grad_keys + part_k).astype(jnp.bfloat16), "seq", 1).astype(jnp.float32),
        shifted((grad_values + part_v).astype(jnp.bfloat16), "seq", 1).astype(jnp.float32),
    )
    query_back = rotate(heads_view(grad_query), cos_four, -sin_four)
    key_back = rotate(heads_view(grad_keys), cos_four, -sin_four)
    grad_qkv = jnp.stack([query_back, key_back, heads_view(grad_values)], axis=2)
    grad_qkv = grad_qkv.reshape(row_count, 3 * width).astype(jnp.bfloat16)
    grad_wqkv = jnp.einsum("rd,re->de", flat_tokens, grad_qkv, preferred_element_type=jnp.float32)
    grad_tokens = grad_res1 + jnp.einsum(
        "re,de->rd", grad_qkv, wide_qkv, preferred_element_type=jnp.float32
    )
    grad_tokens = grad_tokens.astype(jnp.bfloat16).reshape(slot_count, span_len, width)
    grad_norm = jnp.stack([gain_one_grad, bias_one_grad, gain_two_grad, bias_two_grad], axis=0)
    col_qkv, col_out, col_gate, col_up, col_down, col_norm = (
        lax.psum_scatter(
            grad_wqkv.astype(jnp.bfloat16), "dp", scatter_dimension=1, tiled=True
        ).astype(jnp.float32),
        lax.psum_scatter(
            grad_wout.astype(jnp.bfloat16), "dp", scatter_dimension=1, tiled=True
        ).astype(jnp.float32),
        lax.psum_scatter(
            grad_wgate.astype(jnp.bfloat16), "dp", scatter_dimension=1, tiled=True
        ).astype(jnp.float32),
        lax.psum_scatter(
            grad_wup.astype(jnp.bfloat16), "dp", scatter_dimension=1, tiled=True
        ).astype(jnp.float32),
        lax.psum_scatter(
            grad_wdown.astype(jnp.bfloat16), "dp", scatter_dimension=1, tiled=True
        ).astype(jnp.float32),
        lax.psum_scatter(
            grad_norm.astype(jnp.bfloat16), "dp", scatter_dimension=1, tiled=True
        ).astype(jnp.float32),
    )
    own_qkv, own_out, own_gate, own_up, own_down, own_norm = (
        lax.psum_scatter(
            col_qkv.astype(jnp.bfloat16), "seq", scatter_dimension=0, tiled=True
        ).astype(jnp.float32),
        lax.psum_scatter(
            col_out.astype(jnp.bfloat16), "seq", scatter_dimension=0, tiled=True
        ).astype(jnp.float32),
        lax.psum_scatter(
            col_gate.astype(jnp.bfloat16), "seq", scatter_dimension=0, tiled=True
        ).astype(jnp.float32),
        lax.psum_scatter(
            col_up.astype(jnp.bfloat16), "seq", scatter_dimension=0, tiled=True
        ).astype(jnp.float32),
        lax.psum_scatter(
            col_down.astype(jnp.bfloat16), "seq", scatter_dimension=0, tiled=True
        ).astype(jnp.float32),
        lax.psum_scatter(
            col_norm.astype(jnp.bfloat16), "seq", scatter_dimension=1, tiled=True
        ).astype(jnp.float32),
    )
    return (output, grad_tokens, own_qkv, own_out, own_gate, own_up, own_down, own_norm)


MESH = pl.DeviceIdType.MESH
CHIPS, ZS = 16, 4
OFFSETS = sorted(((dx, dy, dz) for dx in (0, 1) for dy in (0, 1) for dz in range(-3, 4)),
                 key=lambda o: (2 * (o[0] + o[1]) + abs(o[2]), abs(o[2]), o))


def pick(index, values):
    out = jnp.int32(0)
    for position, value in enumerate(values):
        if value:
            out = out + jnp.where(index == position, jnp.int32(value), 0)
    return out


def spread(order, dx, dy, dz):
    zero = {"x": dx == 0, "y": dy == 0, "z": dz == 0}
    flags = {}
    for position, axis in enumerate(order):
        flag = zero[axis] if axis != "z" else None
        for later in order[position + 1:]:
            flag = zero[later] if flag is None else flag & zero[later]
        flags[axis] = flag
    up, down = dz <= 0, dz >= 0
    if flags["z"] is not None:
        up, down = up & flags["z"], down & flags["z"]
    return flags["x"], flags["y"], up, down


def place():
    core, chip = lax.axis_index("dp"), lax.axis_index("seq")
    return core, chip, chip % 2, (chip // 2) % 2, chip // 4


def chip_at(x, y, z):
    return (z * 2 + y) * 2 + x


def meet_all(core, chip):
    greet_all(core, chip)
    all_here()


def onward(order, dx, dy, dz):
    zero = {"x": dx == 0, "y": dy == 0, "z": dz == 0}
    links = []
    for position, axis in enumerate(order):
        if all(zero[later] for later in order[position + 1:]):
            if axis == "z":
                links += [2] * (dz <= 0) + [3] * (dz >= 0)
            elif zero[axis]:
                links.append("xy".index(axis))
    return links


def when(condition, action):
    if condition is True:
        action()
    else:
        pl.when(condition)(action)


def to_slot(core, chip, j, source, target, sends, recvs):
    half = CHIPS // 2
    slot = (chip + 1 + j) % half
    to = core * half + slot
    src = source.at[slot]
    self_copy = (chip // half == core) & (to == chip)

    @pl.when(self_copy)
    def _():
        pltpu.make_async_copy(src, target, recvs.at[chip % half]).start()

    @pl.when(jnp.logical_not(self_copy))
    def _():
        pltpu.make_async_remote_copy(
            src_ref=src, dst_ref=target, send_sem=sends.at[slot], recv_sem=recvs.at[chip % half],
            device_id={"dp": chip // half, "seq": to}, device_id_type=MESH).start()


def from_slot(core, chip, j, source, target, sends, recvs):
    half = CHIPS // 2
    i = (chip + 1 + j) % half
    to_core, to_chip = chip // half, core * half + i
    span = target.shape[1]
    src, dst = source.at[pl.ds(pl.multiple_of(i * span, span), span)], target.at[chip % half]
    self_copy = (to_core == core) & (to_chip == chip)

    @pl.when(self_copy)
    def _():
        pltpu.make_async_copy(src, dst, recvs.at[chip % half]).start()

    @pl.when(jnp.logical_not(self_copy))
    def _():
        pltpu.make_async_remote_copy(
            src_ref=src, dst_ref=dst, send_sem=sends.at[i], recv_sem=recvs.at[chip % half],
            device_id={"dp": to_core, "seq": to_chip}, device_id_type=MESH).start()


def sent_blocks(core, chip, part, sends):
    half = CHIPS // 2

    def one(i, carry):
        @pl.when(jnp.logical_not((chip // half == core) & (core * half + i == chip)))
        def _():
            pltpu.make_async_copy(part, part, sends.at[i]).wait()
        return carry

    lax.fori_loop(0, half, one, 0)


def greet_all(core, chip):
    barrier = pltpu.get_barrier_semaphore()
    me = core * CHIPS + chip

    def greet(step, carry):
        other = (me + step) % (2 * CHIPS)
        pl.semaphore_signal(barrier, inc=1, device_id={"dp": other // CHIPS, "seq": other % CHIPS}, device_id_type=MESH)
        return carry

    lax.fori_loop(1, 2 * CHIPS, greet, 0)


def all_here():
    pl.semaphore_wait(pltpu.get_barrier_semaphore(), 2 * CHIPS - 1)


LOW, F32 = jnp.bfloat16, jnp.float32
EPS = 1e-12
HEAD = 64
LANES = 128
GROUP = 256
FULL = pl.BlockSpec(memory_space=pltpu.VMEM)


def nn(a, b):
    return jnp.dot(a, b, preferred_element_type=F32)


def nt(a, b):
    return lax.dot_general(a, b, (((1,), (1,)), ((), ())), preferred_element_type=F32)


def tn(a, b):
    return lax.dot_general(a, b, (((0,), (0,)), ((), ())), preferred_element_type=F32)


def lane_of(shape):
    return lax.broadcasted_iota(jnp.int32, shape, 1)


def turn(u):
    parts = []
    for start in range(0, u.shape[1], LANES):
        part = u[:, start:start + LANES]
        first = lane_of(part.shape) % HEAD < HEAD // 2
        parts.append(jnp.where(first, pltpu.roll(part, LANES - HEAD // 2, 1), pltpu.roll(part, HEAD // 2, 1)))
    return jnp.concatenate(parts, 1)


def ln_parts(u):
    center = u - jnp.mean(u, axis=1, keepdims=True)
    inv = lax.rsqrt(jnp.mean(center * center, axis=1, keepdims=True) + EPS)
    return center * inv, inv


def ln_back(g, n, inv):
    return inv * (g - jnp.mean(g, axis=1, keepdims=True) - n * jnp.mean(g * n, axis=1, keepdims=True))


def middle_kernel(tiles, x_ref, att_ref, wo_ref, wg_ref, wu_ref, wd_ref, cot_ref, ln_ref, bias_ref,
                  y_out, dwg_ref, dwu_ref, dwd_ref, dwo_ref, gatt_ref, gres_ref, small_ref,
                  n1_ref, inv1_ref, hid_ref, hidt_ref, gate_ref, up_ref, acc_ref, gb_ref, y_ref, dln_ref, y_send, y_recv):
    index = pl.program_id(0)
    width = x_ref.shape[1]
    half = width // 2
    rows = att_ref.shape[0]
    core, chip = lax.axis_index("dp"), lax.axis_index("seq")
    mine = pl.ds(pl.multiple_of(core * rows, rows), rows)
    eighth = CHIPS // 2

    def wide(ref):
        return jnp.concatenate([ref[0], ref[1]], 1)

    @pl.when(index == 0)
    def _():
        greet_all(core, chip)
        n1, inv1 = ln_parts(x_ref[mine, :].astype(F32) + nn(att_ref[...], wide(wo_ref)))
        hidden = n1 * ln_ref[0:1, :] + ln_ref[1:2, :]
        n1_ref[...] = n1
        inv1_ref[...] = jnp.broadcast_to(inv1, inv1_ref.shape)
        acc_ref[...] = hidden
        low = hidden.astype(LOW)
        hid_ref[...] = low
        hidt_ref[...] = low.T

    tile = wg_ref.shape[2]
    f = jnp.where(index < tiles, index, index - tiles)
    cols = pl.ds(pl.multiple_of(f * tile, tile), tile)

    @pl.when(index < tiles)
    def _():
        gate, up = nn(hid_ref[...], wg_ref[0]), nn(hid_ref[...], wu_ref[0])
        gate_ref[:, cols] = gate
        up_ref[:, cols] = up
        acc_ref[...] += nn((gate * jax.nn.sigmoid(gate) * up).astype(LOW), wide(wd_ref))

    @pl.when(index == tiles - 1)
    def _():
        n2, inv2 = ln_parts(acc_ref[...])
        all_here()
        valid = jnp.where(bias_ref[mine, 0:1] == 0.0, 1.0, 0.0)
        y_ref[...] = ((n2 * ln_ref[2:3, :] + ln_ref[3:4, :]) * valid).astype(LOW)
        for j in range(eighth):
            from_slot(core, chip, j, y_ref, y_out, y_send, y_recv)
        g_y = cot_ref[...].astype(F32) * valid
        dln_ref[2:3, :] = jnp.sum(g_y * n2, axis=0, keepdims=True)
        dln_ref[3:4, :] = jnp.sum(g_y, axis=0, keepdims=True)
        g_res2 = ln_back(g_y * ln_ref[2:3, :], n2, inv2)
        acc_ref[...] = g_res2
        gb_ref[...] = g_res2.astype(LOW)

    @pl.when(index >= tiles)
    def _():
        gate, up = gate_ref[:, cols], up_ref[:, cols]
        sig = jax.nn.sigmoid(gate)
        act = gate * sig
        gb = gb_ref[...]
        dwd = tn((act * up).astype(LOW), gb)
        dwd_ref[0] = dwd[:, :half].astype(LOW)
        dwd_ref[1] = dwd[:, half:].astype(LOW)
        g_inner = nt(gb, wide(wd_ref))
        g_gate = (g_inner * up * sig * (1.0 + gate * (1.0 - sig))).astype(LOW)
        g_up = (g_inner * act).astype(LOW)
        dwg_ref[0] = nn(hidt_ref[...], g_gate).astype(LOW)
        dwu_ref[0] = nn(hidt_ref[...], g_up).astype(LOW)
        acc_ref[...] += nt(g_gate, wg_ref[0]) + nt(g_up, wu_ref[0])

    @pl.when(index == 2 * tiles - 1)
    def _():
        g_hidden, n1 = acc_ref[...], n1_ref[...]
        dln_ref[0:1, :] = jnp.sum(g_hidden * n1, axis=0, keepdims=True)
        dln_ref[1:2, :] = jnp.sum(g_hidden, axis=0, keepdims=True)
        g_res1 = ln_back(g_hidden * ln_ref[0:1, :], n1, inv1_ref[:, 0:1])
        gres_ref[...] = g_res1
        gb1 = g_res1.astype(LOW)
        dwo = tn(att_ref[...], gb1)
        dwo_ref[0] = dwo[:, :half].astype(LOW)
        dwo_ref[1] = dwo[:, half:].astype(LOW)
        gatt_ref[...] = nt(gb1, wide(wo_ref)).astype(LOW)
        small_ref[...] = jnp.zeros_like(small_ref)
        share = width // (2 * CHIPS)
        for device in range(2 * CHIPS):
            small_ref[device, 0:4, 0:share] = dln_ref[0:4, device * share:device * share + share]
        sent_blocks(core, chip, y_out.at[0], y_send)
        lax.fori_loop(0, eighth, lambda i, carry: (pltpu.make_async_copy(y_out.at[i], y_out.at[i], y_recv.at[i]).wait(), carry)[1], 0)


def middle(x, att, wo, wg, wu, wd, cot, ln, bias_col):
    rows, width = att.shape
    hidden = wd.shape[1]
    tile = 512
    tiles = hidden // tile
    anywhere = pl.BlockSpec(memory_space=pl.ANY)
    per = wg.shape[2] // tile
    at = lambda i: jnp.where(i < tiles, i, i - tiles)
    late = lambda i: jnp.maximum(i - tiles, 0)
    cols = lambda pick: pl.BlockSpec((1, width, tile), lambda i: (pick(i) // per, 0, pick(i) % per))
    rowb = lambda pick: pl.BlockSpec((2, tile, wd.shape[2]), lambda i: (0, pick(i), 0))
    sds = jax.ShapeDtypeStruct
    return pl.pallas_call(
        functools.partial(middle_kernel, tiles), grid=(2 * tiles,),
        out_shape=[sds((8, rows // 8, width), LOW), sds(wg.shape, LOW), sds(wu.shape, LOW), sds(wd.shape, LOW), sds((2, width, width // 2), LOW),
                   sds((rows, width), LOW), sds((rows, width), F32), sds((2 * CHIPS, 8, LANES), F32)],
        in_specs=[FULL, FULL, pl.BlockSpec((2, width, width // 2), lambda i: (0, 0, 3)), cols(at), cols(at), rowb(at), FULL, FULL, FULL],
        out_specs=[anywhere, cols(late), cols(late), rowb(late), FULL, FULL, FULL, FULL],
        scratch_shapes=[pltpu.VMEM((rows, width), F32), pltpu.VMEM((rows, LANES), F32), pltpu.VMEM((rows, width), LOW),
                        pltpu.VMEM((width, rows), LOW), pltpu.VMEM((rows, hidden), F32), pltpu.VMEM((rows, hidden), F32),
                        pltpu.VMEM((rows, width), F32), pltpu.VMEM((rows, width), LOW), pltpu.VMEM((rows, width), LOW), pltpu.VMEM((8, width), F32)]
        + [pltpu.SemaphoreType.DMA((8,))] * 2,
        compiler_params=pltpu.CompilerParams(collective_id=2, has_side_effects=True, vmem_limit_bytes=60 << 20),
        cost_estimate=pl.CostEstimate(flops=24 * 10**9, bytes_accessed=6 * 10**7, transcendentals=3 * 10**6),
        name="middle")(x, att, wo, wg, wu, wd, cot, ln, bias_col)


def finish_kernel(count, share, *refs):
    sources, targets, holds, (in_sem, out_sem) = refs[:count], refs[count:2 * count], refs[2 * count:3 * count], refs[3 * count:]
    loads = [pltpu.make_async_copy(source, hold, in_sem.at[n]) for n, (source, hold) in enumerate(zip(sources, holds))]
    stores = [pltpu.make_async_copy(hold, target, out_sem.at[n]) for n, (hold, target) in enumerate(zip(holds[:-1], targets[:-1]))]
    for load in loads:
        load.start()
    for load, store in zip(loads[:-1], stores):
        load.wait()
        store.start()
    loads[-1].wait()
    targets[-1][...] = holds[-1][0:4, 0:share]
    for store in stores:
        store.wait()


def finish(results, share):
    count = len(results)
    anywhere = pl.BlockSpec(memory_space=pl.ANY)
    shapes = [jax.ShapeDtypeStruct(r.shape, r.dtype) for r in results]
    shapes[-1] = jax.ShapeDtypeStruct((4, share), results[-1].dtype)
    return pl.pallas_call(
        functools.partial(finish_kernel, count, share), out_shape=shapes,
        in_specs=[anywhere] * count, out_specs=[anywhere] * (count - 1) + [FULL],
        scratch_shapes=[pltpu.VMEM(r.shape, r.dtype) for r in results] + [pltpu.SemaphoreType.DMA((count,))] * 2,
        name="finish")(*results)

FIRST_ORDERS = ("yzx", "xzy", "zyx", "zxy")
REST_ORDERS = ("xzy", "zyx", "zyx")
REST_STARTS = (12, 6, 0)
REST_MIXES = 20
TOKENS_AT = (1, 4, 7, 10, 13, 16, 18, 20)
COTS_AT = (2, 3, 4, 5, 6, 7, 8, 9)
CHUNK = 256


def front_kernel(tok, cot, w_qkv, w_out, w_gate, w_up, w_down, ln_in, len_in, turns_far, turns_near,
                 x_all, c_own, ln_out, w_first, wide_gate, wide_up, wide_down, q_out, k_out, v_out, att_out, cos_out, sin_out, bias_out, lse_out, *refs):
    (xv, wv, qv, kv, vv, attv, cosv, sinv, biasv, rowv, small, smalls, lnv, lsev), refs = refs[:14], refs[14:]
    (first_send, first_recv, first_sib, rest_send, rest_recv, rest_sib, own_sem, tok_send, tok_recv, tok_sib, cot_recv,
     small_send, small_recv, out_sem) = refs
    core, chip, x, y, z = place()
    other = 1 - core
    slots, span = tok.shape[0], tok.shape[1]
    half = CHIPS // 2
    me = core * CHIPS + chip
    rows, width = qv.shape
    can = (True, True, z < ZS - 1, z > 0, True)
    neighbours = (
        {"dp": core, "seq": chip_at(1 - x, y, z)},
        {"dp": core, "seq": chip_at(x, 1 - y, z)},
        {"dp": core, "seq": chip_at(x, y, jnp.minimum(z + 1, ZS - 1))},
        {"dp": core, "seq": chip_at(x, y, jnp.maximum(z - 1, 0))},
        {"dp": other, "seq": chip},
    )
    shards, wides = (w_gate, w_up, w_down), (wide_gate, wide_up, wide_down)
    n_first = w_out.shape[0]
    c_first = w_out.shape[1]

    def first_region(n, owner, source):
        return wv.at[owner, pl.ds(pl.multiple_of(source * n_first, n_first), n_first), n * c_first:n * c_first + c_first]

    def first_own(n):
        return w_out if n == 3 else w_qkv.at[:, n * c_first:n * c_first + c_first]

    def rest_region(m, owner, source):
        size = shards[m].shape[0]
        return wides[m].at[owner, pl.ds(pl.multiple_of(source * size, size), size)]

    def first_piece(n, source, link, own=False):
        target = first_region(n, core, source)
        return pltpu.make_async_remote_copy(
            src_ref=first_own(n) if own else target, dst_ref=target, send_sem=first_send.at[n, link, source],
            recv_sem=first_sib.at[n, source] if link == 4 else first_recv.at[n, source],
            device_id=neighbours[link], device_id_type=MESH)

    def rest_piece(m, source, link, own=False):
        target = rest_region(m, core, source)
        return pltpu.make_async_remote_copy(
            src_ref=shards[m] if own else target, dst_ref=target, send_sem=rest_send.at[m, link, source],
            recv_sem=rest_sib.at[m, source] if link == 4 else rest_recv.at[m, source],
            device_id=neighbours[link], device_id_type=MESH)

    def valid(offset):
        dz = offset[2]
        return True if dz == 0 else (z < ZS - dz if dz > 0 else z >= -dz)

    def source_at(offset):
        return chip_at((x + offset[0]) % 2, (y + offset[1]) % 2, z + offset[2])

    def arrive(piece, orders, offset):
        def one():
            source = source_at(offset)
            for m, order in enumerate(orders):
                piece(m, source, 0).wait_recv()
                for link in onward(order, *offset) + [4]:
                    when(can[link], piece(m, source, link).start)
        when(valid(offset), one)

    def send_own(piece, orders, m):
        for link in onward(orders[m], 0, 0, 0) + [4]:
            when(can[link], piece(m, chip, link, own=True).start)

    def drain(piece, orders):
        for offset in OFFSETS:
            def one():
                source = source_at(offset)
                for m, order in enumerate(orders):
                    for link in onward(order, *offset) + [4]:
                        when(can[link], piece(m, source, link).wait_send)
            when(valid(offset), one)

    def rows_of(ref, index):
        return ref.at[pl.ds(pl.multiple_of(index * span, span), span)]

    def deliver(j, source, target, sends, recvs):
        slot = (chip + 1 + j) % half
        to = core * half + slot
        src, dst = source.at[slot], target
        self_copy = (chip // half == core) & (to == chip)

        @pl.when(self_copy)
        def _():
            pltpu.make_async_copy(src, dst, recvs.at[chip % half]).start()

        @pl.when(jnp.logical_not(self_copy))
        def _():
            pltpu.make_async_remote_copy(
                src_ref=src, dst_ref=dst, send_sem=sends.at[slot], recv_sem=recvs.at[chip % half],
                device_id={"dp": chip // half, "seq": to}, device_id_type=MESH).start()

    def small_to(step):
        to = (me + step) % (2 * CHIPS)
        return pltpu.make_async_remote_copy(
            src_ref=small, dst_ref=smalls.at[me], send_sem=small_send.at[step], recv_sem=small_recv.at[me],
            device_id={"dp": to // CHIPS, "seq": to % CHIPS}, device_id_type=MESH)

    lane = lax.broadcasted_iota(jnp.int32, (1, LANES), 1)
    counts = jnp.zeros((1, LANES), F32)
    for j in range(slots):
        counts = counts + jnp.where(lane == j, len_in[j].astype(F32), 0.0)
    small[...] = jnp.zeros_like(small)
    small[0:ln_in.shape[0], 0:ln_in.shape[1]] = ln_in[...].astype(F32)
    small[4:5, :] = counts
    meet_all(core, chip)

    for n in range(4):
        send_own(first_piece, FIRST_ORDERS, n)
        pltpu.make_async_copy(first_own(n), first_region(n, core, chip), own_sem.at[n]).start()
    lax.fori_loop(1, 2 * CHIPS, lambda s, c: (small_to(s).start(), c)[1], 0)
    own_small = pltpu.make_async_copy(small, smalls.at[me], small_recv.at[me])
    own_small.start()

    sign = jnp.where(lane % HEAD < HEAD // 2, -1.0, 1.0).astype(F32)
    near = turns_near.shape[1]
    for far in range(turns_far.shape[1]):
        part = slice(far * near, far * near + near)
        ca, sa = turns_far[0, far:far + 1, :], turns_far[1, far:far + 1, :]
        cosv[part, :] = ca * turns_near[0] - sa * turns_near[1]
        sinv[part, :] = (sa * turns_near[0] + ca * turns_near[1]) * sign

    def relay(i, carry):
        block = rows_of(xv, core * half + i)
        pltpu.make_async_copy(block, block, tok_recv.at[i]).wait()
        pltpu.make_async_remote_copy(
            src_ref=block, dst_ref=block, send_sem=tok_send.at[2, i], recv_sem=tok_sib.at[i],
            device_id=neighbours[4], device_id_type=MESH).start()
        return carry

    waiting = list(OFFSETS[1:])
    for index, offset in enumerate(OFFSETS[1:]):
        for j in range(half):
            if index == TOKENS_AT[j]:
                deliver(j, tok, rows_of(xv, chip), tok_send.at[0], tok_recv)
        for m in range(3):
            if index == REST_STARTS[m]:
                send_own(rest_piece, REST_ORDERS, m)
                pltpu.make_async_copy(shards[m], rest_region(m, core, chip), own_sem.at[4 + m]).start()
        arrive(first_piece, FIRST_ORDERS, offset)
        if index >= REST_MIXES:
            arrive(rest_piece, REST_ORDERS, waiting.pop(0))

    def first_in(source, carry):
        for n in range(4):
            block = first_region(n, other, source)
            pltpu.make_async_copy(block, block, first_sib.at[n, source]).wait()
        return carry

    def small_in(step, carry):
        source = (me + step) % (2 * CHIPS)
        pltpu.make_async_copy(smalls.at[source], smalls.at[source], small_recv.at[source]).wait()
        return carry

    def tok_in(i, carry):
        block = rows_of(xv, other * half + i)
        pltpu.make_async_copy(block, block, tok_sib.at[i]).wait()
        return carry

    lax.fori_loop(0, half, relay, 0)
    lax.fori_loop(0, half, tok_in, 0)
    lax.fori_loop(0, CHIPS, first_in, 0)
    for n in range(4):
        pltpu.make_async_copy(first_own(n), first_region(n, core, chip), own_sem.at[n]).wait()
    lax.fori_loop(1, 2 * CHIPS, small_in, 0)
    own_small.wait()
    norms, share = ln_in.shape
    lnv[...] = jnp.zeros_like(lnv)
    lnv[0:norms, :] = jnp.concatenate([smalls[device, 0:norms, 0:share] for device in range(2 * CHIPS)], 1)
    counted = smalls[chip // half * CHIPS, 4:5, :]
    length = jnp.sum(jnp.where(lane == chip % half, counted, 0.0), axis=1, keepdims=True)
    at_row = lax.broadcasted_iota(jnp.int32, biasv.shape, 0).astype(F32)
    biasv[...] = jnp.where(at_row < length, 0.0, masked_score)
    at_lane = lax.broadcasted_iota(jnp.int32, rowv.shape, 1).astype(F32)
    rowv[...] = jnp.where(at_lane < length, 0.0, masked_score)
    outs = [pltpu.make_async_copy(source, target, out_sem.at[n]) for n, (source, target) in enumerate((
        (xv, x_all), (wv, w_first), (lnv, ln_out), (cosv, cos_out), (sinv, sin_out), (biasv, bias_out),
        (qv, q_out), (kv, k_out), (vv, v_out), (attv, att_out), (lsev, lse_out)))]
    for copy in outs[:6]:
        copy.start()

    mine = pl.ds(pl.multiple_of(core * rows, rows), rows)
    blocks = width // LANES
    per = 3 * blocks // 2

    def weights(block):
        return jnp.concatenate([wv[b // per, :, pl.ds(pl.multiple_of(b % per * LANES, LANES), LANES)] for b in (block, block + 1)], 1)

    def turned(u, cos, sin):
        return u * jnp.concatenate([cos, cos], 1) + turn(u) * jnp.concatenate([sin, sin], 1)

    per_group = (GROUP // LANES) * (rows // CHUNK)
    chunks = width // GROUP * per_group

    def chunk(index, carry):
        group, inner = index // per_group, index % per_group
        cols = pl.ds(pl.multiple_of(group * GROUP, GROUP), GROUP)

        @pl.when(inner == 0)
        def _():
            q = turned(nn(xv[mine, :], weights(2 * group)), cosv[mine, :], sinv[mine, :]).astype(LOW)
            qv[:, cols] = q * jnp.asarray(0.125, LOW)
            kv[:, cols] = turned(nn(xv[...], weights(blocks + 2 * group)), cosv[...], sinv[...]).astype(LOW)
            vv[:, cols] = nn(xv[...], weights(2 * blocks + 2 * group)).astype(LOW)

        pair, block = inner // (rows // CHUNK), inner % (rows // CHUNK)
        here = pl.ds(pl.multiple_of(block * CHUNK, CHUNK), CHUNK)
        lanes = pl.ds(pl.multiple_of(group * GROUP + pair * LANES, LANES), LANES)
        qp, kp, vp = qv[here, lanes], kv[:, lanes], vv[:, lanes]
        low = lane_of(qp.shape) < HEAD
        parts = []
        for head in range(2):
            qm = jnp.where(low if head == 0 else jnp.logical_not(low), qp, jnp.zeros_like(qp))
            s = nt(qm, kp) + rowv[0:1, :]
            top = jnp.max(s, axis=1, keepdims=True)
            p = jnp.exp(s - top)
            total = jnp.sum(p, axis=1, keepdims=True)
            at_head = pl.ds(2 * (group * (GROUP // LANES) + pair) + head, 1)
            lsev[at_head, here] = jnp.broadcast_to(top + jnp.log(total), (CHUNK, LANES)).T[0:1, :]
            parts.append(nn(p.astype(LOW), vp) / total)
        attv[here, lanes] = jnp.where(low, parts[0], parts[1]).astype(LOW)

        for k in range(chunks):
            @pl.when(index == k)
            def _():
                for j in range(half):
                    if k == COTS_AT[j]:
                        deliver(j, cot, rows_of(c_own, chip % half), tok_send.at[1], cot_recv)
                if waiting:
                    arrive(rest_piece, REST_ORDERS, waiting.pop(0))
        return carry

    lax.fori_loop(0, chunks, chunk, 0)
    for copy in outs[6:]:
        copy.start()
    while waiting:
        arrive(rest_piece, REST_ORDERS, waiting.pop(0))

    def ends(i, carry):
        block = rows_of(c_own, i)
        pltpu.make_async_copy(block, block, cot_recv.at[i]).wait()
        block = rows_of(xv, core * half + i)
        pltpu.make_async_copy(block, block, tok_send.at[2, i]).wait()
        self_copy = (chip // half == core) & (core * half + i == chip)

        @pl.when(jnp.logical_not(self_copy))
        def _():
            pltpu.make_async_copy(tok.at[i], tok.at[i], tok_send.at[0, i]).wait()
            pltpu.make_async_copy(cot.at[i], cot.at[i], tok_send.at[1, i]).wait()
        return carry

    def rest_in(source, carry):
        for m in range(3):
            block = rest_region(m, other, source)
            pltpu.make_async_copy(block, block, rest_sib.at[m, source]).wait()
        return carry

    lax.fori_loop(1, 2 * CHIPS, lambda s, c: (small_to(s).wait_send(), c)[1], 0)
    lax.fori_loop(0, half, ends, 0)
    drain(first_piece, FIRST_ORDERS)
    drain(rest_piece, REST_ORDERS)
    lax.fori_loop(0, CHIPS, rest_in, 0)
    for m in range(3):
        pltpu.make_async_copy(shards[m], rest_region(m, core, chip), own_sem.at[4 + m]).wait()
    for copy in outs:
        copy.wait()


def front(tokens, cotangent, w_qkv, w_out, w_gate, w_up, w_down, ln_params, lengths, turns_far, turns_near):
    slots, span, width = tokens.shape
    total, rows = span * CHIPS, span * CHIPS // 2
    sds, mem, dma = jax.ShapeDtypeStruct, pltpu.VMEM, pltpu.SemaphoreType.DMA
    anywhere, vmem, smem = (pl.BlockSpec(memory_space=s) for s in (pl.ANY, pltpu.VMEM, pltpu.SMEM))
    wide = lambda w: sds((2, w.shape[0] * CHIPS, w.shape[1]), LOW)
    first = (2, width, w_qkv.shape[1] + w_out.shape[1])
    table, small = (total, LANES), (8, LANES)
    outs = [sds((total, width), LOW), sds((rows, width), LOW), sds((8, width), F32), sds(first, LOW),
            wide(w_gate), wide(w_up), wide(w_down), sds((rows, width), LOW), sds((total, width), LOW), sds((total, width), LOW),
            sds((rows, width), LOW), sds(table, F32), sds(table, F32), sds(table, F32), sds((16, rows), F32)]
    return pl.pallas_call(
        front_kernel,
        out_shape=outs,
        in_specs=[anywhere] * 7 + [vmem, smem, vmem, vmem],
        out_specs=[anywhere] * len(outs),
        scratch_shapes=[
            mem((total, width), LOW), mem(first, LOW), mem((rows, width), LOW), mem((total, width), LOW), mem((total, width), LOW),
            mem((rows, width), LOW), mem(table, F32), mem(table, F32), mem(table, F32), mem((8, total), F32), mem(small, F32),
            mem((2 * CHIPS,) + small, F32), mem((8, width), F32), mem((16, rows), F32),
            dma((4, 5, CHIPS)), dma((4, CHIPS)), dma((4, CHIPS)), dma((3, 5, CHIPS)), dma((3, CHIPS)), dma((3, CHIPS)), dma((7,)),
            dma((3, 8)), dma((8,)), dma((8,)), dma((8,)), dma((2 * CHIPS,)), dma((2 * CHIPS,)), dma((11,))],
        compiler_params=pltpu.CompilerParams(collective_id=0, has_side_effects=True, vmem_limit_bytes=60 << 20),
        name="front",
    )(tokens, cotangent, w_qkv, w_out, w_gate, w_up, w_down, ln_params, lengths, turns_far, turns_near)

BACK_ORDERS = ("xzy", "zyx", "zyx")
LATE_ORDERS = ("zxy", "zyx", "zxy")
FAR_FIRST = OFFSETS[::-1]
SIDES = {"x": 2, "y": 2, "z": ZS}


def far_first(index):
    words = [sum((o[0] + 2 * o[1] + 4 * (o[2] + 3)) << (5 * place) for place, o in enumerate(FAR_FIRST[start:start + 6]))
             for start in range(0, len(FAR_FIRST), 6)]
    word = jnp.int32(words[0])
    for place, value in enumerate(words[1:], 1):
        word = jnp.where(index >= 6 * place, jnp.int32(value), word)
    code = lax.shift_right_logical(word, 5 * (index % 6)) & 31
    return code & 1, lax.shift_right_logical(code, 1) & 1, lax.shift_right_logical(code, 2) - 3


def landing_slots(order):
    sizes, room = {}, 1
    for axis in order:
        sizes[axis] = room * (ZS if axis == "z" else 1)
        room *= SIDES[axis]
    return sizes["x"], sizes["y"], sizes["z"], sizes["z"]


def landing_index(order, link, x, y, z):
    axis = "xyzz"[link]
    index = 0
    for before in order:
        if before == axis:
            break
        index = index * SIDES[before] + {"x": x, "y": y, "z": z}[before]
    return index * ZS + z if axis == "z" else index


def back_scatter_kernel(dwg, dwu, dwd, dwo, dsmall, x_in, w_in, q_in, k_in, v_in, g_in, res_in, cos_in, sin_in, bias_in, att_in, lse_in,
                        gt_out, f_gate, f_up, f_down, f_out, f_qkv, f_small, *refs):
    (xv, wv, qv, kv, vv, gv, own_acc, cosv, sinv, biasv, xt, oth_acc, dq, dk, dv, dw, attv, lsev), refs = refs[:18], refs[18:]
    owns, refs = refs[:3], refs[3:]
    sibs, refs = refs[:4], refs[4:]
    down_out, refs = refs[0], refs[1:]
    lands, refs = refs[:24], refs[24:]
    (gt_low, gt_sib, smalls), refs = refs[:3], refs[3:]
    (in_sem, send_sem, recv_sem, sib_send, sib_recv, own_sem, late_send, late_recv, late_sib_send, late_sib_recv,
     gt_sem, tok_send, gt_recv, small_send, small_recv) = refs
    core, chip, x, y, z = place()
    other = 1 - core
    half = CHIPS // 2
    me = core * CHIPS + chip
    rows = qv.shape[0]
    mine = pl.ds(pl.multiple_of(core * rows, rows), rows)
    theirs = pl.ds(pl.multiple_of(other * rows, rows), rows)
    neighbours = (
        {"dp": core, "seq": chip_at(1 - x, y, z)},
        {"dp": core, "seq": chip_at(x, 1 - y, z)},
        {"dp": core, "seq": chip_at(x, y, jnp.minimum(z + 1, ZS - 1))},
        {"dp": core, "seq": chip_at(x, y, jnp.maximum(z - 1, 0))},
    )
    sibling = {"dp": other, "seq": chip}

    loads = [pltpu.make_async_copy(source, target, in_sem.at[n]) for n, (source, target) in enumerate((
        (k_in, kv), (q_in, qv), (bias_in, biasv), (v_in, vv), (g_in, gv), (att_in, attv), (lse_in, lsev), (x_in, xv), (w_in, wv), (res_in, own_acc), (cos_in, cosv), (sin_in, sinv)))]
    for load in loads:
        load.start()

    def cut(ref, size, index):
        return ref.at[pl.ds(pl.multiple_of(index * size, size), size)]

    rows_gate, rows_down, rows_out = f_gate.shape[0], f_down.shape[0], f_out.shape[0]

    def parts(m, owner, dest):
        if m == 0:
            return [(cut(dwg.at[owner], rows_gate, dest), 0, rows_gate)]
        if m == 1:
            return [(cut(dwu.at[owner], rows_gate, dest), 0, rows_gate)]
        return [(cut(dwd.at[owner], rows_down, dest), 0, rows_down), (cut(dwo.at[owner], rows_out, dest), rows_down, rows_out)]

    def to_sibling(m, dest):
        return [pltpu.make_async_remote_copy(
            src_ref=source, dst_ref=sibs[m].at[dest, pl.ds(start, size)], send_sem=sib_send.at[m + n, dest],
            recv_sem=sib_recv.at[m + n, dest], device_id=sibling, device_id_type=MESH)
            for n, (source, start, size) in enumerate(parts(m, other, dest))]

    def own_load(m, dest, slot):
        return [pltpu.make_async_copy(source, owns[m].at[slot, pl.ds(start, size)], own_sem.at[m + n, slot])
                for n, (source, start, size) in enumerate(parts(m, core, dest))]

    def dest_of(index):
        dx, dy, dz = far_first(index)
        return dx, dy, dz, (z + dz >= 0) & (z + dz < ZS), (x + dx) % 2, (y + dy) % 2, jnp.clip(z + dz, 0, ZS - 1)

    greet_all(core, chip)

    def reduce_piece(order, lands_m, send_at, recv_at, own, acc, offset, target, last, final):
        dx, dy, dz = offset
        tx, ty, tz = target
        fx, fy, up, down = spread(order, dx, dy, dz)
        flags = (fx, fy, up & (z < ZS - 1), down & (z > 0))

        @pl.when(jnp.logical_not(last))
        def _():
            acc[...] += own()

        @pl.when(last)
        def _():
            final[...] = acc[...].astype(F32) + own().astype(F32)

        for link in range(4):
            land = lands_m[link].at[landing_index(order, link, tx, ty, tz)]

            @pl.when(flags[link])
            def _():
                pltpu.make_async_copy(land, land, recv_at(link)).wait()

            @pl.when(flags[link] & jnp.logical_not(last))
            def _():
                acc[...] += land[...]

            @pl.when(flags[link] & last)
            def _():
                final[...] += land[...].astype(F32)

        away = {"x": dx != 0, "y": dy != 0, "z": dz != 0}
        taken = None
        for axis in order[::-1]:
            here = away[axis] if taken is None else away[axis] & jnp.logical_not(taken)
            taken = away[axis] if taken is None else taken | away[axis]
            for link in {"x": (0,), "y": (1,), "z": (2, 3)}[axis]:
                go = here if axis != "z" else (here & (dz > 0 if link == 2 else dz < 0))
                there = {0: 0, 1: 1, 2: 3, 3: 2}[link]

                @pl.when(go)
                def _():
                    pltpu.make_async_remote_copy(
                        src_ref=acc, dst_ref=lands_m[there].at[landing_index(order, there, tx, ty, tz)],
                        send_sem=send_at, recv_sem=recv_at(there), device_id=neighbours[link], device_id_type=MESH).start()

    def early(index):
        dx, dy, dz, valid, tx, ty, tz = dest_of(index)
        last = index == len(FAR_FIRST) - 1
        prefetch(index + 2)

        @pl.when(valid)
        def _():
            dest = chip_at(tx, ty, tz)
            for m in range(3):
                for copy in own_load(m, dest, index % 3):
                    copy.wait()
                for copy in to_sibling(m, dest):
                    copy.wait_recv()
                reduce_piece(BACK_ORDERS[m], lands[4 * m:4 * m + 4], send_sem.at[m, dest], lambda link: recv_sem.at[m, link, dest],
                             lambda: owns[m][index % 3], sibs[m].at[dest], (dx, dy, dz), (tx, ty, tz), last, (f_gate, f_up, down_out)[m])

    step = 256
    per_group = (GROUP // LANES) * (rows // step) * 2
    groups = xv.shape[1] // GROUP
    chunks = groups * per_group
    blocks = xv.shape[1] // LANES
    for load in loads[:7]:
        load.wait()

    def chunk(index):
        group, inner = index // per_group, index % per_group
        pair, block, head = inner // (per_group // 2), inner // 2 % (rows // step), inner % 2
        here = pl.ds(pl.multiple_of(block * step, step), step)
        lanes = pl.ds(pl.multiple_of(group * GROUP + pair * LANES, LANES), LANES)
        out_lanes = pl.ds(pl.multiple_of(pair * LANES, LANES), LANES)

        @pl.when(inner == 0)
        def _():
            dq[...] = jnp.zeros_like(dq)
            dk[...] = jnp.zeros_like(dk)
            dv[...] = jnp.zeros_like(dv)

        qp, gp = qv[here, lanes], gv[here, lanes]
        keep = lane_of(qp.shape) // HEAD == head
        qm, gm = jnp.where(keep, qp, jnp.zeros_like(qp)), jnp.where(keep, gp, jnp.zeros_like(gp))
        kp, vp = kv[:, lanes], vv[:, lanes]
        s = nt(kp, qm) + jnp.concatenate([biasv[...]] * (step // LANES), 1)
        p = jnp.exp(s - lsev[pl.ds(2 * (group * (GROUP // LANES) + pair) + head, 1), here])
        dp = nt(vp, gm)
        shares = gm.astype(F32) * attv[here, lanes].astype(F32)
        delta = lax.dot_general(jnp.ones((8, LANES), F32), shares, (((1,), (1,)), ((), ())),
                                precision=lax.Precision.HIGHEST, preferred_element_type=F32)[0:1, :]
        ds = (p * (dp - delta)).astype(LOW)
        dv[:, out_lanes] += nn(p.astype(LOW), gm)
        dk[:, out_lanes] += nn(ds, qm)
        dq[here, out_lanes] += jnp.where(keep, tn(ds, kp), 0.0)

        @pl.when(index == per_group - 1)
        def _():
            for load in loads[7:]:
                load.wait()
            xt[...] = xv[...].T
            oth_acc[...] = jnp.zeros_like(oth_acc)

        @pl.when(inner == per_group - 1)
        def _():
            finish(group)

    def finish(group):
        def back(u, cos, sin):
            return u * jnp.concatenate([cos, cos], 1) - turn(u) * jnp.concatenate([sin, sin], 1)

        def put(block, value):
            per = dw.shape[2] // LANES
            for i in range(2):
                b = block + i
                dw[b // per, :, pl.ds(pl.multiple_of(b % per * LANES, LANES), LANES)] = value[:, i * LANES:i * LANES + LANES].astype(LOW)

        def weights(block):
            per = dw.shape[2] // LANES
            return jnp.concatenate([wv[b // per, :, pl.ds(pl.multiple_of(b % per * LANES, LANES), LANES)] for b in (block, block + 1)], 1)

        gq = back(dq[...] * 0.125, cosv[mine, :], sinv[mine, :]).astype(LOW)
        dk[...] = back(dk[...], cosv[...], sinv[...])
        put(2 * group, nn(xt[:, mine], gq))
        put(blocks + 2 * group, nn(xt[...], dk[...].astype(LOW)))
        put(2 * blocks + 2 * group, nn(xt[...], dv[...].astype(LOW)))
        wq, wk, wvv = (weights(n * blocks + 2 * group) for n in range(3))
        own_acc[...] += nt(gq, wq) + nt(dk[mine, :].astype(LOW), wk) + nt(dv[mine, :].astype(LOW), wvv)
        oth_acc[...] += nt(dk[theirs, :].astype(LOW), wk) + nt(dv[theirs, :].astype(LOW), wvv)

    def turn_of(index, carry):
        chunk(index)

        @pl.when(index - ahead < mixed)
        def _():
            early(index - ahead)
        return carry

    ahead = 1
    lax.fori_loop(0, ahead, lambda index, c: (chunk(index), c)[1], 0)
    all_here()

    def begin(index, carry):
        dx, dy, dz, valid, tx, ty, tz = dest_of(index)

        @pl.when(valid)
        def _():
            for m in range(3):
                for copy in to_sibling(m, chip_at(tx, ty, tz)):
                    copy.start()
        return carry

    lax.fori_loop(0, len(FAR_FIRST), begin, 0)

    def prefetch(index):
        dx, dy, dz, valid, tx, ty, tz = dest_of(index)

        @pl.when(valid & (index < len(FAR_FIRST)))
        def _():
            for m in range(3):
                for copy in own_load(m, chip_at(tx, ty, tz), index % 3):
                    copy.start()

    prefetch(jnp.int32(0))
    prefetch(jnp.int32(1))

    def small_to(step):
        to = (me + step) % (2 * CHIPS)
        return pltpu.make_async_remote_copy(
            src_ref=dsmall.at[to], dst_ref=smalls.at[me], send_sem=small_send.at[step], recv_sem=small_recv.at[me],
            device_id={"dp": to // CHIPS, "seq": to % CHIPS}, device_id_type=MESH)

    lax.fori_loop(1, 2 * CHIPS, lambda s, c: (small_to(s).start(), c)[1], 0)
    own_small = pltpu.make_async_copy(dsmall.at[me], smalls.at[me], small_recv.at[me])
    own_small.start()

    mixed = min(chunks - ahead, len(FAR_FIRST) - 4)
    lax.fori_loop(ahead, chunks, turn_of, 0)

    gt_low[...] = oth_acc[...].astype(LOW)
    third = f_qkv.shape[1] // len(LATE_ORDERS)

    def late_to_sibling(dest):
        return pltpu.make_async_remote_copy(
            src_ref=cut(dw.at[other], rows_gate, dest), dst_ref=sibs[3].at[dest], send_sem=late_sib_send.at[dest],
            recv_sem=late_sib_recv.at[dest], device_id=sibling, device_id_type=MESH)

    def late_begin(index, carry):
        dx, dy, dz, valid, tx, ty, tz = dest_of(index)

        @pl.when(valid)
        def _():
            late_to_sibling(chip_at(tx, ty, tz)).start()
        return carry

    lax.fori_loop(0, len(FAR_FIRST), late_begin, 0)
    cross = pltpu.make_async_remote_copy(src_ref=gt_low, dst_ref=gt_sib, send_sem=gt_sem.at[0], recv_sem=gt_sem.at[1],
                                         device_id=sibling, device_id_type=MESH)
    cross.start()

    def late(offset):
        dx, dy, dz = offset
        final_step = offset == (0, 0, 0)

        def one():
            tx, ty, tz = (x + dx) % 2, (y + dy) % 2, z + dz
            dest = chip_at(tx, ty, tz)
            late_to_sibling(dest).wait_recv()
            for n, order in enumerate(LATE_ORDERS):
                lanes = slice(n * third, n * third + third)
                acc = sibs[3].at[dest, :, lanes]
                own = dw[core, pl.ds(pl.multiple_of(dest * rows_gate, rows_gate), rows_gate), lanes]
                total = f_qkv.at[:, lanes] if final_step else acc
                total[...] = (acc[...].astype(F32) + own.astype(F32)).astype(total.dtype)
                for link in onward(order, dx, dy, dz):
                    land = lands[12 + 4 * n + link].at[landing_index(order, link, tx, ty, tz)]

                    def add():
                        pltpu.make_async_copy(land, land, late_recv.at[n, link, dest]).wait()
                        total[...] += land[...].astype(total.dtype)
                    when({2: z < ZS - 1, 3: z > 0}.get(link, True), add)
                if not final_step:
                    link = next({"x": 0, "y": 1, "z": 2 if dz > 0 else 3}[axis] for axis in order[::-1] if {"x": dx, "y": dy, "z": dz}[axis])
                    there = {0: 0, 1: 1, 2: 3, 3: 2}[link]
                    pltpu.make_async_remote_copy(
                        src_ref=acc, dst_ref=lands[12 + 4 * n + there].at[landing_index(order, there, tx, ty, tz)],
                        send_sem=late_send.at[n, dest], recv_sem=late_recv.at[n, there, dest],
                        device_id=neighbours[link], device_id_type=MESH).start()
        when(True if dz == 0 else (z < ZS - dz if dz > 0 else z >= -dz), one)

    early_steps, left = 8, mixed
    for step_index, offset in enumerate(FAR_FIRST):
        if step_index == early_steps:
            cross.wait()
            gt_low[...] = (own_acc[...] + gt_sib[...].astype(F32)).astype(LOW)
            for j in range(half):
                from_slot(core, chip, j, gt_low, gt_out, tok_send, gt_recv)
        late(offset)
        if step_index % 2 == 1 and left < len(FAR_FIRST):
            early(jnp.int32(left))
            left += 1
    f_down[...] = down_out[0:rows_down, :]
    f_out[...] = down_out[rows_down:rows_down + rows_out, :]

    def small_end(s, carry):
        small_to(s).wait_send()
        source = (me + s) % (2 * CHIPS)
        pltpu.make_async_copy(smalls.at[source], smalls.at[source], small_recv.at[source]).wait()
        return carry

    lax.fori_loop(1, 2 * CHIPS, small_end, 0)
    own_small.wait()
    f_small[...] = jnp.sum(smalls[...], axis=0)

    sent_blocks(core, chip, gt_out.at[0], tok_send)
    lax.fori_loop(0, half, lambda i, c: (pltpu.make_async_copy(gt_out.at[i], gt_out.at[i], gt_recv.at[i]).wait(), c)[1], 0)

    def sent(dest, carry):
        for m in range(3):
            for copy in to_sibling(m, dest):
                copy.wait_send()
        late_to_sibling(dest).wait_send()

        @pl.when(dest != chip)
        def _():
            for m in range(3):
                pltpu.make_async_copy(sibs[m].at[dest], sibs[m].at[dest], send_sem.at[m, dest]).wait()
            for n in range(len(LATE_ORDERS)):
                part = sibs[3].at[dest, :, pl.ds(n * third, third)]
                pltpu.make_async_copy(part, part, late_send.at[n, dest]).wait()
        return carry

    lax.fori_loop(0, CHIPS, sent, 0)


def back_scatter(dwg, dwu, dwd, dwo, dsmall, x, w, q, k, v, g_att, g_res1, cos, sin, bias_col, att, lse):
    tokens, width = x.shape
    rows = tokens // 2
    span = rows // 8
    anywhere, vmem = pl.BlockSpec(memory_space=pl.ANY), pl.BlockSpec(memory_space=pltpu.VMEM)
    n_gate, n_down, n_out = width // CHIPS, dwd.shape[1] // CHIPS, dwo.shape[1] // CHIPS
    c_gate, c_down = dwg.shape[2], dwd.shape[2]
    c_qkv = 3 * width // 2
    third = c_qkv // len(LATE_ORDERS)
    sds, mem = jax.ShapeDtypeStruct, pltpu.VMEM
    out8 = sds((8, span, width), LOW)
    finals = [sds((n_gate, c_gate), F32), sds((n_gate, c_gate), F32), sds((n_down, c_down), F32), sds((n_out, c_down), F32),
              sds((n_gate, c_qkv), F32), sds(dsmall.shape[1:], F32)]
    pieces = [(n_gate, c_gate), (n_gate, c_gate), (n_down + n_out, c_down)]
    scratch = [mem((tokens, width), LOW), mem(w.shape, LOW), mem((rows, width), LOW), mem((tokens, width), LOW), mem((tokens, width), LOW),
               mem((rows, width), LOW), mem((rows, width), F32), mem(cos.shape, F32), mem(sin.shape, F32), mem(bias_col.shape, F32),
               mem((width, tokens), LOW), mem((rows, width), F32), mem((rows, GROUP), F32), mem((tokens, GROUP), F32), mem((tokens, GROUP), F32),
               mem((2, width, c_qkv), LOW), mem((rows, width), LOW), mem(lse.shape, F32)]
    scratch += [mem((3,) + piece, LOW) for piece in pieces]
    scratch += [mem((CHIPS,) + piece, LOW) for piece in pieces] + [mem((CHIPS, n_gate, c_qkv), LOW)]
    scratch += [mem(pieces[2], F32)]
    for order, piece in zip(BACK_ORDERS, pieces):
        scratch += [mem((n,) + piece, LOW) for n in landing_slots(order)]
    for order in LATE_ORDERS:
        scratch += [mem((n, n_gate, third), LOW) for n in landing_slots(order)]
    scratch += [mem((rows, width), LOW), mem((rows, width), LOW), mem(dsmall.shape, F32)]
    dma = pltpu.SemaphoreType.DMA
    scratch += [dma((12,)), dma((3, CHIPS)), dma((3, 4, CHIPS)), dma((4, CHIPS)), dma((4, CHIPS)), dma((4, 3)), dma((3, CHIPS)), dma((3, 4, CHIPS)),
                dma((CHIPS,)), dma((CHIPS,)), dma((2,)), dma((8,)), dma((8,)), dma((2 * CHIPS,)), dma((2 * CHIPS,))]
    return pl.pallas_call(
        back_scatter_kernel,
        out_shape=[out8] + finals,
        in_specs=[anywhere] * 17,
        out_specs=[anywhere] + [vmem] * len(finals),
        scratch_shapes=scratch,
        compiler_params=pltpu.CompilerParams(collective_id=1, has_side_effects=True, vmem_limit_bytes=67043328),
        name="back_scatter",
    )(dwg, dwu, dwd, dwo, dsmall, x, w, q, k, v, g_att, g_res1, cos, sin, bias_col, att, lse)


def rotary_turns(tokens, near):
    pair_index = (np.arange(LANES) % (HEAD // 2)).astype(np.float32)
    inverse = np.power(np.float32(1000.0), np.float32(-2.0) * pair_index / np.float32(HEAD))

    def table(positions):
        angles = positions.astype(np.float32)[:, None] * inverse[None, :]
        return jnp.asarray(np.stack([np.cos(angles), np.sin(angles)]), F32)

    return table(np.arange(0, tokens, near)), table(np.arange(near))


def local_by_slot(tokens, lengths, w_qkv, w_out, w_gate, w_up, w_down, ln_params, cotangent):
    slots, span, width = tokens.shape
    share = ln_params.shape[1]
    turns_far, turns_near = rotary_turns(span * CHIPS, span)
    x, cot, ln, w_in, wg, wu, wd, q, k, v, att, cos, sin, bias_col, lse = front(
        tokens, cotangent, w_qkv, w_out, w_gate, w_up, w_down, ln_params, lengths, turns_far, turns_near)
    y, dwg, dwu, dwd, dwo, g_att, g_res1, dsmall = middle(x, att, w_in, wg, wu, wd, cot, ln, bias_col)
    results = back_scatter(dwg, dwu, dwd, dwo, dsmall, x, w_in, q, k, v, g_att, g_res1, cos, sin, bias_col, att, lse)
    output, grad_tokens, d_gate, d_up, d_down, d_out, d_qkv, d_small = finish([y, *results], share)
    return (output, grad_tokens, d_qkv, d_out, d_gate, d_up, d_down, d_small)


def solution(mesh):
    placed = (
        P("dp", "seq", None),
        P("dp"),
        P("seq", "dp"),
        P("seq", "dp"),
        P("seq", "dp"),
        P("seq", "dp"),
        P("seq", "dp"),
        P(None, ("dp", "seq")),
        P("dp", "seq", None),
    )

    def run(tokens, *rest):
        by_slot = mesh.shape["dp"] == 2 and mesh.shape["seq"] == CHIPS and tokens.shape[0] == CHIPS
        body = local_by_slot if by_slot else local
        return jax.shard_map(
            body,
            mesh=mesh,
            in_specs=placed,
            out_specs=(
                P("dp", "seq", None),
                P("dp", "seq", None),
                P("seq", "dp"),
                P("seq", "dp"),
                P("seq", "dp"),
                P("seq", "dp"),
                P("seq", "dp"),
                P(None, ("dp", "seq")),
            ),
            check_vma=False,
        )(tokens, *rest)

    return run
```
